32 devices in a mesh: dp: 1 (over z), sp: 32 (over y, x, core).
Axes of the slice: x: 4, y: 4, z: 1, core: 2. Of those that a mesh axis runs over, the one named last changes fastest.
The devices are a block of a 4x4x8 slice.
Arguments:
- x_patch: bfloat16 [64, 576, 512], P('dp', 'sp')
- w_tok1: bfloat16 [576, 256], P('sp')
- b_tok1: float32 [256], P('sp')
- w_tok2: bfloat16 [256, 576], P(None, 'sp')
- b_tok2: float32 [576], P('sp')
- w_ch1: bfloat16 [512, 2048], replicated
- b_ch1: float32 [2048], replicated
- w_ch2: bfloat16 [2048, 512], replicated
- b_ch2: float32 [512], replicated
- ln1_gain: float32 [512], replicated
- ln1_bias: float32 [512], replicated
- ln2_gain: float32 [512], replicated
- ln2_bias: float32 [512], replicated
Outputs:
- output: bfloat16 [64, 576, 512], P('dp', 'sp')
All inputs are finite; a program needn't handle non-finite values.
Results may differ from the reference program's by a relative error of at most 0.00440373.
Values are sent between devices in bfloat16 or wider.
A program may use at most 768 MiB of HBM per device.

```python
import jax
import jax.numpy as jnp
from jax import lax

BATCH = 64
PATCHES = 576
CHANNELS = 512
TOKEN_HID = 256
CHAN_HID = 2048
LN_EPS = 1e-6


def draw_normal(rng_key, out_shape, spread):
    return jax.random.normal(rng_key, out_shape, jnp.float32) * spread


def setup_inputs(seed: int = 0, part: int = 0) -> dict:
    shared = jax.random.split(jax.random.key(seed), 12)
    x_key = jax.random.fold_in(jax.random.key(seed + 1), part)
    x_patch = jax.random.normal(x_key, (BATCH, PATCHES, CHANNELS), jnp.float32)
    return {
        "x_patch": x_patch.astype(jnp.bfloat16),
        "w_tok1": draw_normal(shared[0], (PATCHES, TOKEN_HID), PATCHES ** -0.5).astype(jnp.bfloat16),
        "b_tok1": draw_normal(shared[1], (TOKEN_HID,), 0.5),
        "w_tok2": draw_normal(shared[2], (TOKEN_HID, PATCHES), TOKEN_HID ** -0.5).astype(jnp.bfloat16),
        "b_tok2": draw_normal(shared[3], (PATCHES,), 0.5),
        "w_ch1": draw_normal(shared[4], (CHANNELS, CHAN_HID), CHANNELS ** -0.5).astype(jnp.bfloat16),
        "b_ch1": draw_normal(shared[5], (CHAN_HID,), 0.5),
        "w_ch2": draw_normal(shared[6], (CHAN_HID, CHANNELS), CHAN_HID ** -0.5).astype(jnp.bfloat16),
        "b_ch2": draw_normal(shared[7], (CHANNELS,), 0.3),
        "ln1_gain": 1.0 + draw_normal(shared[8], (CHANNELS,), 0.2),
        "ln1_bias": draw_normal(shared[9], (CHANNELS,), 0.3),
        "ln2_gain": 1.0 + draw_normal(shared[10], (CHANNELS,), 0.2),
        "ln2_bias": draw_normal(shared[11], (CHANNELS,), 0.3),
    }


def layer_norm(values, ln_gain, ln_bias):
    mean_val = jnp.mean(values, axis=-1, keepdims=True)
    centred = values - mean_val
    var_val = jnp.mean(centred * centred, axis=-1, keepdims=True)
    return centred * lax.rsqrt(var_val + LN_EPS) * ln_gain + ln_bias


def reference(x_patch, w_tok1, b_tok1, w_tok2, b_tok2, w_ch1, b_ch1, w_ch2, b_ch2, ln1_gain, ln1_bias, ln2_gain, ln2_bias):
    def one_image(x_img):
        x_wide = x_img.astype(jnp.float32)
        normed = layer_norm(x_wide, ln1_gain, ln1_bias).astype(jnp.bfloat16)
        tok_pre = jnp.dot(w_tok1.T, normed, preferred_element_type=jnp.float32) + b_tok1[:, None]
        tok_act = jax.nn.gelu(tok_pre).astype(jnp.bfloat16)
        tok_out = jnp.dot(w_tok2.T, tok_act, preferred_element_type=jnp.float32) + b_tok2[:, None]
        x_mid = (x_wide + tok_out).astype(jnp.bfloat16)
        mid_wide = x_mid.astype(jnp.float32)
        normed_two = layer_norm(mid_wide, ln2_gain, ln2_bias).astype(jnp.bfloat16)
        ch_pre = jnp.dot(normed_two, w_ch1, preferred_element_type=jnp.float32) + b_ch1
        ch_act = jax.nn.gelu(ch_pre).astype(jnp.bfloat16)
        ch_out = jnp.dot(ch_act, w_ch2, preferred_element_type=jnp.float32) + b_ch2
        return (mid_wide + ch_out).astype(jnp.bfloat16)

    return lax.map(one_image, x_patch)
```

```python
import jax
import jax.numpy as jnp
from jax import lax
from jax.sharding import PartitionSpec as P

LN_EPS = 1e-6


def layer_norm(values, ln_gain, ln_bias):
    mean_val = jnp.mean(values, axis=-1, keepdims=True)
    centred = values - mean_val
    var_val = jnp.mean(centred * centred, axis=-1, keepdims=True)
    return centred * lax.rsqrt(var_val + LN_EPS) * ln_gain + ln_bias


def channel_mix(x_mid, w_ch1, b_ch1, w_ch2, b_ch2, ln2_gain, ln2_bias):
    mid_wide = x_mid.astype(jnp.float32)
    normed_two = layer_norm(mid_wide, ln2_gain, ln2_bias).astype(jnp.bfloat16)
    ch_pre = jnp.einsum("bsc,cf->bsf", normed_two, w_ch1, preferred_element_type=jnp.float32) + b_ch1
    ch_act = jax.nn.gelu(ch_pre).astype(jnp.bfloat16)
    ch_out = jnp.einsum("bsf,fc->bsc", ch_act, w_ch2, preferred_element_type=jnp.float32) + b_ch2
    return (mid_wide + ch_out).astype(jnp.bfloat16)


def solution(mesh):
    row_spec = P("dp", "sp", None)

    def local_layer(x_blk, w1_rows, b1_part, w2_cols, b2_part, w_ch1, b_ch1, w_ch2, b_ch2, ln1_gain, ln1_bias, ln2_gain, ln2_bias):
        x_img = lax.all_to_all(x_blk, "sp", split_axis=0, concat_axis=1, tiled=True)
        w1 = lax.all_gather(w1_rows, "sp", axis=0, tiled=True)
        w2 = lax.all_gather(w2_cols, "sp", axis=1, tiled=True)
        b1 = lax.all_gather(b1_part, "sp", axis=0, tiled=True)
        b2 = lax.all_gather(b2_part, "sp", axis=0, tiled=True)
        x_wide = x_img.astype(jnp.float32)
        normed = layer_norm(x_wide, ln1_gain, ln1_bias).astype(jnp.bfloat16)
        tok_pre = jnp.einsum("sd,bsc->bdc", w1, normed, preferred_element_type=jnp.float32) + b1[None, :, None]
        tok_act = jax.nn.gelu(tok_pre).astype(jnp.bfloat16)
        tok_out = jnp.einsum("ds,bdc->bsc", w2, tok_act, preferred_element_type=jnp.float32) + b2[None, :, None]
        x_mid = (x_wide + tok_out).astype(jnp.bfloat16)
        z_img = channel_mix(x_mid, w_ch1, b_ch1, w_ch2, b_ch2, ln2_gain, ln2_bias)
        return lax.all_to_all(z_img, "sp", split_axis=1, concat_axis=0, tiled=True)

    in_specs = (row_spec, P("sp", None), P("sp"), P(None, "sp"), P("sp"), P(None, None), P(None), P(None, None), P(None), P(None), P(None), P(None), P(None))
    return jax.shard_map(local_layer, mesh=mesh, in_specs=in_specs, out_specs=row_spec, check_vma=False)
```

```python
import functools
import math

import jax
import jax.numpy as jnp
from jax import lax
from jax.experimental import pallas as pl
from jax.experimental.pallas import tpu as pltpu
from jax.sharding import PartitionSpec as P

LN_EPS = 1e-6
AXIS = "sp"
LANES = 128
CORES = 2
VMEM_LIMIT = 67043328
BF16 = jnp.bfloat16
F32 = jnp.float32


def layer_norm(values, ln_gain, ln_bias):
    mean_val = jnp.mean(values, axis=-1, keepdims=True)
    centred = values - mean_val
    var_val = jnp.mean(centred * centred, axis=-1, keepdims=True)
    return centred * lax.rsqrt(var_val + LN_EPS) * ln_gain + ln_bias


def gelu(a):
    return 0.5 * a * (1.0 + jnp.tanh(math.sqrt(2.0 / math.pi) * (a + 0.044715 * (a * a * a))))


def widen(column, copies):
    return jnp.concatenate([column] * copies, axis=1)


def mixer_kernel(
    n, chunks, ff_tile,
    x_hbm, w1_hbm, w2_hbm, b1_ref, b2_ref, wc1_hbm, bc1_ref, wc2_hbm, bc2_ref, g1_ref, o1_ref, g2_ref, o2_ref,
    out_ref,
    x_own, x_img, z_img, w_own, w_all, w1_t, w2_big, b_own, b_all, b1_col, b2_col, h_acc, act, wc1, wc2, tally, w_tally, b_tally,
    local_sem, mine_sem, own_sem, chan_sem, w_send, w_recv, d_send, d_recv, b_send, b_recv, x_send, x_recv, z_send, z_recv,
):
    me = lax.axis_index(AXIS)
    side = math.isqrt(n // CORES)
    my_core = lax.rem(me, CORES)
    my_x = lax.rem(me // CORES, side)
    my_y = me // (CORES * side)
    patches, rows, chans = x_img.shape
    pairs = patches // 2
    hid = w1_hbm.shape[1]
    per = patches // chunks
    m = per * rows

    def peer(k):
        core = lax.rem(my_core + lax.rem(k, CORES), CORES)
        col = lax.rem(my_x + lax.rem(k // CORES, side), side)
        row = lax.rem(my_y + k // (CORES * side), side)
        return (row * side + col) * CORES + core

    def two(j):
        return pl.ds(pl.multiple_of(2 * j, 2), 2)

    def settle(counted, sem):
        pltpu.make_async_copy(counted, counted, sem).wait()

    loads = [pltpu.make_async_copy(x_hbm, x_own, local_sem.at[0])]
    for q in range(pairs):
        loads.append(pltpu.make_async_copy(w1_hbm.at[pl.ds(2 * q, 2), :], w_own.at[q, :, pl.ds(0, hid)], local_sem.at[1 + q]))
        loads.append(pltpu.make_async_copy(w2_hbm.at[pl.ds(2 * q, 2), :], w_own.at[q, :, pl.ds(hid, hid)], local_sem.at[1 + pairs + q]))
    mine = [pltpu.make_async_copy(x_hbm.at[:, two(me), :], x_img.at[:, two(me), :], mine_sem.at[0])]
    for q in range(pairs):
        mine.append(pltpu.make_async_copy(w1_hbm.at[pl.ds(2 * q, 2), :], w_all.at[q, two(me), pl.ds(0, hid)], mine_sem.at[1 + q]))
        mine.append(pltpu.make_async_copy(w2_hbm.at[pl.ds(2 * q, 2), :], w_all.at[q, two(me), pl.ds(hid, hid)], mine_sem.at[1 + pairs + q]))
    for c in loads + mine:
        c.start()
    chan_loads = [pltpu.make_async_copy(wc1_hbm, wc1, chan_sem.at[0]), pltpu.make_async_copy(wc2_hbm, wc2, chan_sem.at[1])]
    for c in chan_loads:
        c.start()
    b_own[...] = jnp.zeros_like(b_own)
    is_mine = lax.broadcasted_iota(jnp.int32, (rows, LANES), 0) // 2 == me
    for i, b_ref in enumerate((b1_ref, b2_ref)):
        b_own[i, :, pl.ds(0, b_ref.shape[1])] = jnp.broadcast_to(b_ref[...], (2, b_ref.shape[1]))
        b_all[i] = jnp.where(is_mine, jnp.broadcast_to(b_own[i, pl.ds(0, 1), :], (rows, LANES)), 0.0)

    barrier = pltpu.get_barrier_semaphore()

    @pl.loop(0, n)
    def _(k):
        pl.semaphore_signal(barrier, inc=1, device_id={AXIS: peer(k)})

    pl.semaphore_wait(barrier, n)
    for c in loads + mine:
        c.wait()

    def remote(src, dst, ss, rs, j):
        return pltpu.make_async_remote_copy(src_ref=src, dst_ref=dst, send_sem=ss, recv_sem=rs, device_id={AXIS: j})

    @pl.loop(1, n // CORES)
    def _(k):
        remote(w_own, w_all.at[:, two(me), :], w_send, w_recv, peer(CORES * k)).start()

    @pl.loop(1, n)
    def _(k):
        remote(b_own, b_all.at[:, two(me), :], b_send, b_recv, peer(k)).start()

    for t in range(chunks):
        part = pl.ds(t * per, per)

        @pl.loop(1, n)
        def _(k):
            j = peer(k)
            remote(x_own.at[part, two(j), :], x_img.at[part, two(me), :], x_send, x_recv.at[t], j).start()

    half = w_all.at[:, pl.ds(0, n), :]
    settle(w_tally, w_recv)
    other = peer(1)

    @pl.loop(0, n // CORES)
    def _(k):
        blk = w_all.at[:, two(CORES * k + my_core), :]
        remote(blk, blk, d_send, d_recv, other).start()

    settle(half, d_recv)
    settle(b_tally, b_recv)

    even = lax.rem(lax.broadcasted_iota(jnp.int32, (rows, 2 * hid), 0), 2) == 0
    keep = even == (lax.broadcasted_iota(jnp.int32, (rows, 2 * hid), 1) < hid)
    for q in range(pairs):
        wq = w_all[q].astype(F32)
        first = jnp.where(even, wq, pltpu.roll(wq, 1, 0))
        second = jnp.where(even, pltpu.roll(wq, rows - 1, 0), wq)
        ones, twos = [], []
        for d in (first, second):
            ones.append(jnp.where(keep, jnp.concatenate([d[:, :hid]] * 2, axis=1), 0.0))
            twos.append(jnp.where(keep, jnp.concatenate([d[:, hid:]] * 2, axis=1), 0.0))
        w1_t[:, pl.ds(2 * rows * q, 2 * rows)] = jnp.transpose(jnp.concatenate(ones, axis=0)).astype(BF16)
        w2_big[pl.ds(2 * rows * q, 2 * rows), :] = jnp.concatenate(twos, axis=0).astype(BF16)

    per_dev = hid // n
    picked = b_all[0, pl.ds(0, n, stride=2), :]
    spread = jnp.broadcast_to(picked.reshape(n, 1, LANES), (n, per_dev, LANES))
    diag = lax.broadcasted_iota(jnp.int32, spread.shape, 1) == lax.broadcasted_iota(jnp.int32, spread.shape, 2)
    col1 = jnp.broadcast_to(jnp.sum(jnp.where(diag, spread, 0.0), axis=2, keepdims=True), spread.shape)
    for i in range(2):
        b1_col[pl.ds(hid * i, hid), :] = col1.reshape(hid, LANES)
    tail = b_all[1]
    for s in range(patches):
        b2_col[pl.ds(rows * s, rows), :] = jnp.broadcast_to(tail[:, s : s + 1], (rows, LANES))

    wide = chans // LANES
    for t in range(chunks):
        part = x_img.at[pl.ds(t * per, per)]
        settle(tally.at[:, pl.ds(0, per)], x_recv.at[t])
        u = layer_norm(part[...].reshape(m, chans).astype(F32), g1_ref[...], o1_ref[...]).astype(BF16)
        term = jnp.dot(w1_t[:, pl.ds(t * m, m)], u, preferred_element_type=F32)
        h_acc[...] = term if t == 0 else h_acc[...] + term
    g = gelu(h_acc[...] + widen(b1_col[...], wide)).astype(BF16)
    for c in chan_loads:
        c.wait()

    ff = wc1.shape[1]
    owns = []
    for t in range(chunks):
        part = pl.ds(t * per, per)
        tok = jnp.dot(w2_big[pl.ds(t * m, m), :], g, preferred_element_type=F32) + widen(b2_col[pl.ds(t * m, m), :], wide)
        x_mid = (x_img[part].reshape(m, chans).astype(F32) + tok).astype(BF16)
        mid_wide = x_mid.astype(F32)
        v = layer_norm(mid_wide, g2_ref[...], o2_ref[...]).astype(BF16)
        for f in range(ff // ff_tile):
            cols = pl.ds(f * ff_tile, ff_tile)
            pre = jnp.dot(v, wc1[:, cols], preferred_element_type=F32) + bc1_ref[:, cols]
            act[:, cols] = gelu(pre).astype(BF16)
        ch_out = jnp.dot(act[...], wc2[...], preferred_element_type=F32) + bc2_ref[...]
        z_img[part] = (mid_wide + ch_out).astype(BF16).reshape(per, rows, chans)

        own = pltpu.make_async_copy(z_img.at[part, two(me), :], out_ref.at[part, two(me), :], own_sem.at[t])
        own.start()
        owns.append(own)

        @pl.loop(1, n)
        def _(k):
            j = peer(k)
            remote(z_img.at[part, two(j), :], out_ref.at[part, two(me), :], z_send, z_recv, j).start()

    for c in owns:
        c.wait()
    for counted, sem in ((tally, z_recv), (tally, z_send), (tally, x_send), (w_tally, w_send), (b_tally, b_send), (half, d_send)):
        settle(counted, sem)


def solution(mesh, chunks=3, ff_tile=512):
    row_spec = P("dp", AXIS, None)
    n = mesh.shape[AXIS]

    def local_layer(x_blk, w1_rows, b1_part, w2_cols, b2_part, w_ch1, b_ch1, w_ch2, b_ch2, ln1_gain, ln1_bias, ln2_gain, ln2_bias):
        x_t = jnp.transpose(x_blk, (1, 0, 2))
        w2_rows = jnp.transpose(w2_cols)
        patches, rows, chans = x_t.shape
        hid = w1_rows.shape[1]
        ff = w_ch1.shape[1]
        m = patches // chunks * rows
        any_spec = pl.BlockSpec(memory_space=pltpu.HBM)
        vm = pl.BlockSpec(memory_space=pltpu.VMEM)
        sem = pltpu.SemaphoreType.DMA
        z_t = pl.pallas_call(
            functools.partial(mixer_kernel, n, chunks, ff_tile),
            name="mixer",
            out_shape=jax.ShapeDtypeStruct(x_t.shape, BF16),
            in_specs=[any_spec, any_spec, any_spec, vm, vm, any_spec, vm, any_spec, vm, vm, vm, vm, vm],
            out_specs=any_spec,
            scratch_shapes=[
                pltpu.VMEM(x_t.shape, BF16),
                pltpu.VMEM(x_t.shape, BF16),
                pltpu.VMEM(x_t.shape, BF16),
                pltpu.VMEM((patches // 2, 2, 2 * hid), BF16),
                pltpu.VMEM((patches // 2, rows, 2 * hid), BF16),
                pltpu.VMEM((2 * hid, patches * rows), BF16),
                pltpu.VMEM((patches * rows, 2 * hid), BF16),
                pltpu.VMEM((2, 2, LANES), F32),
                pltpu.VMEM((2, rows, LANES), F32),
                pltpu.VMEM((2 * hid, LANES), F32),
                pltpu.VMEM((patches * rows, LANES), F32),
                pltpu.VMEM((2 * hid, chans), F32),
                pltpu.VMEM((m, ff), BF16),
                pltpu.VMEM(w_ch1.shape, BF16),
                pltpu.VMEM(w_ch2.shape, BF16),
                pltpu.VMEM((n - 1, patches, 2, chans), BF16),
                pltpu.VMEM((n // CORES - 1, patches // 2, 2, 2 * hid), BF16),
                pltpu.VMEM((n - 1, 2, 2, LANES), F32),
                sem((1 + patches,)),
                sem((1 + patches,)),
                sem((chunks,)),
                sem((2,)),
                sem, sem, sem, sem, sem, sem, sem,
                sem((chunks,)),
                sem, sem,
            ],
            compiler_params=pltpu.CompilerParams(collective_id=0, has_side_effects=True, vmem_limit_bytes=VMEM_LIMIT),
        )(
            x_t, w1_rows, w2_rows, b1_part[None, :], b2_part[None, :], w_ch1, b_ch1[None, :], w_ch2, b_ch2[None, :],
            ln1_gain[None, :], ln1_bias[None, :], ln2_gain[None, :], ln2_bias[None, :],
        )
        return jnp.transpose(z_t, (1, 0, 2))

    in_specs = (row_spec, P(AXIS, None), P(AXIS), P(None, AXIS), P(AXIS), P(None, None), P(None), P(None, None), P(None), P(None), P(None), P(None), P(None))
    return jax.shard_map(local_layer, mesh=mesh, in_specs=in_specs, out_specs=row_spec, check_vma=False)
```

```python
import functools
import math

import jax
import jax.numpy as jnp
from jax import lax
from jax.experimental import pallas as pl
from jax.experimental.pallas import tpu as pltpu
from jax.sharding import PartitionSpec as P

LN_EPS = 1e-6
AXIS = "sp"
LANES = 128
CORES = 2
PAIR = 2
VMEM_LIMIT = 67043328
BF16 = jnp.bfloat16
F32 = jnp.float32


def layer_norm(values, ln_gain, ln_bias):
    mean_val = jnp.mean(values, axis=-1, keepdims=True)
    centred = values - mean_val
    var_val = jnp.mean(centred * centred, axis=-1, keepdims=True)
    return centred * lax.rsqrt(var_val + LN_EPS) * ln_gain + ln_bias


def gelu(a):
    return 0.5 * a * (1.0 + jnp.tanh(math.sqrt(2.0 / math.pi) * (a + 0.044715 * (a * a * a))))


def widen(column, copies):
    return jnp.concatenate([column] * copies, axis=1)


def send_order(side):
    hops = lambda d: min(d, side - d)
    flows = []
    for dx, dy in sorted(
        ((dx, dy) for dx in range(side) for dy in range(side) if dx or dy),
        key=lambda o: (hops(o[0]) + hops(o[1]), max(hops(o[0]), hops(o[1])), o),
    ):
        for flow in ((dx, dy), ((side - dx) % side, (side - dy) % side)):
            if flow not in flows:
                flows.append(flow)
    return flows[::-1]


def mixer_kernel(
    n, a_parts, b_parts, b_after, ff_tile,
    x_hbm, w1_hbm, w2_hbm, b1_hbm, b2_hbm, wc1_hbm, bc1_hbm, wc2_hbm, bc2_hbm, g1_hbm, o1_hbm, g2_hbm, o2_hbm,
    out_ref, spare,
    x_own, x_img, z_img, w1_own, w2_own, w1_all, w2_all, w1_t, w2_big, b_own, b_all, b1_col, b2_col, h_mine, h_other, act, wc1, wc2,
    b1_v, b2_v, bc1, bc2, g1, o1, g2, o2, x_tally, w_tally, b_tally,
    local_sem, mine_sem, chan_sem, small_sem, own_sem,
    w_send, w_recv, b_send, b_recv, x_send, x_recv, h_send, h_recv, z_send, z_recv,
):
    me = lax.axis_index(AXIS)
    side = math.isqrt(n // CORES)
    my_core = lax.rem(me, CORES)
    my_chip = me // CORES
    my_x = lax.rem(my_chip, side)
    my_y = my_chip // side
    cols = [lax.rem(my_x + d, side) for d in range(side)]
    lines = [lax.rem(my_y + d, side) * side for d in range(side)]
    chips = [lines[dy] + cols[dx] for dx, dy in send_order(side)]
    other = me + 1 - 2 * my_core
    n_chips = n // CORES
    _, patches, rows, chans = x_img.shape
    pairs = patches // 2
    hid = w1_hbm.shape[1]
    wide = chans // LANES
    ff = wc1.shape[1]

    def two(j):
        return pl.ds(pl.multiple_of(2 * j, 2), 2)

    def image_rows(chip, p):
        return pl.ds(pl.multiple_of(2 * CORES * chip + 2 * p, 2), 2)

    def settle(counted, sem):
        pltpu.make_async_copy(counted, counted, sem).wait()

    def remote(src, dst, ss, rs, j):
        pltpu.make_async_remote_copy(src_ref=src, dst_ref=dst, send_sem=ss, recv_sem=rs, device_id={AXIS: j}).start()

    def to_twins(src, dst, ss, rs):
        for k in chips:
            remote(src(k), dst, ss, rs, CORES * k + my_core)

    b_all[...] = jnp.zeros_like(b_all)
    weights, mine = [], []
    for i, (w_hbm, w_own, w_all) in enumerate(((w1_hbm, w1_own, w1_all), (w2_hbm, w2_own, w2_all))):
        for q in range(pairs):
            src = w_hbm.at[pl.ds(2 * q, 2), :]
            weights.append(pltpu.make_async_copy(src, w_own.at[q], local_sem.at[i, q]))
            mine.append(pltpu.make_async_copy(src, w_all.at[q, two(my_chip), :], mine_sem.at[i, q]))
    x_load = pltpu.make_async_copy(x_hbm, x_own, chan_sem.at[2])
    biases = [pltpu.make_async_copy(b1_hbm, b1_v, small_sem.at[0]), pltpu.make_async_copy(b2_hbm, b2_v, small_sem.at[1])]
    x_mine = [pltpu.make_async_copy(x_hbm.at[:, image_rows(my_chip, p), :], x_img.at[p, :, two(my_chip), :], chan_sem.at[3 + p]) for p in range(PAIR)]
    smalls = [
        pltpu.make_async_copy(src, dst, small_sem.at[2 + i])
        for i, (src, dst) in enumerate(((g1_hbm, g1), (o1_hbm, o1), (g2_hbm, g2), (o2_hbm, o2), (bc1_hbm, bc1), (bc2_hbm, bc2)))
    ]
    chan_loads = [pltpu.make_async_copy(wc1_hbm, wc1, chan_sem.at[0]), pltpu.make_async_copy(wc2_hbm, wc2, chan_sem.at[1])]
    for c in weights + biases + [x_load]:
        c.start()

    barrier = pltpu.get_barrier_semaphore()
    for j in [CORES * k + my_core for k in chips] + [other]:
        pl.semaphore_signal(barrier, inc=1, device_id={AXIS: j})
    for c in mine + x_mine + smalls + chan_loads:
        c.start()
    b_own[...] = jnp.zeros_like(b_own)
    for c in biases:
        c.wait()
    for i, b_v in enumerate((b1_v, b2_v)):
        b_own[i, :, pl.ds(0, b_v.shape[1])] = jnp.broadcast_to(b_v[...], (2, b_v.shape[1]))
    for c in weights + [x_load]:
        c.wait()
    pl.semaphore_wait(barrier, n_chips)

    to_twins(lambda k: w1_own, w1_all.at[:, two(my_chip), :], w_send.at[0], w_recv.at[0])
    to_twins(lambda k: x_own.at[:, image_rows(k, 0), :], x_img.at[0, :, two(my_chip), :], x_send.at[0], x_recv.at[0])
    to_twins(lambda k: b_own, b_all.at[:, two(my_chip), :], b_send, b_recv)
    to_twins(lambda k: w2_own, w2_all.at[:, two(my_chip), :], w_send.at[1], w_recv.at[1])
    to_twins(lambda k: x_own.at[:, image_rows(k, 1), :], x_img.at[1, :, two(my_chip), :], x_send.at[1], x_recv.at[1])

    for c in mine + x_mine + smalls:
        c.wait()

    even = lax.rem(lax.broadcasted_iota(jnp.int32, (rows, hid), 0), 2) == 0
    keep = (lax.rem(lax.broadcasted_iota(jnp.int32, (rows, 2 * hid), 0), 2) == 0) == (
        lax.broadcasted_iota(jnp.int32, (rows, 2 * hid), 1) < hid
    )

    def expand(w_all, q):
        wq = w_all[q].astype(F32)
        first = jnp.where(even, wq, pltpu.roll(wq, 1, 0))
        second = jnp.where(even, pltpu.roll(wq, rows - 1, 0), wq)
        return [jnp.where(keep, jnp.concatenate([d, d], axis=1), 0.0) for d in (first, second)]

    settle(w_tally, w_recv.at[0])
    q = 0
    while q < pairs:
        group = [q] if q + 1 == pairs else [q, q + 1]
        block = jnp.concatenate([d for g in group for d in expand(w1_all, g)], axis=0)
        w1_t[:, pl.ds(2 * rows * q, block.shape[0])] = jnp.transpose(block).astype(BF16)
        q += len(group)

    def half_sum(p):
        settle(x_tally, x_recv.at[p])
        u = layer_norm(x_img[p].reshape(patches * rows, chans).astype(F32), g1[...], o1[...]).astype(BF16)
        for i in range(PAIR):
            span = pl.ds(hid * i, hid)
            h_mine[p, span, :] = jnp.dot(w1_t[span, :], u, preferred_element_type=F32) + widen(b1_col[...], wide)
            remote(h_mine.at[p, span, :], h_other.at[p, span, :], h_send.at[p, i], h_recv.at[p, i], other)

    def activate(p):
        halves = []
        for i in range(PAIR):
            span = pl.ds(hid * i, hid)
            settle(h_other.at[p, span, :], h_recv.at[p, i])
            halves.append(gelu(h_mine[p, span, :] + h_other[p, span, :]).astype(BF16))
        return jnp.concatenate(halves, axis=0)

    def finish(p, g, at, per):
        m = per * rows
        part = pl.ds(at, per)
        span = pl.ds(at * rows, m)
        tok = jnp.dot(w2_big[span, :], g, preferred_element_type=F32) + widen(b2_col[span, :], wide)
        x_mid = (x_img[p, part].reshape(m, chans).astype(F32) + tok).astype(BF16)
        mid_wide = x_mid.astype(F32)
        v = layer_norm(mid_wide, g2[...], o2[...]).astype(BF16)
        for f in range(ff // ff_tile):
            cols_f = pl.ds(f * ff_tile, ff_tile)
            pre = jnp.dot(v, wc1[:, cols_f], preferred_element_type=F32) + bc1[:, cols_f]
            act[pl.ds(0, m), cols_f] = gelu(pre).astype(BF16)
        ch_out = jnp.dot(act[pl.ds(0, m), :], wc2[...], preferred_element_type=F32) + bc2[...]
        z_img[p, part] = (mid_wide + ch_out).astype(BF16).reshape(per, rows, chans)

    def send_back(p, at, per):
        part = pl.ds(at, per)
        out = pltpu.make_async_copy(z_img.at[p, part, two(my_chip), :], spare.at[p, part], own_sem.at[0])
        out.start()
        to_twins(lambda k: z_img.at[p, part, two(k), :], out_ref.at[part, image_rows(my_chip, p), :], z_send.at[p], z_recv.at[p])
        out.wait()
        back = pltpu.make_async_copy(spare.at[p, part], out_ref.at[part, image_rows(my_chip, p), :], own_sem.at[1])
        back.start()
        return back

    settle(b_tally, b_recv)
    is_mine = lax.broadcasted_iota(jnp.int32, (rows, LANES), 0) // 2 == my_chip
    for i in range(2):
        b_all[i] = jnp.where(is_mine, jnp.broadcast_to(b_own[i, pl.ds(0, 1), :], (rows, LANES)), b_all[i])
    per_chip = hid // n_chips
    picked = b_all[0, pl.ds(0, n_chips, stride=2), :]
    spread = jnp.broadcast_to(picked.reshape(n_chips, 1, LANES), (n_chips, per_chip, LANES))
    place = lax.broadcasted_iota(jnp.int32, spread.shape, 1) - (per_chip // CORES) * my_core
    diag = place == lax.broadcasted_iota(jnp.int32, spread.shape, 2)
    col1 = jnp.broadcast_to(jnp.sum(jnp.where(diag, spread, 0.0), axis=2, keepdims=True), spread.shape)
    b1_col[...] = col1.reshape(hid, LANES)
    tail = b_all[1]
    for s in range(patches):
        b2_col[pl.ds(rows * s, rows), :] = jnp.broadcast_to(tail[:, s : s + 1], (rows, LANES))

    half_sum(0)
    settle(w_tally, w_recv.at[1])
    for q in range(pairs):
        w2_big[pl.ds(2 * rows * q, 2 * rows), :] = jnp.concatenate(expand(w2_all, q), axis=0).astype(BF16)
    for c in chan_loads:
        c.wait()

    back = None
    for p, parts in enumerate((a_parts, b_parts)):
        g = activate(p)
        at = 0
        for t, per in enumerate(parts):
            finish(p, g, at, per)
            if back is not None:
                back.wait()
            back = send_back(p, at, per)
            at += per
            if p == 0 and t == b_after:
                half_sum(1)

    back.wait()
    for p in range(PAIR):
        settle(x_tally, z_recv.at[p])
    for p in range(PAIR):
        settle(x_tally, z_send.at[p])
        settle(x_tally, x_send.at[p])
        settle(w_tally, w_send.at[p])
        for i in range(PAIR):
            settle(h_mine.at[p, pl.ds(hid * i, hid), :], h_send.at[p, i])
    settle(b_tally, b_send)


def solution(mesh, a_split=(1, 1), b_split=(4, 3, 2), b_after=0, ff_tile=512):
    row_spec = P("dp", AXIS, None)
    n = mesh.shape[AXIS]

    def local_layer(x_blk, w1_rows, b1_part, w2_cols, b2_part, w_ch1, b_ch1, w_ch2, b_ch2, ln1_gain, ln1_bias, ln2_gain, ln2_bias):
        x_t = jnp.transpose(x_blk, (1, 0, 2))
        w2_rows = jnp.transpose(w2_cols)
        patches, images, chans = x_t.shape
        n_chips = n // CORES
        rows = 2 * n_chips
        hid = w1_rows.shape[1]
        ff = w_ch1.shape[1]
        a_parts = [patches * w // sum(a_split) for w in a_split]
        b_parts = [patches * w // sum(b_split) for w in b_split]
        m = max(a_parts + b_parts) * rows
        hbm = pl.BlockSpec(memory_space=pltpu.HBM)
        sem = pltpu.SemaphoreType.DMA
        smalls = [v[None, :] for v in (b1_part, b2_part, b_ch1, b_ch2, ln1_gain, ln1_bias, ln2_gain, ln2_bias)]
        b1, b2, bc1, bc2, g1, o1, g2, o2 = smalls
        z_t, _ = pl.pallas_call(
            functools.partial(mixer_kernel, n, a_parts, b_parts, b_after, ff_tile),
            name="mixer",
            out_shape=(pltpu.VMEM(x_t.shape, BF16), pltpu.HBM((PAIR, patches, 2, chans), BF16)),
            in_specs=[hbm] * 13,
            out_specs=(pl.BlockSpec(memory_space=pltpu.VMEM), hbm),
            scratch_shapes=[
                pltpu.VMEM(x_t.shape, BF16),
                pltpu.VMEM((PAIR, patches, rows, chans), BF16),
                pltpu.VMEM((PAIR, patches, rows, chans), BF16),
                pltpu.VMEM((patches // 2, 2, hid), BF16),
                pltpu.VMEM((patches // 2, 2, hid), BF16),
                pltpu.VMEM((patches // 2, rows, hid), BF16),
                pltpu.VMEM((patches // 2, rows, hid), BF16),
                pltpu.VMEM((PAIR * hid, patches * rows), BF16),
                pltpu.VMEM((patches * rows, PAIR * hid), BF16),
                pltpu.VMEM((2, 2, LANES), F32),
                pltpu.VMEM((2, rows, LANES), F32),
                pltpu.VMEM((hid, LANES), F32),
                pltpu.VMEM((patches * rows, LANES), F32),
                pltpu.VMEM((PAIR, PAIR * hid, chans), F32),
                pltpu.VMEM((PAIR, PAIR * hid, chans), F32),
                pltpu.VMEM((m, ff), BF16),
                pltpu.VMEM(w_ch1.shape, BF16),
                pltpu.VMEM(w_ch2.shape, BF16),
                *[pltpu.VMEM(v.shape, F32) for v in smalls],
                pltpu.VMEM((n_chips - 1, patches, 2, chans), BF16),
                pltpu.VMEM((n_chips - 1, patches // 2, 2, hid), BF16),
                pltpu.VMEM((n_chips - 1, 2, 2, LANES), F32),
                sem((2, patches // 2)),
                sem((2, patches // 2)),
                sem((5,)),
                sem((8,)),
                sem((2,)),
                sem((2,)), sem((2,)),
                sem, sem,
                sem((PAIR,)), sem((PAIR,)),
                sem((PAIR, PAIR)), sem((PAIR, PAIR)),
                sem((PAIR,)), sem((PAIR,)),
            ],
            compiler_params=pltpu.CompilerParams(
                collective_id=0, has_side_effects=True, vmem_limit_bytes=VMEM_LIMIT - 2 * math.prod(x_t.shape)
            ),
        )(x_t, w1_rows, w2_rows, b1, b2, w_ch1, bc1, w_ch2, bc2, g1, o1, g2, o2)
        return jnp.transpose(z_t, (1, 0, 2))

    in_specs = (row_spec, P(AXIS, None), P(AXIS), P(None, AXIS), P(AXIS), P(None, None), P(None), P(None, None), P(None), P(None), P(None), P(None), P(None))
    return jax.shard_map(local_layer, mesh=mesh, in_specs=in_specs, out_specs=row_spec, check_vma=False)
```

```python
import functools
import math

import jax
import jax.numpy as jnp
from jax import lax
from jax.experimental import pallas as pl
from jax.experimental.pallas import tpu as pltpu
from jax.sharding import PartitionSpec as P

LN_EPS = 1e-6
AXIS = "sp"
LANES = 128
CORES = 2
PAIR = 2
VMEM_LIMIT = 67043328
BF16 = jnp.bfloat16
F32 = jnp.float32


def layer_norm(values, ln_gain, ln_bias):
    mean_val = jnp.mean(values, axis=-1, keepdims=True)
    centred = values - mean_val
    var_val = jnp.mean(centred * centred, axis=-1, keepdims=True)
    return centred * lax.rsqrt(var_val + LN_EPS) * ln_gain + ln_bias


def gelu(a):
    return 0.5 * a * (1.0 + jnp.tanh(math.sqrt(2.0 / math.pi) * (a + 0.044715 * (a * a * a))))


def widen(column, copies):
    return jnp.concatenate([column] * copies, axis=1)


def send_order(side):
    hops = lambda d: min(d, side - d)
    flows = []
    for dx, dy in sorted(
        ((dx, dy) for dx in range(side) for dy in range(side) if dx or dy),
        key=lambda o: (hops(o[0]) + hops(o[1]), max(hops(o[0]), hops(o[1])), o),
    ):
        for flow in ((dx, dy), ((side - dx) % side, (side - dy) % side)):
            if flow not in flows:
                flows.append(flow)
    return flows[::-1]


def mixer_kernel(
    n, x_parts, z_parts, b_after, ff_tile,
    x_hbm, w1_hbm, w2_hbm, b1_hbm, b2_hbm, wc1_hbm, bc1_hbm, wc2_hbm, bc2_hbm, g1_hbm, o1_hbm, g2_hbm, o2_hbm,
    out_ref, spare,
    x_own, x_img, z_img, w1_own, w2_own, w1_all, w2_all, w1_t, w2_big, b_own, b_all, b1_col, b2_col, h_mine, h_other, u_all, v_part, mid_part, act, wc1, wc2,
    b1_v, b2_v, bc1, bc2, g1, o1, g2, o2, x_tally, w_tally, b_tally,
    local_sem, mine_sem, chan_sem, small_sem, own_sem,
    w_send, w_recv, b_send, b_recv, x_send, x_recv, h_send, h_recv, z_send, z_recv,
):
    me = lax.axis_index(AXIS)
    side = math.isqrt(n // CORES)
    my_core = lax.rem(me, CORES)
    my_chip = me // CORES
    my_x = lax.rem(my_chip, side)
    my_y = my_chip // side
    cols = [lax.rem(my_x + d, side) for d in range(side)]
    lines = [lax.rem(my_y + d, side) * side for d in range(side)]
    chips = [lines[dy] + cols[dx] for dx, dy in send_order(side)]
    other = me + 1 - 2 * my_core
    n_chips = n // CORES
    _, patches, rows, chans = x_img.shape
    pairs = patches // 2
    hid = w1_hbm.shape[1]
    wide = chans // LANES
    ff = wc1.shape[1]

    def two(j):
        return pl.ds(pl.multiple_of(2 * j, 2), 2)

    def image_rows(chip, p):
        return pl.ds(pl.multiple_of(2 * CORES * chip + 2 * p, 2), 2)

    def settle(counted, sem):
        pltpu.make_async_copy(counted, counted, sem).wait()

    def remote(src, dst, ss, rs, j):
        pltpu.make_async_remote_copy(src_ref=src, dst_ref=dst, send_sem=ss, recv_sem=rs, device_id={AXIS: j}).start()

    def to_twins(src, dst, ss, rs):
        for k in chips:
            remote(src(k), dst, ss, rs, CORES * k + my_core)

    b_all[...] = jnp.zeros_like(b_all)
    weights, mine = [], []
    for i, (w_hbm, w_own, w_all) in enumerate(((w1_hbm, w1_own, w1_all), (w2_hbm, w2_own, w2_all))):
        for q in range(pairs):
            src = w_hbm.at[pl.ds(2 * q, 2), :]
            weights.append(pltpu.make_async_copy(src, w_own.at[q], local_sem.at[i, q]))
            mine.append(pltpu.make_async_copy(src, w_all.at[q, two(my_chip), :], mine_sem.at[i, q]))
    x_load = pltpu.make_async_copy(x_hbm, x_own, chan_sem.at[2])
    biases = [pltpu.make_async_copy(b1_hbm, b1_v, small_sem.at[0]), pltpu.make_async_copy(b2_hbm, b2_v, small_sem.at[1])]
    x_mine = [pltpu.make_async_copy(x_hbm.at[:, image_rows(my_chip, p), :], x_img.at[p, :, two(my_chip), :], chan_sem.at[3 + p]) for p in range(PAIR)]
    smalls = [
        pltpu.make_async_copy(src, dst, small_sem.at[2 + i])
        for i, (src, dst) in enumerate(((g1_hbm, g1), (o1_hbm, o1), (g2_hbm, g2), (o2_hbm, o2), (bc1_hbm, bc1), (bc2_hbm, bc2)))
    ]
    chan_loads = [pltpu.make_async_copy(wc1_hbm, wc1, chan_sem.at[0]), pltpu.make_async_copy(wc2_hbm, wc2, chan_sem.at[1])]
    for c in weights + biases + [x_load]:
        c.start()

    barrier = pltpu.get_barrier_semaphore()
    for j in [CORES * k + my_core for k in chips] + [other]:
        pl.semaphore_signal(barrier, inc=1, device_id={AXIS: j})
    for c in mine + x_mine + smalls + chan_loads:
        c.start()
    b_own[...] = jnp.zeros_like(b_own)
    for c in biases:
        c.wait()
    for i, b_v in enumerate((b1_v, b2_v)):
        b_own[i, :, pl.ds(0, b_v.shape[1])] = jnp.broadcast_to(b_v[...], (2, b_v.shape[1]))
    for c in weights + [x_load]:
        c.wait()
    pl.semaphore_wait(barrier, n_chips)

    def send_x(p):
        at = 0
        for t, per in enumerate(x_parts[p]):
            part = pl.ds(at, per)
            to_twins(lambda k: x_own.at[part, image_rows(k, p), :], x_img.at[p, part, two(my_chip), :], x_send.at[p], x_recv.at[p, t])
            at += per

    to_twins(lambda k: w1_own, w1_all.at[:, two(my_chip), :], w_send.at[0], w_recv.at[0])
    to_twins(lambda k: b_own, b_all.at[:, two(my_chip), :], b_send, b_recv)
    send_x(0)
    to_twins(lambda k: w2_own, w2_all.at[:, two(my_chip), :], w_send.at[1], w_recv.at[1])
    send_x(1)

    for c in mine + x_mine + smalls:
        c.wait()

    even = lax.rem(lax.broadcasted_iota(jnp.int32, (rows, hid), 0), 2) == 0
    keep = (lax.rem(lax.broadcasted_iota(jnp.int32, (rows, 2 * hid), 0), 2) == 0) == (
        lax.broadcasted_iota(jnp.int32, (rows, 2 * hid), 1) < hid
    )

    def expand(w_all, q):
        wq = w_all[q].astype(F32)
        first = jnp.where(even, wq, pltpu.roll(wq, 1, 0))
        second = jnp.where(even, pltpu.roll(wq, rows - 1, 0), wq)
        return [jnp.where(keep, jnp.concatenate([d, d], axis=1), 0.0) for d in (first, second)]

    settle(w_tally, w_recv.at[0])
    q = 0
    while q < pairs:
        group = [q] if q + 1 == pairs else [q, q + 1]
        block = jnp.concatenate([d for g in group for d in expand(w1_all, g)], axis=0)
        w1_t[:, pl.ds(2 * rows * q, block.shape[0])] = jnp.transpose(block).astype(BF16)
        q += len(group)

    def half_sum(p):
        at = 0
        for t, per in enumerate(x_parts[p]):
            settle(x_tally.at[:, pl.ds(0, per)], x_recv.at[p, t])
            wide_x = x_img[p, pl.ds(at, per)].reshape(per * rows, chans).astype(F32)
            u_all[pl.ds(at * rows, per * rows), :] = layer_norm(wide_x, g1[...], o1[...]).astype(BF16)
            at += per
        u = u_all[...]
        for i in range(PAIR):
            span = pl.ds(hid * i, hid)
            h_mine[p, span, :] = jnp.dot(w1_t[span, :], u, preferred_element_type=F32) + widen(b1_col[...], wide)
            remote(h_mine.at[p, span, :], h_other.at[p, span, :], h_send.at[p, i], h_recv.at[p, i], other)

    def activate(p):
        halves = []
        for i in range(PAIR):
            span = pl.ds(hid * i, hid)
            settle(h_other.at[p, span, :], h_recv.at[p, i])
            halves.append(gelu(h_mine[p, span, :] + h_other[p, span, :]).astype(BF16))
        return jnp.concatenate(halves, axis=0)

    def prepare(slot, p, g, at, per):
        m = per * rows
        span = pl.ds(at * rows, m)
        tok = jnp.dot(w2_big[span, :], g, preferred_element_type=F32) + widen(b2_col[span, :], wide)
        x_mid = (x_img[p, pl.ds(at, per)].reshape(m, chans).astype(F32) + tok).astype(BF16)
        mid_part[slot, pl.ds(0, m), :] = x_mid
        v_part[slot, pl.ds(0, m), :] = layer_norm(x_mid.astype(F32), g2[...], o2[...]).astype(BF16)

    def expand_channels(slot, per):
        m = pl.ds(0, per * rows)
        v = v_part[slot, m, :]
        for f in range(ff // ff_tile):
            cols_f = pl.ds(f * ff_tile, ff_tile)
            pre = jnp.dot(v, wc1[:, cols_f], preferred_element_type=F32) + bc1[:, cols_f]
            act[m, cols_f] = gelu(pre).astype(BF16)

    def contract_channels(slot, p, at, per):
        m = pl.ds(0, per * rows)
        ch_out = jnp.dot(act[m, :], wc2[...], preferred_element_type=F32) + bc2[...]
        z_img[p, pl.ds(at, per)] = (mid_part[slot, m, :].astype(F32) + ch_out).astype(BF16).reshape(per, rows, chans)

    def own_block(i, p, at, per):
        part = pl.ds(at, per)
        away = pltpu.make_async_copy(z_img.at[p, part, two(my_chip), :], spare.at[p, part], own_sem.at[0, i])
        back = pltpu.make_async_copy(spare.at[p, part], out_ref.at[part, image_rows(my_chip, p), :], own_sem.at[1, i])
        return away, back

    settle(b_tally, b_recv)
    is_mine = lax.broadcasted_iota(jnp.int32, (rows, LANES), 0) // 2 == my_chip
    for i in range(2):
        b_all[i] = jnp.where(is_mine, jnp.broadcast_to(b_own[i, pl.ds(0, 1), :], (rows, LANES)), b_all[i])
    per_chip = hid // n_chips
    picked = b_all[0, pl.ds(0, n_chips, stride=2), :]
    spread = jnp.broadcast_to(picked.reshape(n_chips, 1, LANES), (n_chips, per_chip, LANES))
    place = lax.broadcasted_iota(jnp.int32, spread.shape, 1) - (per_chip // CORES) * my_core
    diag = place == lax.broadcasted_iota(jnp.int32, spread.shape, 2)
    col1 = jnp.broadcast_to(jnp.sum(jnp.where(diag, spread, 0.0), axis=2, keepdims=True), spread.shape)
    b1_col[...] = col1.reshape(hid, LANES)
    tail = b_all[1]
    for s in range(patches):
        b2_col[pl.ds(rows * s, rows), :] = jnp.broadcast_to(tail[:, s : s + 1], (rows, LANES))

    half_sum(0)
    settle(w_tally, w_recv.at[1])
    for q in range(pairs):
        w2_big[pl.ds(2 * rows * q, 2 * rows), :] = jnp.concatenate(expand(w2_all, q), axis=0).astype(BF16)
    for c in chan_loads:
        c.wait()

    steps = [(p, sum(parts[:t]), per) for p, parts in enumerate(z_parts) for t, per in enumerate(parts)]
    g = activate(0)
    prepare(0, 0, g, *steps[0][1:])
    own = []
    for i, (p, at, per) in enumerate(steps):
        slot = i % 2
        part = pl.ds(at, per)
        expand_channels(slot, per)
        if i + 1 < len(steps):
            following = steps[i + 1]
            if following[0] != p:
                g = activate(following[0])
            prepare(1 - slot, following[0], g, *following[1:])
        contract_channels(slot, p, at, per)
        if own:
            own[-1][0].wait()
            own[-1][1].start()
        own.append(own_block(i, p, at, per))
        own[-1][0].start()
        to_twins(lambda k: z_img.at[p, part, two(k), :], out_ref.at[part, image_rows(my_chip, p), :], z_send.at[p], z_recv.at[p])
        if i == b_after:
            half_sum(1)

    own[-1][0].wait()
    own[-1][1].start()
    for _, back in own:
        back.wait()
    for p in range(PAIR):
        settle(x_tally, z_recv.at[p])
    for p in range(PAIR):
        settle(x_tally, z_send.at[p])
        settle(x_tally, x_send.at[p])
        settle(w_tally, w_send.at[p])
        for i in range(PAIR):
            settle(h_mine.at[p, pl.ds(hid * i, hid), :], h_send.at[p, i])
    settle(b_tally, b_send)


def solution(mesh, x_split=((1, 1), (1,)), z_split=((1, 1), (4, 3, 2)), b_after=0, ff_tile=512):
    row_spec = P("dp", AXIS, None)
    n = mesh.shape[AXIS]

    def local_layer(x_blk, w1_rows, b1_part, w2_cols, b2_part, w_ch1, b_ch1, w_ch2, b_ch2, ln1_gain, ln1_bias, ln2_gain, ln2_bias):
        x_t = jnp.transpose(x_blk, (1, 0, 2))
        w2_rows = jnp.transpose(w2_cols)
        patches, images, chans = x_t.shape
        n_chips = n // CORES
        rows = 2 * n_chips
        hid = w1_rows.shape[1]
        ff = w_ch1.shape[1]
        x_parts, z_parts = ([[patches * w // sum(ws) for w in ws] for ws in split] for split in (x_split, z_split))
        m = max(max(parts) for parts in z_parts) * rows
        hbm = pl.BlockSpec(memory_space=pltpu.HBM)
        sem = pltpu.SemaphoreType.DMA
        smalls = [v[None, :] for v in (b1_part, b2_part, b_ch1, b_ch2, ln1_gain, ln1_bias, ln2_gain, ln2_bias)]
        b1, b2, bc1, bc2, g1, o1, g2, o2 = smalls
        z_t, _ = pl.pallas_call(
            functools.partial(mixer_kernel, n, x_parts, z_parts, b_after, ff_tile),
            name="mixer",
            out_shape=(pltpu.VMEM(x_t.shape, BF16), pltpu.HBM((PAIR, patches, 2, chans), BF16)),
            in_specs=[hbm] * 13,
            out_specs=(pl.BlockSpec(memory_space=pltpu.VMEM), hbm),
            scratch_shapes=[
                pltpu.VMEM(x_t.shape, BF16),
                pltpu.VMEM((PAIR, patches, rows, chans), BF16),
                pltpu.VMEM((PAIR, patches, rows, chans), BF16),
                pltpu.VMEM((patches // 2, 2, hid), BF16),
                pltpu.VMEM((patches // 2, 2, hid), BF16),
                pltpu.VMEM((patches // 2, rows, hid), BF16),
                pltpu.VMEM((patches // 2, rows, hid), BF16),
                pltpu.VMEM((PAIR * hid, patches * rows), BF16),
                pltpu.VMEM((patches * rows, PAIR * hid), BF16),
                pltpu.VMEM((2, 2, LANES), F32),
                pltpu.VMEM((2, rows, LANES), F32),
                pltpu.VMEM((hid, LANES), F32),
                pltpu.VMEM((patches * rows, LANES), F32),
                pltpu.VMEM((PAIR, PAIR * hid, chans), F32),
                pltpu.VMEM((PAIR, PAIR * hid, chans), F32),
                pltpu.VMEM((patches * rows, chans), BF16),
                pltpu.VMEM((2, m, chans), BF16),
                pltpu.VMEM((2, m, chans), BF16),
                pltpu.VMEM((m, ff), BF16),
                pltpu.VMEM(w_ch1.shape, BF16),
                pltpu.VMEM(w_ch2.shape, BF16),
                *[pltpu.VMEM(v.shape, F32) for v in smalls],
                pltpu.VMEM((n_chips - 1, patches, 2, chans), BF16),
                pltpu.VMEM((n_chips - 1, patches // 2, 2, hid), BF16),
                pltpu.VMEM((n_chips - 1, 2, 2, LANES), F32),
                sem((2, patches // 2)),
                sem((2, patches // 2)),
                sem((5,)),
                sem((8,)),
                sem((2, sum(len(parts) for parts in z_parts))),
                sem((2,)), sem((2,)),
                sem, sem,
                sem((PAIR,)), sem((PAIR, max(len(parts) for parts in x_parts))),
                sem((PAIR, PAIR)), sem((PAIR, PAIR)),
                sem((PAIR,)), sem((PAIR,)),
            ],
            compiler_params=pltpu.CompilerParams(
                collective_id=0, has_side_effects=True, vmem_limit_bytes=VMEM_LIMIT - 2 * math.prod(x_t.shape)
            ),
        )(x_t, w1_rows, w2_rows, b1, b2, w_ch1, bc1, w_ch2, bc2, g1, o1, g2, o2)
        return jnp.transpose(z_t, (1, 0, 2))

    in_specs = (row_spec, P(AXIS, None), P(AXIS), P(None, AXIS), P(AXIS), P(None, None), P(None), P(None, None), P(None), P(None), P(None), P(None), P(None))
    return jax.shard_map(local_layer, mesh=mesh, in_specs=in_specs, out_specs=row_spec, check_vma=False)
```

```python
import functools
import math

import jax
import jax.numpy as jnp
from jax import lax
from jax.experimental import pallas as pl
from jax.experimental.pallas import tpu as pltpu
from jax.sharding import PartitionSpec as P

LN_EPS = 1e-6
AXIS = "sp"
LANES = 128
CORES = 2
PAIR = 2
VMEM_LIMIT = 67043328
BF16 = jnp.bfloat16
F32 = jnp.float32


def layer_norm(values, ln_gain, ln_bias):
    mean_val = jnp.mean(values, axis=-1, keepdims=True)
    centred = values - mean_val
    var_val = jnp.mean(centred * centred, axis=-1, keepdims=True)
    return centred * lax.rsqrt(var_val + LN_EPS) * ln_gain + ln_bias


def gelu(a):
    return 0.5 * a * (1.0 + jnp.tanh(math.sqrt(2.0 / math.pi) * (a + 0.044715 * (a * a * a))))


def widen(column, copies):
    return jnp.concatenate([column] * copies, axis=1)


def send_order(side):
    hops = lambda d: min(d, side - d)
    flows = []
    for dx, dy in sorted(
        ((dx, dy) for dx in range(side) for dy in range(side) if dx or dy),
        key=lambda o: (hops(o[0]) + hops(o[1]), max(hops(o[0]), hops(o[1])), o),
    ):
        for flow in ((dx, dy), ((side - dx) % side, (side - dy) % side)):
            if flow not in flows:
                flows.append(flow)
    return flows[::-1]


def mixer_kernel(
    n, x_parts, z_parts, b_after, ff_tile,
    x_hbm, w1_hbm, w2_hbm, b1_hbm, b2_hbm, wc1_hbm, bc1_hbm, wc2_hbm, bc2_hbm, g1_hbm, o1_hbm, g2_hbm, o2_hbm,
    out_ref, spare,
    x_own, x_img, z_img, w1_own, w2_own, w1_all, w2_all, w1_t, w2_big, b_own, b_all, b1_col, b2_col, h_mine, h_other, v_part, mid_part, act, wc1, wc2,
    b1_v, b2_v, bc1, bc2, g1, o1, g2, o2, x_tally, w_tally, b_tally,
    local_sem, mine_sem, chan_sem, small_sem, own_sem,
    w_send, w_recv, b_send, b_recv, x_send, x_recv, h_send, h_recv, z_send, z_recv,
):
    me = lax.axis_index(AXIS)
    side = math.isqrt(n // CORES)
    my_core = lax.rem(me, CORES)
    my_chip = me // CORES
    my_x = lax.rem(my_chip, side)
    my_y = my_chip // side
    cols = [lax.rem(my_x + d, side) for d in range(side)]
    lines = [lax.rem(my_y + d, side) * side for d in range(side)]
    chips = [lines[dy] + cols[dx] for dx, dy in send_order(side)]
    row_chips = [lines[0] + cols[dx] for dx, dy in send_order(side) if dy == 0]
    col_chips = [lines[dy] + cols[0] for dx, dy in send_order(side) if dx == 0]
    other = me + 1 - 2 * my_core
    n_chips = n // CORES
    _, patches, rows, chans = x_img.shape
    pairs = patches // 2
    hid = w1_hbm.shape[1]
    wide = chans // LANES
    ff = wc1.shape[1]

    def two(j):
        return pl.ds(pl.multiple_of(2 * j, 2), 2)

    def image_rows(chip, p):
        return pl.ds(pl.multiple_of(2 * CORES * chip + 2 * p, 2), 2)

    def settle(counted, sem):
        pltpu.make_async_copy(counted, counted, sem).wait()

    def remote(src, dst, ss, rs, j):
        pltpu.make_async_remote_copy(src_ref=src, dst_ref=dst, send_sem=ss, recv_sem=rs, device_id={AXIS: j}).start()

    def to_twins(src, dst, ss, rs, targets=chips):
        for k in targets:
            remote(src(k), dst, ss, rs, CORES * k + my_core)

    b_all[...] = jnp.zeros_like(b_all)
    weights, mine = [], []
    for i, (w_hbm, w_own, w_all) in enumerate(((w1_hbm, w1_own, w1_all), (w2_hbm, w2_own, w2_all))):
        for q in range(pairs):
            src = w_hbm.at[pl.ds(2 * q, 2), :]
            weights.append(pltpu.make_async_copy(src, w_own.at[q], local_sem.at[i, q]))
            mine.append(pltpu.make_async_copy(src, w_all.at[q, two(my_chip), :], mine_sem.at[i, q]))
    x_load = pltpu.make_async_copy(x_hbm, x_own, chan_sem.at[2])
    biases = [pltpu.make_async_copy(b1_hbm, b1_v, small_sem.at[0]), pltpu.make_async_copy(b2_hbm, b2_v, small_sem.at[1])]
    x_mine = [pltpu.make_async_copy(x_hbm.at[:, image_rows(my_chip, p), :], x_img.at[p, :, two(my_chip), :], chan_sem.at[3 + p]) for p in range(PAIR)]
    smalls = [
        pltpu.make_async_copy(src, dst, small_sem.at[2 + i])
        for i, (src, dst) in enumerate(((g1_hbm, g1), (o1_hbm, o1), (g2_hbm, g2), (o2_hbm, o2), (bc1_hbm, bc1), (bc2_hbm, bc2)))
    ]
    chan_loads = [pltpu.make_async_copy(wc1_hbm, wc1, chan_sem.at[0]), pltpu.make_async_copy(wc2_hbm, wc2, chan_sem.at[1])]
    for c in weights + biases + [x_load]:
        c.start()

    barrier = pltpu.get_barrier_semaphore()
    for j in [CORES * k + my_core for k in chips] + [other]:
        pl.semaphore_signal(barrier, inc=1, device_id={AXIS: j})
    for c in mine + x_mine + smalls + chan_loads:
        c.start()
    b_own[...] = jnp.zeros_like(b_own)
    for c in biases:
        c.wait()
    for i, b_v in enumerate((b1_v, b2_v)):
        b_own[i, :, pl.ds(0, b_v.shape[1])] = jnp.broadcast_to(b_v[...], (2, b_v.shape[1]))
    for c in weights + [x_load]:
        c.wait()
    pl.semaphore_wait(barrier, n_chips)

    def send_x(p, t):
        part = pl.ds(sum(x_parts[p][:t]), x_parts[p][t])
        to_twins(lambda k: x_own.at[part, image_rows(k, p), :], x_img.at[p, part, two(my_chip), :], x_send.at[p], x_recv.at[p, t])

    to_twins(lambda k: w1_own, w1_all.at[:, two(my_chip), :], w_send.at[0], w_recv.at[0, 0], row_chips)
    to_twins(lambda k: w2_own, w2_all.at[:, two(my_chip), :], w_send.at[1], w_recv.at[1, 0], col_chips)
    to_twins(lambda k: b_own, b_all.at[:, two(my_chip), :], b_send, b_recv)
    send_x(0, 0)
    for c in mine + x_mine + smalls:
        c.wait()
    near = w_tally.at[pl.ds(0, side - 1)]
    far = w_tally.at[pl.ds(0, side * (side - 1))]
    line = w1_all.at[:, pl.ds(pl.multiple_of(2 * side * my_y, 2 * side), 2 * side), :]
    settle(near, w_recv.at[0, 0])
    to_twins(lambda k: line, line, w_send.at[0], w_recv.at[0, 1], col_chips)
    settle(near, w_recv.at[1, 0])
    for c in [my_chip] + col_chips:
        block = w2_all.at[:, two(c), :]
        to_twins(lambda k: block, block, w_send.at[1], w_recv.at[1, 1], row_chips)
    for t in range(1, len(x_parts[0])):
        send_x(0, t)
    for t in range(len(x_parts[1])):
        send_x(1, t)

    even = lax.rem(lax.broadcasted_iota(jnp.int32, (rows, hid), 0), 2) == 0
    keep = (lax.rem(lax.broadcasted_iota(jnp.int32, (rows, 2 * hid), 0), 2) == 0) == (
        lax.broadcasted_iota(jnp.int32, (rows, 2 * hid), 1) < hid
    )

    def expand(w_all, q):
        wq = w_all[q].astype(F32)
        first = jnp.where(even, wq, pltpu.roll(wq, 1, 0))
        second = jnp.where(even, pltpu.roll(wq, rows - 1, 0), wq)
        return [jnp.where(keep, jnp.concatenate([d, d], axis=1), 0.0) for d in (first, second)]

    settle(far, w_recv.at[0, 1])
    q = 0
    while q < pairs:
        group = [q] if q + 1 == pairs else [q, q + 1]
        block = jnp.concatenate([d for g in group for d in expand(w1_all, g)], axis=0)
        w1_t[:, pl.ds(2 * rows * q, block.shape[0])] = jnp.transpose(block).astype(BF16)
        q += len(group)

    def half_sum(p):
        at = 0
        for t, per in enumerate(x_parts[p]):
            settle(x_tally.at[:, pl.ds(0, per)], x_recv.at[p, t])
            wide_x = x_img[p, pl.ds(at, per)].reshape(per * rows, chans).astype(F32)
            u = layer_norm(wide_x, g1[...], o1[...]).astype(BF16)
            for i in range(PAIR):
                span = pl.ds(hid * i, hid)
                before = h_mine[p, span, :] if t else widen(b1_col[...], wide)
                h_mine[p, span, :] = before + jnp.dot(w1_t[span, pl.ds(at * rows, per * rows)], u, preferred_element_type=F32)
                if t == len(x_parts[p]) - 1:
                    remote(h_mine.at[p, span, :], h_other.at[p, span, :], h_send.at[p, i], h_recv.at[p, i], other)
            at += per

    def activate(p):
        halves = []
        for i in range(PAIR):
            span = pl.ds(hid * i, hid)
            settle(h_other.at[p, span, :], h_recv.at[p, i])
            halves.append(gelu(h_mine[p, span, :] + h_other[p, span, :]).astype(BF16))
        return jnp.concatenate(halves, axis=0)

    def prepare(slot, p, g, at, per):
        m = per * rows
        span = pl.ds(at * rows, m)
        tok = jnp.dot(w2_big[span, :], g, preferred_element_type=F32) + widen(b2_col[span, :], wide)
        x_mid = (x_img[p, pl.ds(at, per)].reshape(m, chans).astype(F32) + tok).astype(BF16)
        mid_part[slot, pl.ds(0, m), :] = x_mid
        v_part[slot, pl.ds(0, m), :] = layer_norm(x_mid.astype(F32), g2[...], o2[...]).astype(BF16)

    def expand_channels(slot, per):
        m = pl.ds(0, per * rows)
        v = v_part[slot, m, :]
        for f in range(ff // ff_tile):
            cols_f = pl.ds(f * ff_tile, ff_tile)
            pre = jnp.dot(v, wc1[:, cols_f], preferred_element_type=F32) + bc1[:, cols_f]
            act[m, cols_f] = gelu(pre).astype(BF16)

    def contract_channels(slot, p, at, per):
        m = pl.ds(0, per * rows)
        ch_out = jnp.dot(act[m, :], wc2[...], preferred_element_type=F32) + bc2[...]
        z_img[p, pl.ds(at, per)] = (mid_part[slot, m, :].astype(F32) + ch_out).astype(BF16).reshape(per, rows, chans)

    def own_block(i, p, at, per):
        part = pl.ds(at, per)
        away = pltpu.make_async_copy(z_img.at[p, part, two(my_chip), :], spare.at[p, part], own_sem.at[0, i])
        back = pltpu.make_async_copy(spare.at[p, part], out_ref.at[part, image_rows(my_chip, p), :], own_sem.at[1, i])
        return away, back

    settle(b_tally, b_recv)
    is_mine = lax.broadcasted_iota(jnp.int32, (rows, LANES), 0) // 2 == my_chip
    for i in range(2):
        b_all[i] = jnp.where(is_mine, jnp.broadcast_to(b_own[i, pl.ds(0, 1), :], (rows, LANES)), b_all[i])
    per_chip = hid // n_chips
    picked = b_all[0, pl.ds(0, n_chips, stride=2), :]
    spread = jnp.broadcast_to(picked.reshape(n_chips, 1, LANES), (n_chips, per_chip, LANES))
    place = lax.broadcasted_iota(jnp.int32, spread.shape, 1) - (per_chip // CORES) * my_core
    diag = place == lax.broadcasted_iota(jnp.int32, spread.shape, 2)
    col1 = jnp.broadcast_to(jnp.sum(jnp.where(diag, spread, 0.0), axis=2, keepdims=True), spread.shape)
    b1_col[...] = col1.reshape(hid, LANES)
    tail = b_all[1]
    for s in range(patches):
        b2_col[pl.ds(rows * s, rows), :] = jnp.broadcast_to(tail[:, s : s + 1], (rows, LANES))

    settle(far, w_recv.at[1, 1])
    for q in range(pairs):
        w2_big[pl.ds(2 * rows * q, 2 * rows), :] = jnp.concatenate(expand(w2_all, q), axis=0).astype(BF16)
    half_sum(0)
    for c in chan_loads:
        c.wait()

    steps = [(p, sum(parts[:t]), per) for p, parts in enumerate(z_parts) for t, per in enumerate(parts)]
    g = activate(0)
    prepare(0, 0, g, *steps[0][1:])
    own = []
    for i, (p, at, per) in enumerate(steps):
        slot = i % 2
        part = pl.ds(at, per)
        expand_channels(slot, per)
        following = steps[i + 1] if i + 1 < len(steps) else None
        if following and i:
            if following[0] != p:
                g = activate(following[0])
            prepare(1 - slot, following[0], g, *following[1:])
        contract_channels(slot, p, at, per)
        if own:
            own[-1][0].wait()
            own[-1][1].start()
        own.append(own_block(i, p, at, per))
        own[-1][0].start()
        to_twins(lambda k: z_img.at[p, part, two(k), :], out_ref.at[part, image_rows(my_chip, p), :], z_send.at[p], z_recv.at[p])
        if i == 0:
            prepare(1 - slot, p, g, *following[1:])
        if i == b_after:
            half_sum(1)

    own[-1][0].wait()
    own[-1][1].start()
    for _, back in own:
        back.wait()
    for p in range(PAIR):
        settle(x_tally, z_recv.at[p])
    for p in range(PAIR):
        settle(x_tally, z_send.at[p])
        settle(x_tally, x_send.at[p])
        settle(w_tally, w_send.at[p])
        for i in range(PAIR):
            settle(h_mine.at[p, pl.ds(hid * i, hid), :], h_send.at[p, i])
    settle(b_tally, b_send)


def solution(mesh, x_split=((1, 1), (1,)), z_split=((1, 2, 3), (4, 3, 2)), b_after=1, ff_tile=512):
    row_spec = P("dp", AXIS, None)
    n = mesh.shape[AXIS]

    def local_layer(x_blk, w1_rows, b1_part, w2_cols, b2_part, w_ch1, b_ch1, w_ch2, b_ch2, ln1_gain, ln1_bias, ln2_gain, ln2_bias):
        x_t = jnp.transpose(x_blk, (1, 0, 2))
        w2_rows = jnp.transpose(w2_cols)
        patches, images, chans = x_t.shape
        n_chips = n // CORES
        rows = 2 * n_chips
        hid = w1_rows.shape[1]
        ff = w_ch1.shape[1]
        x_parts, z_parts = ([[patches * w // sum(ws) for w in ws] for ws in split] for split in (x_split, z_split))
        m = max(max(parts) for parts in z_parts) * rows
        hbm = pl.BlockSpec(memory_space=pltpu.HBM)
        sem = pltpu.SemaphoreType.DMA
        smalls = [v[None, :] for v in (b1_part, b2_part, b_ch1, b_ch2, ln1_gain, ln1_bias, ln2_gain, ln2_bias)]
        b1, b2, bc1, bc2, g1, o1, g2, o2 = smalls
        z_t, _ = pl.pallas_call(
            functools.partial(mixer_kernel, n, x_parts, z_parts, b_after, ff_tile),
            name="mixer",
            out_shape=(pltpu.VMEM(x_t.shape, BF16), pltpu.HBM((PAIR, patches, 2, chans), BF16)),
            in_specs=[hbm] * 13,
            out_specs=(pl.BlockSpec(memory_space=pltpu.VMEM), hbm),
            scratch_shapes=[
                pltpu.VMEM(x_t.shape, BF16),
                pltpu.VMEM((PAIR, patches, rows, chans), BF16),
                pltpu.VMEM((PAIR, patches, rows, chans), BF16),
                pltpu.VMEM((patches // 2, 2, hid), BF16),
                pltpu.VMEM((patches // 2, 2, hid), BF16),
                pltpu.VMEM((patches // 2, rows, hid), BF16),
                pltpu.VMEM((patches // 2, rows, hid), BF16),
                pltpu.VMEM((PAIR * hid, patches * rows), BF16),
                pltpu.VMEM((patches * rows, PAIR * hid), BF16),
                pltpu.VMEM((2, 2, LANES), F32),
                pltpu.VMEM((2, rows, LANES), F32),
                pltpu.VMEM((hid, LANES), F32),
                pltpu.VMEM((patches * rows, LANES), F32),
                pltpu.VMEM((PAIR, PAIR * hid, chans), F32),
                pltpu.VMEM((PAIR, PAIR * hid, chans), F32),
                pltpu.VMEM((2, m, chans), BF16),
                pltpu.VMEM((2, m, chans), BF16),
                pltpu.VMEM((m, ff), BF16),
                pltpu.VMEM(w_ch1.shape, BF16),
                pltpu.VMEM(w_ch2.shape, BF16),
                *[pltpu.VMEM(v.shape, F32) for v in smalls],
                pltpu.VMEM((n_chips - 1, patches, 2, chans), BF16),
                pltpu.VMEM((n_chips - 1, patches // 2, 2, hid), BF16),
                pltpu.VMEM((n_chips - 1, 2, 2, LANES), F32),
                sem((2, patches // 2)),
                sem((2, patches // 2)),
                sem((5,)),
                sem((8,)),
                sem((2, sum(len(parts) for parts in z_parts))),
                sem((2,)), sem((2, 2)),
                sem, sem,
                sem((PAIR,)), sem((PAIR, max(len(parts) for parts in x_parts))),
                sem((PAIR, PAIR)), sem((PAIR, PAIR)),
                sem((PAIR,)), sem((PAIR,)),
            ],
            compiler_params=pltpu.CompilerParams(
                collective_id=0, has_side_effects=True, vmem_limit_bytes=VMEM_LIMIT - 2 * math.prod(x_t.shape)
            ),
        )(x_t, w1_rows, w2_rows, b1, b2, w_ch1, bc1, w_ch2, bc2, g1, o1, g2, o2)
        return jnp.transpose(z_t, (1, 0, 2))

    in_specs = (row_spec, P(AXIS, None), P(AXIS), P(None, AXIS), P(AXIS), P(None, None), P(None), P(None, None), P(None), P(None), P(None), P(None), P(None))
    return jax.shard_map(local_layer, mesh=mesh, in_specs=in_specs, out_specs=row_spec, check_vma=False)
```

```python
import functools
import math

import jax
import jax.numpy as jnp
from jax import lax
from jax.experimental import pallas as pl
from jax.experimental.pallas import tpu as pltpu
from jax.sharding import PartitionSpec as P

LN_EPS = 1e-6
AXIS = "sp"
LANES = 128
CORES = 2
PAIR = 2
SWAPS = 4
VMEM_LIMIT = 67043328
BF16 = jnp.bfloat16
F32 = jnp.float32


def layer_norm(values, ln_gain, ln_bias):
    mean_val = jnp.mean(values, axis=-1, keepdims=True)
    centred = values - mean_val
    var_val = jnp.mean(centred * centred, axis=-1, keepdims=True)
    return centred * lax.rsqrt(var_val + LN_EPS) * ln_gain + ln_bias


def gelu(a):
    return 0.5 * a * (1.0 + jnp.tanh(math.sqrt(2.0 / math.pi) * (a + 0.044715 * (a * a * a))))


def widen(column, copies):
    return jnp.concatenate([column] * copies, axis=1)


def send_order(side):
    hops = lambda d: min(d, side - d)
    flows = []
    for dx, dy in sorted(
        ((dx, dy) for dx in range(side) for dy in range(side) if dx or dy),
        key=lambda o: (hops(o[0]) + hops(o[1]), max(hops(o[0]), hops(o[1])), o),
    ):
        for flow in ((dx, dy), ((side - dx) % side, (side - dy) % side)):
            if flow not in flows:
                flows.append(flow)
    return flows[::-1]


def mixer_kernel(
    n, x_parts, z_parts, b_after, ff_tile,
    x_hbm, w1_hbm, w2_hbm, b1_hbm, b2_hbm, wc1_hbm, bc1_hbm, wc2_hbm, bc2_hbm, g1_hbm, o1_hbm, g2_hbm, o2_hbm,
    out_ref, spare,
    x_own, x_img, z_img, w1_own, w2_own, w1_all, w2_all, w1_t, w2_big, b_own, b_all, b1_col, b2_col, h_mine, h_other, v_part, mid_part, act, wc1, wc2,
    b1_v, b2_v, bc1, bc2, g1, o1, g2, o2, x_tally, w_tally, b_tally,
    local_sem, mine_sem, chan_sem, small_sem, own_sem,
    w_send, w_recv, b_send, b_recv, x_send, x_recv, h_send, h_recv, z_send, z_recv,
):
    me = lax.axis_index(AXIS)
    side = math.isqrt(n // CORES)
    my_core = lax.rem(me, CORES)
    my_chip = me // CORES
    my_x = lax.rem(my_chip, side)
    my_y = my_chip // side
    cols = [lax.rem(my_x + d, side) for d in range(side)]
    lines = [lax.rem(my_y + d, side) * side for d in range(side)]
    chips = [lines[dy] + cols[dx] for dx, dy in send_order(side)]
    row_chips = [lines[0] + cols[dx] for dx, dy in send_order(side) if dy == 0]
    col_chips = [lines[dy] + cols[0] for dx, dy in send_order(side) if dx == 0]
    other = me + 1 - 2 * my_core
    n_chips = n // CORES
    _, patches, rows, chans = x_img.shape
    pairs = patches // 2
    hid = w1_hbm.shape[1]
    wide = chans // LANES
    ff = wc1.shape[1]
    piece = PAIR * hid // SWAPS

    def two(j):
        return pl.ds(pl.multiple_of(2 * j, 2), 2)

    def image_rows(chip, p):
        return pl.ds(pl.multiple_of(2 * CORES * chip + 2 * p, 2), 2)

    def settle(counted, sem):
        pltpu.make_async_copy(counted, counted, sem).wait()

    def remote(src, dst, ss, rs, j):
        pltpu.make_async_remote_copy(src_ref=src, dst_ref=dst, send_sem=ss, recv_sem=rs, device_id={AXIS: j}).start()

    def to_twins(src, dst, ss, rs, targets=chips):
        for k in targets:
            remote(src(k), dst, ss, rs, CORES * k + my_core)

    b_all[...] = jnp.zeros_like(b_all)

    barrier = pltpu.get_barrier_semaphore()
    for j in [CORES * k + my_core for k in chips] + [other]:
        pl.semaphore_signal(barrier, inc=1, device_id={AXIS: j})

    weights, mine = [], []
    for i, (w_hbm, w_own, w_all) in enumerate(((w1_hbm, w1_own, w1_all), (w2_hbm, w2_own, w2_all))):
        for q in range(pairs):
            src = w_hbm.at[pl.ds(2 * q, 2), :]
            weights.append(pltpu.make_async_copy(src, w_own.at[q], local_sem.at[i, q]))
            mine.append(pltpu.make_async_copy(src, w_all.at[q, two(my_chip), :], mine_sem.at[i, q]))
    x_load = pltpu.make_async_copy(x_hbm, x_own, chan_sem.at[2])
    biases = [pltpu.make_async_copy(b1_hbm, b1_v, small_sem.at[0]), pltpu.make_async_copy(b2_hbm, b2_v, small_sem.at[1])]
    x_mine = [pltpu.make_async_copy(x_hbm.at[:, image_rows(my_chip, p), :], x_img.at[p, :, two(my_chip), :], chan_sem.at[3 + p]) for p in range(PAIR)]
    smalls = [
        pltpu.make_async_copy(src, dst, small_sem.at[2 + i])
        for i, (src, dst) in enumerate(((g1_hbm, g1), (o1_hbm, o1), (g2_hbm, g2), (o2_hbm, o2), (bc1_hbm, bc1), (bc2_hbm, bc2)))
    ]
    chan_loads = [pltpu.make_async_copy(wc1_hbm, wc1, chan_sem.at[0]), pltpu.make_async_copy(wc2_hbm, wc2, chan_sem.at[1])]
    for c in weights + biases + [x_load] + mine + x_mine + smalls + chan_loads:
        c.start()
    b_own[...] = jnp.zeros_like(b_own)
    for c in biases:
        c.wait()
    for i, b_v in enumerate((b1_v, b2_v)):
        b_own[i, :, pl.ds(0, b_v.shape[1])] = jnp.broadcast_to(b_v[...], (2, b_v.shape[1]))
    for c in weights + [x_load]:
        c.wait()
    pl.semaphore_wait(barrier, n_chips)

    def send_x(p, t):
        part = pl.ds(sum(x_parts[p][:t]), x_parts[p][t])
        to_twins(lambda k: x_own.at[part, image_rows(k, p), :], x_img.at[p, part, two(my_chip), :], x_send.at[p], x_recv.at[p, t])

    to_twins(lambda k: w1_own, w1_all.at[:, two(my_chip), :], w_send.at[0], w_recv.at[0, 0], row_chips)
    to_twins(lambda k: w2_own, w2_all.at[:, two(my_chip), :], w_send.at[1], w_recv.at[1, 0], col_chips)
    to_twins(lambda k: b_own, b_all.at[:, two(my_chip), :], b_send, b_recv)
    send_x(0, 0)
    for c in mine + x_mine + smalls:
        c.wait()
    near = w_tally.at[pl.ds(0, side - 1)]
    far = w_tally.at[pl.ds(0, side * (side - 1))]
    line = w1_all.at[:, pl.ds(pl.multiple_of(2 * side * my_y, 2 * side), 2 * side), :]
    settle(near, w_recv.at[0, 0])
    to_twins(lambda k: line, line, w_send.at[0], w_recv.at[0, 1], col_chips)
    for t in range(1, len(x_parts[0])):
        send_x(0, t)
    settle(near, w_recv.at[1, 0])
    for c in [my_chip] + col_chips:
        block = w2_all.at[:, two(c), :]
        to_twins(lambda k: block, block, w_send.at[1], w_recv.at[1, 1], row_chips)
    for t in range(len(x_parts[1])):
        send_x(1, t)

    even = lax.rem(lax.broadcasted_iota(jnp.int32, (rows, hid), 0), 2) == 0
    keep = (lax.rem(lax.broadcasted_iota(jnp.int32, (rows, 2 * hid), 0), 2) == 0) == (
        lax.broadcasted_iota(jnp.int32, (rows, 2 * hid), 1) < hid
    )

    def expand(w_all, q):
        wq = w_all[q].astype(F32)
        first = jnp.where(even, wq, pltpu.roll(wq, 1, 0))
        second = jnp.where(even, pltpu.roll(wq, rows - 1, 0), wq)
        return [jnp.where(keep, jnp.concatenate([d, d], axis=1), 0.0) for d in (first, second)]

    settle(far, w_recv.at[0, 1])
    q = 0
    while q < pairs:
        group = [q] if q + 1 == pairs else [q, q + 1]
        block = jnp.concatenate([d for g in group for d in expand(w1_all, g)], axis=0)
        w1_t[:, pl.ds(2 * rows * q, block.shape[0])] = jnp.transpose(block).astype(BF16)
        q += len(group)

    def half_sum(p):
        at = 0
        for t, per in enumerate(x_parts[p]):
            settle(x_tally.at[:, pl.ds(0, per)], x_recv.at[p, t])
            wide_x = x_img[p, pl.ds(at, per)].reshape(per * rows, chans).astype(F32)
            u = layer_norm(wide_x, g1[...], o1[...]).astype(BF16)
            for i in range(SWAPS):
                span = pl.ds(piece * i, piece)
                before = h_mine[p, span, :] if t else widen(b1_col[pl.ds(piece * i % hid, piece), :], wide)
                h_mine[p, span, :] = before + jnp.dot(w1_t[span, pl.ds(at * rows, per * rows)], u, preferred_element_type=F32)
                if t == len(x_parts[p]) - 1:
                    remote(h_mine.at[p, span, :], h_other.at[p, span, :], h_send.at[p, i], h_recv.at[p, i], other)
            at += per

    def activate(p):
        halves = []
        for i in range(SWAPS):
            span = pl.ds(piece * i, piece)
            settle(h_other.at[p, span, :], h_recv.at[p, i])
            halves.append(gelu(h_mine[p, span, :] + h_other[p, span, :]).astype(BF16))
        return jnp.concatenate(halves, axis=0)

    def prepare(slot, p, g, at, per):
        m = per * rows
        span = pl.ds(at * rows, m)
        tok = jnp.dot(w2_big[span, :], g, preferred_element_type=F32) + widen(b2_col[span, :], wide)
        x_mid = (x_img[p, pl.ds(at, per)].reshape(m, chans).astype(F32) + tok).astype(BF16)
        mid_part[slot, pl.ds(0, m), :] = x_mid
        v_part[slot, pl.ds(0, m), :] = layer_norm(x_mid.astype(F32), g2[...], o2[...]).astype(BF16)

    def expand_channels(slot, per):
        m = pl.ds(0, per * rows)
        v = v_part[slot, m, :]
        for f in range(ff // ff_tile):
            cols_f = pl.ds(f * ff_tile, ff_tile)
            pre = jnp.dot(v, wc1[:, cols_f], preferred_element_type=F32) + bc1[:, cols_f]
            act[m, cols_f] = gelu(pre).astype(BF16)

    def contract_channels(slot, p, at, per):
        m = pl.ds(0, per * rows)
        ch_out = jnp.dot(act[m, :], wc2[...], preferred_element_type=F32) + bc2[...]
        z_img[p, pl.ds(at, per)] = (mid_part[slot, m, :].astype(F32) + ch_out).astype(BF16).reshape(per, rows, chans)

    def own_block(i, p, at, per):
        part = pl.ds(at, per)
        away = pltpu.make_async_copy(z_img.at[p, part, two(my_chip), :], spare.at[p, part], own_sem.at[0, i])
        back = pltpu.make_async_copy(spare.at[p, part], out_ref.at[part, image_rows(my_chip, p), :], own_sem.at[1, i])
        return away, back

    settle(b_tally, b_recv)
    is_mine = lax.broadcasted_iota(jnp.int32, (rows, LANES), 0) // 2 == my_chip
    for i in range(2):
        b_all[i] = jnp.where(is_mine, jnp.broadcast_to(b_own[i, pl.ds(0, 1), :], (rows, LANES)), b_all[i])
    per_chip = hid // n_chips
    picked = b_all[0, pl.ds(0, n_chips, stride=2), :]
    spread = jnp.broadcast_to(picked.reshape(n_chips, 1, LANES), (n_chips, per_chip, LANES))
    place = lax.broadcasted_iota(jnp.int32, spread.shape, 1) - (per_chip // CORES) * my_core
    diag = place == lax.broadcasted_iota(jnp.int32, spread.shape, 2)
    col1 = jnp.broadcast_to(jnp.sum(jnp.where(diag, spread, 0.0), axis=2, keepdims=True), spread.shape)
    b1_col[...] = col1.reshape(hid, LANES)
    tail = b_all[1]
    for s in range(patches):
        b2_col[pl.ds(rows * s, rows), :] = jnp.broadcast_to(tail[:, s : s + 1], (rows, LANES))

    half_sum(0)
    settle(far, w_recv.at[1, 1])
    for q in range(pairs):
        w2_big[pl.ds(2 * rows * q, 2 * rows), :] = jnp.concatenate(expand(w2_all, q), axis=0).astype(BF16)
    for c in chan_loads:
        c.wait()

    steps = [(p, sum(parts[:t]), per) for p, parts in enumerate(z_parts) for t, per in enumerate(parts)]
    g = activate(0)
    prepare(0, 0, g, *steps[0][1:])
    own = []
    for i, (p, at, per) in enumerate(steps):
        slot = i % 2
        part = pl.ds(at, per)
        expand_channels(slot, per)
        following = steps[i + 1] if i + 1 < len(steps) else None
        if following and i:
            if following[0] != p:
                g = activate(following[0])
            prepare(1 - slot, following[0], g, *following[1:])
        contract_channels(slot, p, at, per)
        if own:
            own[-1][0].wait()
            own[-1][1].start()
        own.append(own_block(i, p, at, per))
        own[-1][0].start()
        to_twins(lambda k: z_img.at[p, part, two(k), :], out_ref.at[part, image_rows(my_chip, p), :], z_send.at[p], z_recv.at[p])
        if i == 0:
            prepare(1 - slot, p, g, *following[1:])
        if i == b_after:
            half_sum(1)

    own[-1][0].wait()
    own[-1][1].start()
    for _, back in own:
        back.wait()
    for p in range(PAIR):
        settle(x_tally, z_recv.at[p])
    for p in range(PAIR):
        settle(x_tally, z_send.at[p])
        settle(x_tally, x_send.at[p])
        settle(w_tally, w_send.at[p])
        for i in range(SWAPS):
            settle(h_mine.at[p, pl.ds(piece * i, piece), :], h_send.at[p, i])
    settle(b_tally, b_send)


def solution(mesh, x_split=((4, 3, 2), (1,)), z_split=((2, 1), (4, 3, 2)), b_after=0, ff_tile=512):
    row_spec = P("dp", AXIS, None)
    n = mesh.shape[AXIS]

    def local_layer(x_blk, w1_rows, b1_part, w2_cols, b2_part, w_ch1, b_ch1, w_ch2, b_ch2, ln1_gain, ln1_bias, ln2_gain, ln2_bias):
        x_t = jnp.transpose(x_blk, (1, 0, 2))
        w2_rows = jnp.transpose(w2_cols)
        patches, images, chans = x_t.shape
        n_chips = n // CORES
        rows = 2 * n_chips
        hid = w1_rows.shape[1]
        ff = w_ch1.shape[1]
        x_parts, z_parts = ([[patches * w // sum(ws) for w in ws] for ws in split] for split in (x_split, z_split))
        m = max(max(parts) for parts in z_parts) * rows
        hbm = pl.BlockSpec(memory_space=pltpu.HBM)
        sem = pltpu.SemaphoreType.DMA
        smalls = [v[None, :] for v in (b1_part, b2_part, b_ch1, b_ch2, ln1_gain, ln1_bias, ln2_gain, ln2_bias)]
        b1, b2, bc1, bc2, g1, o1, g2, o2 = smalls
        z_t, _ = pl.pallas_call(
            functools.partial(mixer_kernel, n, x_parts, z_parts, b_after, ff_tile),
            name="mixer",
            out_shape=(pltpu.VMEM(x_t.shape, BF16), pltpu.HBM((PAIR, patches, 2, chans), BF16)),
            in_specs=[hbm] * 13,
            out_specs=(pl.BlockSpec(memory_space=pltpu.VMEM), hbm),
            scratch_shapes=[
                pltpu.VMEM(x_t.shape, BF16),
                pltpu.VMEM((PAIR, patches, rows, chans), BF16),
                pltpu.VMEM((PAIR, patches, rows, chans), BF16),
                pltpu.VMEM((patches // 2, 2, hid), BF16),
                pltpu.VMEM((patches // 2, 2, hid), BF16),
                pltpu.VMEM((patches // 2, rows, hid), BF16),
                pltpu.VMEM((patches // 2, rows, hid), BF16),
                pltpu.VMEM((PAIR * hid, patches * rows), BF16),
                pltpu.VMEM((patches * rows, PAIR * hid), BF16),
                pltpu.VMEM((2, 2, LANES), F32),
                pltpu.VMEM((2, rows, LANES), F32),
                pltpu.VMEM((hid, LANES), F32),
                pltpu.VMEM((patches * rows, LANES), F32),
                pltpu.VMEM((PAIR, PAIR * hid, chans), F32),
                pltpu.VMEM((PAIR, PAIR * hid, chans), F32),
                pltpu.VMEM((2, m, chans), BF16),
                pltpu.VMEM((2, m, chans), BF16),
                pltpu.VMEM((m, ff), BF16),
                pltpu.VMEM(w_ch1.shape, BF16),
                pltpu.VMEM(w_ch2.shape, BF16),
                *[pltpu.VMEM(v.shape, F32) for v in smalls],
                pltpu.VMEM((n_chips - 1, patches, 2, chans), BF16),
                pltpu.VMEM((n_chips - 1, patches // 2, 2, hid), BF16),
                pltpu.VMEM((n_chips - 1, 2, 2, LANES), F32),
                sem((2, patches // 2)),
                sem((2, patches // 2)),
                sem((5,)),
                sem((8,)),
                sem((2, sum(len(parts) for parts in z_parts))),
                sem((2,)), sem((2, 2)),
                sem, sem,
                sem((PAIR,)), sem((PAIR, max(len(parts) for parts in x_parts))),
                sem((PAIR, SWAPS)), sem((PAIR, SWAPS)),
                sem((PAIR,)), sem((PAIR,)),
            ],
            compiler_params=pltpu.CompilerParams(
                collective_id=0, has_side_effects=True, vmem_limit_bytes=VMEM_LIMIT - 2 * math.prod(x_t.shape)
            ),
        )(x_t, w1_rows, w2_rows, b1, b2, w_ch1, bc1, w_ch2, bc2, g1, o1, g2, o2)
        return jnp.transpose(z_t, (1, 0, 2))

    in_specs = (row_spec, P(AXIS, None), P(AXIS), P(None, AXIS), P(AXIS), P(None, None), P(None), P(None, None), P(None), P(None), P(None), P(None), P(None))
    return jax.shard_map(local_layer, mesh=mesh, in_specs=in_specs, out_specs=row_spec, check_vma=False)
```

```python
import functools
import math

import jax
import jax.numpy as jnp
from jax import lax
from jax.experimental import pallas as pl
from jax.experimental.pallas import tpu as pltpu
from jax.sharding import PartitionSpec as P

LN_EPS = 1e-6
AXIS = "sp"
LANES = 128
CORES = 2
PAIR = 2
SWAPS = 4
VMEM_LIMIT = 67043328
BF16 = jnp.bfloat16
F32 = jnp.float32


def layer_norm(values, ln_gain, ln_bias):
    mean_val = jnp.mean(values, axis=-1, keepdims=True)
    centred = values - mean_val
    var_val = jnp.mean(centred * centred, axis=-1, keepdims=True)
    return centred * lax.rsqrt(var_val + LN_EPS) * ln_gain + ln_bias


def gelu(a):
    scale = math.sqrt(2.0 / math.pi)
    half = 0.5 * a
    return half + half * jnp.tanh(a * (scale + (scale * 0.044715) * (a * a)))


def widen(column, copies):
    return jnp.concatenate([column] * copies, axis=1)


def send_order(side):
    hops = lambda d: min(d, side - d)
    flows = []
    for dx, dy in sorted(
        ((dx, dy) for dx in range(side) for dy in range(side) if dx or dy),
        key=lambda o: (hops(o[0]) + hops(o[1]), max(hops(o[0]), hops(o[1])), o),
    ):
        for flow in ((dx, dy), ((side - dx) % side, (side - dy) % side)):
            if flow not in flows:
                flows.append(flow)
    return flows[::-1]


def mixer_kernel(
    n, x_parts, z_parts, b_after, ff_tile,
    x_hbm, w1_hbm, w2_hbm, b1_hbm, b2_hbm, wc1_hbm, bc1_hbm, wc2_hbm, bc2_hbm, g1_hbm, o1_hbm, g2_hbm, o2_hbm,
    out_ref, spare,
    x_own, x_img, z_img, w1_own, w2_own, w1_all, w2_all, w1_t, w2_big, b_own, b_all, b1_col, b2_col, h_mine, h_other, v_part, mid_part, act, wc1, wc2,
    b1_v, b2_v, bc1, bc2, g1, o1, g2, o2, x_tally, w_tally, b_tally,
    local_sem, mine_sem, chan_sem, small_sem, own_sem,
    w_send, w_recv, b_send, b_recv, x_send, x_recv, h_send, h_recv, z_send, z_recv,
):
    me = lax.axis_index(AXIS)
    side = math.isqrt(n // CORES)
    my_core = lax.rem(me, CORES)
    my_chip = me // CORES
    my_x = lax.rem(my_chip, side)
    my_y = my_chip // side
    cols = [lax.rem(my_x + d, side) for d in range(side)]
    lines = [lax.rem(my_y + d, side) * side for d in range(side)]
    chips = [lines[dy] + cols[dx] for dx, dy in send_order(side)]
    other = me + 1 - 2 * my_core
    n_chips = n // CORES
    _, patches, rows, chans = x_img.shape
    pairs = patches // 2
    hid = w1_hbm.shape[1]
    wide = chans // LANES
    ff = wc1.shape[1]
    piece = PAIR * hid // SWAPS

    def two(j):
        return pl.ds(pl.multiple_of(2 * j, 2), 2)

    def image_rows(chip, p):
        return pl.ds(pl.multiple_of(2 * CORES * chip + 2 * p, 2), 2)

    def settle(counted, sem):
        pltpu.make_async_copy(counted, counted, sem).wait()

    def remote(src, dst, ss, rs, j):
        pltpu.make_async_remote_copy(src_ref=src, dst_ref=dst, send_sem=ss, recv_sem=rs, device_id={AXIS: j}).start()

    def to_twins(src, dst, ss, rs):
        for k in chips:
            remote(src(k), dst, ss, rs, CORES * k + my_core)

    b_all[...] = jnp.zeros_like(b_all)

    barrier = pltpu.get_barrier_semaphore()
    for j in [CORES * k + my_core for k in chips] + [other]:
        pl.semaphore_signal(barrier, inc=1, device_id={AXIS: j})

    weights, mine = [], []
    for i, (w_hbm, w_own, w_all) in enumerate(((w1_hbm, w1_own, w1_all), (w2_hbm, w2_own, w2_all))):
        for q in range(pairs):
            src = w_hbm.at[pl.ds(2 * q, 2), :]
            weights.append(pltpu.make_async_copy(src, w_own.at[q], local_sem.at[i, q]))
            mine.append(pltpu.make_async_copy(src, w_all.at[q, two(my_chip), :], mine_sem.at[i, q]))
    x_load = pltpu.make_async_copy(x_hbm, x_own, chan_sem.at[2])
    biases = [pltpu.make_async_copy(b1_hbm, b1_v, small_sem.at[0]), pltpu.make_async_copy(b2_hbm, b2_v, small_sem.at[1])]
    x_mine = [pltpu.make_async_copy(x_hbm.at[:, image_rows(my_chip, p), :], x_img.at[p, :, two(my_chip), :], chan_sem.at[3 + p]) for p in range(PAIR)]
    smalls = [
        pltpu.make_async_copy(src, dst, small_sem.at[2 + i])
        for i, (src, dst) in enumerate(((g1_hbm, g1), (o1_hbm, o1), (g2_hbm, g2), (o2_hbm, o2), (bc1_hbm, bc1), (bc2_hbm, bc2)))
    ]
    chan_loads = [pltpu.make_async_copy(wc1_hbm, wc1, chan_sem.at[0]), pltpu.make_async_copy(wc2_hbm, wc2, chan_sem.at[1])]
    early_weights, late_weights = weights[:pairs], weights[pairs:]
    for c in [x_load] + early_weights + biases + late_weights + mine + x_mine + smalls + chan_loads:
        c.start()
    b_own[...] = jnp.zeros_like(b_own)
    for c in biases:
        c.wait()
    for i, b_v in enumerate((b1_v, b2_v)):
        b_own[i, :, pl.ds(0, b_v.shape[1])] = jnp.broadcast_to(b_v[...], (2, b_v.shape[1]))
    for c in early_weights + [x_load]:
        c.wait()
    pl.semaphore_wait(barrier, n_chips)

    def send_x(p, t):
        part = pl.ds(sum(x_parts[p][:t]), x_parts[p][t])
        to_twins(lambda k: x_own.at[part, image_rows(k, p), :], x_img.at[p, part, two(my_chip), :], x_send.at[p], x_recv.at[p, t])

    to_twins(lambda k: w1_own, w1_all.at[:, two(my_chip), :], w_send.at[0], w_recv.at[0])
    to_twins(lambda k: b_own, b_all.at[:, two(my_chip), :], b_send, b_recv)
    for t in range(len(x_parts[0])):
        send_x(0, t)
    for c in late_weights:
        c.wait()
    to_twins(lambda k: w2_own, w2_all.at[:, two(my_chip), :], w_send.at[1], w_recv.at[1])
    for t in range(len(x_parts[1])):
        send_x(1, t)
    for c in mine + x_mine + smalls:
        c.wait()

    even = lax.rem(lax.broadcasted_iota(jnp.int32, (rows, hid), 0), 2) == 0
    keep = (lax.rem(lax.broadcasted_iota(jnp.int32, (rows, 2 * hid), 0), 2) == 0) == (
        lax.broadcasted_iota(jnp.int32, (rows, 2 * hid), 1) < hid
    )

    def expand(w_all, q):
        wq = w_all[q].astype(F32)
        first = jnp.where(even, wq, pltpu.roll(wq, 1, 0))
        second = jnp.where(even, pltpu.roll(wq, rows - 1, 0), wq)
        return [jnp.where(keep, jnp.concatenate([d, d], axis=1), 0.0) for d in (first, second)]

    settle(w_tally, w_recv.at[0])
    q = 0
    while q < pairs:
        group = [q] if q + 1 == pairs else [q, q + 1]
        block = jnp.concatenate([d for g in group for d in expand(w1_all, g)], axis=0)
        w1_t[:, pl.ds(2 * rows * q, block.shape[0])] = jnp.transpose(block).astype(BF16)
        q += len(group)

    def half_sum(p):
        at = 0
        for t, per in enumerate(x_parts[p]):
            settle(x_tally.at[:, pl.ds(0, per)], x_recv.at[p, t])
            wide_x = x_img[p, pl.ds(at, per)].reshape(per * rows, chans).astype(F32)
            u = layer_norm(wide_x, g1[...], o1[...]).astype(BF16)
            last = t == len(x_parts[p]) - 1
            blocks = PAIR if last else 1
            height = PAIR * hid // blocks
            for i in range(blocks):
                span = pl.ds(height * i, height)
                before = h_mine[p, span, :] if t else widen(jnp.concatenate([b1_col[...]] * (height // hid), axis=0), wide)
                h_mine[p, span, :] = before + jnp.dot(w1_t[span, pl.ds(at * rows, per * rows)], u, preferred_element_type=F32)
                for s in range(SWAPS // blocks * i, SWAPS // blocks * (i + 1)) if last else ():
                    swap = pl.ds(piece * s, piece)
                    remote(h_mine.at[p, swap, :], h_other.at[p, swap, :], h_send.at[p, s], h_recv.at[p, s], other)
            at += per

    def activate(p):
        halves = []
        for i in range(SWAPS):
            span = pl.ds(piece * i, piece)
            settle(h_other.at[p, span, :], h_recv.at[p, i])
            halves.append(gelu(h_mine[p, span, :] + h_other[p, span, :]).astype(BF16))
        return jnp.concatenate(halves, axis=0)

    def prepare(slot, p, g, at, per):
        m = per * rows
        span = pl.ds(at * rows, m)
        tok = jnp.dot(w2_big[span, :], g, preferred_element_type=F32) + widen(b2_col[span, :], wide)
        x_mid = (x_img[p, pl.ds(at, per)].reshape(m, chans).astype(F32) + tok).astype(BF16)
        mid_part[slot, pl.ds(0, m), :] = x_mid
        v_part[slot, pl.ds(0, m), :] = layer_norm(x_mid.astype(F32), g2[...], o2[...]).astype(BF16)

    def expand_channels(slot, per):
        m = pl.ds(0, per * rows)
        v = v_part[slot, m, :]
        for f in range(ff // ff_tile):
            cols_f = pl.ds(f * ff_tile, ff_tile)
            pre = jnp.dot(v, wc1[:, cols_f], preferred_element_type=F32) + bc1[:, cols_f]
            act[m, cols_f] = gelu(pre).astype(BF16)

    def contract_channels(slot, p, at, per):
        m = pl.ds(0, per * rows)
        ch_out = jnp.dot(act[m, :], wc2[...], preferred_element_type=F32) + bc2[...]
        z_img[p, pl.ds(at, per)] = (mid_part[slot, m, :].astype(F32) + ch_out).astype(BF16).reshape(per, rows, chans)

    def own_block(i, p, at, per):
        part = pl.ds(at, per)
        away = pltpu.make_async_copy(z_img.at[p, part, two(my_chip), :], spare.at[p, part], own_sem.at[0, i])
        back = pltpu.make_async_copy(spare.at[p, part], out_ref.at[part, image_rows(my_chip, p), :], own_sem.at[1, i])
        return away, back

    settle(b_tally, b_recv)
    is_mine = lax.broadcasted_iota(jnp.int32, (rows, LANES), 0) // 2 == my_chip
    for i in range(2):
        b_all[i] = jnp.where(is_mine, jnp.broadcast_to(b_own[i, pl.ds(0, 1), :], (rows, LANES)), b_all[i])
    per_chip = hid // n_chips
    picked = b_all[0, pl.ds(0, n_chips, stride=2), :]
    spread = jnp.broadcast_to(picked.reshape(n_chips, 1, LANES), (n_chips, per_chip, LANES))
    place = lax.broadcasted_iota(jnp.int32, spread.shape, 1) - (per_chip // CORES) * my_core
    diag = place == lax.broadcasted_iota(jnp.int32, spread.shape, 2)
    col1 = jnp.broadcast_to(jnp.sum(jnp.where(diag, spread, 0.0), axis=2, keepdims=True), spread.shape)
    b1_col[...] = col1.reshape(hid, LANES)
    tail = b_all[1]
    for s in range(patches):
        b2_col[pl.ds(rows * s, rows), :] = jnp.broadcast_to(tail[:, s : s + 1], (rows, LANES))

    half_sum(0)
    settle(w_tally, w_recv.at[1])
    for q in range(pairs):
        w2_big[pl.ds(2 * rows * q, 2 * rows), :] = jnp.concatenate(expand(w2_all, q), axis=0).astype(BF16)
    for c in chan_loads:
        c.wait()

    steps = [(p, sum(parts[:t]), per) for p, parts in enumerate(z_parts) for t, per in enumerate(parts)]
    g = activate(0)
    prepare(0, 0, g, *steps[0][1:])
    own = []
    for i, (p, at, per) in enumerate(steps):
        slot = i % 2
        part = pl.ds(at, per)
        expand_channels(slot, per)
        following = steps[i + 1] if i + 1 < len(steps) else None
        if following and i:
            if following[0] != p:
                g = activate(following[0])
            prepare(1 - slot, following[0], g, *following[1:])
        contract_channels(slot, p, at, per)
        if own:
            own[-1][0].wait()
            own[-1][1].start()
        own.append(own_block(i, p, at, per))
        own[-1][0].start()
        to_twins(lambda k: z_img.at[p, part, two(k), :], out_ref.at[part, image_rows(my_chip, p), :], z_send.at[p], z_recv.at[p])
        if i == 0:
            prepare(1 - slot, p, g, *following[1:])
        if i == b_after:
            half_sum(1)

    own[-1][0].wait()
    own[-1][1].start()
    for _, back in own:
        back.wait()
    for p in range(PAIR):
        settle(x_tally, z_recv.at[p])
    for p in range(PAIR):
        settle(x_tally, z_send.at[p])
        settle(x_tally, x_send.at[p])
        settle(w_tally, w_send.at[p])
        for i in range(SWAPS):
            settle(h_mine.at[p, pl.ds(piece * i, piece), :], h_send.at[p, i])
    settle(b_tally, b_send)


def solution(mesh, x_split=((4, 3, 2), (1,)), z_split=((2, 1), (4, 3, 2)), b_after=0, ff_tile=512):
    row_spec = P("dp", AXIS, None)
    n = mesh.shape[AXIS]

    def local_layer(x_blk, w1_rows, b1_part, w2_cols, b2_part, w_ch1, b_ch1, w_ch2, b_ch2, ln1_gain, ln1_bias, ln2_gain, ln2_bias):
        x_t = jnp.transpose(x_blk, (1, 0, 2))
        w2_rows = jnp.transpose(w2_cols)
        patches, images, chans = x_t.shape
        n_chips = n // CORES
        rows = 2 * n_chips
        hid = w1_rows.shape[1]
        ff = w_ch1.shape[1]
        x_parts, z_parts = ([[patches * w // sum(ws) for w in ws] for ws in split] for split in (x_split, z_split))
        m = max(max(parts) for parts in z_parts) * rows
        hbm = pl.BlockSpec(memory_space=pltpu.HBM)
        sem = pltpu.SemaphoreType.DMA
        smalls = [v[None, :] for v in (b1_part, b2_part, b_ch1, b_ch2, ln1_gain, ln1_bias, ln2_gain, ln2_bias)]
        b1, b2, bc1, bc2, g1, o1, g2, o2 = smalls
        z_t, _ = pl.pallas_call(
            functools.partial(mixer_kernel, n, x_parts, z_parts, b_after, ff_tile),
            name="mixer",
            out_shape=(pltpu.VMEM(x_t.shape, BF16), pltpu.HBM((PAIR, patches, 2, chans), BF16)),
            in_specs=[hbm] * 13,
            out_specs=(pl.BlockSpec(memory_space=pltpu.VMEM), hbm),
            scratch_shapes=[
                pltpu.VMEM(x_t.shape, BF16),
                pltpu.VMEM((PAIR, patches, rows, chans), BF16),
                pltpu.VMEM((PAIR, patches, rows, chans), BF16),
                pltpu.VMEM((patches // 2, 2, hid), BF16),
                pltpu.VMEM((patches // 2, 2, hid), BF16),
                pltpu.VMEM((patches // 2, rows, hid), BF16),
                pltpu.VMEM((patches // 2, rows, hid), BF16),
                pltpu.VMEM((PAIR * hid, patches * rows), BF16),
                pltpu.VMEM((patches * rows, PAIR * hid), BF16),
                pltpu.VMEM((2, 2, LANES), F32),
                pltpu.VMEM((2, rows, LANES), F32),
                pltpu.VMEM((hid, LANES), F32),
                pltpu.VMEM((patches * rows, LANES), F32),
                pltpu.VMEM((PAIR, PAIR * hid, chans), F32),
                pltpu.VMEM((PAIR, PAIR * hid, chans), F32),
                pltpu.VMEM((2, m, chans), BF16),
                pltpu.VMEM((2, m, chans), BF16),
                pltpu.VMEM((m, ff), BF16),
                pltpu.VMEM(w_ch1.shape, BF16),
                pltpu.VMEM(w_ch2.shape, BF16),
                *[pltpu.VMEM(v.shape, F32) for v in smalls],
                pltpu.VMEM((n_chips - 1, patches, 2, chans), BF16),
                pltpu.VMEM((n_chips - 1, patches // 2, 2, hid), BF16),
                pltpu.VMEM((n_chips - 1, 2, 2, LANES), F32),
                sem((2, patches // 2)),
                sem((2, patches // 2)),
                sem((5,)),
                sem((8,)),
                sem((2, sum(len(parts) for parts in z_parts))),
                sem((2,)), sem((2,)),
                sem, sem,
                sem((PAIR,)), sem((PAIR, max(len(parts) for parts in x_parts))),
                sem((PAIR, SWAPS)), sem((PAIR, SWAPS)),
                sem((PAIR,)), sem((PAIR,)),
            ],
            compiler_params=pltpu.CompilerParams(
                collective_id=0, has_side_effects=True, vmem_limit_bytes=VMEM_LIMIT - 2 * math.prod(x_t.shape)
            ),
        )(x_t, w1_rows, w2_rows, b1, b2, w_ch1, bc1, w_ch2, bc2, g1, o1, g2, o2)
        return jnp.transpose(z_t, (1, 0, 2))

    in_specs = (row_spec, P(AXIS, None), P(AXIS), P(None, AXIS), P(AXIS), P(None, None), P(None), P(None, None), P(None), P(None), P(None), P(None), P(None))
    return jax.shard_map(local_layer, mesh=mesh, in_specs=in_specs, out_specs=row_spec, check_vma=False)
```

```python
import functools
import math

import jax
import jax.numpy as jnp
from jax import lax
from jax.experimental import pallas as pl
from jax.experimental.pallas import tpu as pltpu
from jax.sharding import PartitionSpec as P

LN_EPS = 1e-6
AXIS = "sp"
LANES = 128
CORES = 2
PAIR = 2
SWAPS = 4
VMEM_LIMIT = 67043328
BF16 = jnp.bfloat16
F32 = jnp.float32


def layer_norm(values, ln_gain, ln_bias):
    mean_val = jnp.mean(values, axis=-1, keepdims=True)
    centred = values - mean_val
    var_val = jnp.mean(centred * centred, axis=-1, keepdims=True)
    return centred * lax.rsqrt(var_val + LN_EPS) * ln_gain + ln_bias


def gelu(a):
    scale = math.sqrt(2.0 / math.pi)
    half = 0.5 * a
    return half + half * jnp.tanh(a * (scale + (scale * 0.044715) * (a * a)))


def widen(column, copies):
    return jnp.concatenate([column] * copies, axis=1)


def send_order(side):
    hops = lambda d: min(d, side - d)
    flows = []
    for dx, dy in sorted(
        ((dx, dy) for dx in range(side) for dy in range(side) if dx or dy),
        key=lambda o: (hops(o[0]) + hops(o[1]), max(hops(o[0]), hops(o[1])), o),
    ):
        for flow in ((dx, dy), ((side - dx) % side, (side - dy) % side)):
            if flow not in flows:
                flows.append(flow)
    return flows[::-1]


def mixer_kernel(
    n, x_parts, z_parts, b_after, ff_tile,
    x_hbm, w1_hbm, w2_hbm, b1_hbm, b2_hbm, wc1_hbm, bc1_hbm, wc2_hbm, bc2_hbm, g1_hbm, o1_hbm, g2_hbm, o2_hbm,
    out_ref, spare,
    x_own, x_img, z_img, w1_own, w2_own, w1_all, w2_all, w1_t, w2_big, b_own, b_all, b1_col, b2_col, h_mine, h_other, v_part, mid_part, act, wc1, wc2,
    b1_v, b2_v, bc1, bc2, g1, o1, g2, o2, x_tally, w_tally, b_tally,
    local_sem, mine_sem, chan_sem, small_sem, own_sem,
    w_send, w_recv, b_send, b_recv, x_send, x_recv, h_send, h_recv, z_send, z_recv,
):
    me = lax.axis_index(AXIS)
    side = math.isqrt(n // CORES)
    my_core = lax.rem(me, CORES)
    my_chip = me // CORES
    my_x = lax.rem(my_chip, side)
    my_y = my_chip // side
    cols = [lax.rem(my_x + d, side) for d in range(side)]
    lines = [lax.rem(my_y + d, side) * side for d in range(side)]
    chips = [lines[dy] + cols[dx] for dx, dy in send_order(side)]
    row_chips = [lines[0] + cols[dx] for dx, dy in send_order(side) if dy == 0]
    col_chips = [lines[dy] + cols[0] for dx, dy in send_order(side) if dx == 0]
    other = me + 1 - 2 * my_core
    n_chips = n // CORES
    _, patches, rows, chans = x_img.shape
    pairs = patches // 2
    hid = w1_hbm.shape[1]
    wide = chans // LANES
    ff = wc1.shape[1]
    piece = PAIR * hid // SWAPS

    def two(j):
        return pl.ds(pl.multiple_of(2 * j, 2), 2)

    def image_rows(chip, p):
        return pl.ds(pl.multiple_of(2 * CORES * chip + 2 * p, 2), 2)

    def settle(counted, sem):
        pltpu.make_async_copy(counted, counted, sem).wait()

    def remote(src, dst, ss, rs, j):
        pltpu.make_async_remote_copy(src_ref=src, dst_ref=dst, send_sem=ss, recv_sem=rs, device_id={AXIS: j}).start()

    def to_twins(src, dst, ss, rs, targets=chips):
        for k in targets:
            remote(src(k), dst, ss, rs, CORES * k + my_core)

    b_all[...] = jnp.zeros_like(b_all)

    barrier = pltpu.get_barrier_semaphore()
    for j in [CORES * k + my_core for k in chips] + [other]:
        pl.semaphore_signal(barrier, inc=1, device_id={AXIS: j})

    weights, mine = [], []
    for i, (w_hbm, w_own, w_all) in enumerate(((w1_hbm, w1_own, w1_all), (w2_hbm, w2_own, w2_all))):
        for q in range(pairs):
            src = w_hbm.at[pl.ds(2 * q, 2), :]
            weights.append(pltpu.make_async_copy(src, w_own.at[q], local_sem.at[i, q]))
            mine.append(pltpu.make_async_copy(src, w_all.at[q, two(my_chip), :], mine_sem.at[i, q]))
    x_load = pltpu.make_async_copy(x_hbm, x_own, chan_sem.at[2])
    biases = [pltpu.make_async_copy(b1_hbm, b1_v, small_sem.at[0]), pltpu.make_async_copy(b2_hbm, b2_v, small_sem.at[1])]
    x_mine = [pltpu.make_async_copy(x_hbm.at[:, image_rows(my_chip, p), :], x_img.at[p, :, two(my_chip), :], chan_sem.at[3 + p]) for p in range(PAIR)]
    smalls = [
        pltpu.make_async_copy(src, dst, small_sem.at[2 + i])
        for i, (src, dst) in enumerate(((g1_hbm, g1), (o1_hbm, o1), (g2_hbm, g2), (o2_hbm, o2), (bc1_hbm, bc1), (bc2_hbm, bc2)))
    ]
    chan_loads = [pltpu.make_async_copy(wc1_hbm, wc1, chan_sem.at[0]), pltpu.make_async_copy(wc2_hbm, wc2, chan_sem.at[1])]
    early_weights, late_weights = weights[:pairs], weights[pairs:]
    for c in [x_load] + early_weights + biases + late_weights + mine + x_mine + smalls + chan_loads:
        c.start()
    b_own[...] = jnp.zeros_like(b_own)
    for c in biases:
        c.wait()
    for i, b_v in enumerate((b1_v, b2_v)):
        b_own[i, :, pl.ds(0, b_v.shape[1])] = jnp.broadcast_to(b_v[...], (2, b_v.shape[1]))
    for c in early_weights + [x_load]:
        c.wait()
    pl.semaphore_wait(barrier, n_chips)

    def send_x(p, t):
        part = pl.ds(sum(x_parts[p][:t]), x_parts[p][t])
        to_twins(lambda k: x_own.at[part, image_rows(k, p), :], x_img.at[p, part, two(my_chip), :], x_send.at[p], x_recv.at[p, t])

    halves = (pl.ds(0, (pairs + 1) // 2), pl.ds((pairs + 1) // 2, pairs // 2))

    def first_stage(w, w_own, w_all):
        for h, near in enumerate((row_chips, col_chips)):
            to_twins(lambda k: w_own.at[halves[h]], w_all.at[halves[h], two(my_chip), :], w_send.at[w], w_recv.at[w, h, 0], near)

    def second_stage(w, w_all):
        line = w_all.at[halves[0], pl.ds(pl.multiple_of(2 * side * my_y, 2 * side), 2 * side), :]
        settle(w_tally.at[pl.ds(0, side - 1), halves[0]], w_recv.at[w, 0, 0])
        to_twins(lambda k: line, line, w_send.at[w], w_recv.at[w, 0, 1], col_chips)
        settle(w_tally.at[pl.ds(0, side - 1), halves[1]], w_recv.at[w, 1, 0])
        for c in [my_chip] + col_chips:
            block = w_all.at[halves[1], two(c), :]
            to_twins(lambda k: block, block, w_send.at[w], w_recv.at[w, 1, 1], row_chips)

    def landed(w):
        for h in range(2):
            settle(w_tally.at[pl.ds(0, side * (side - 1)), halves[h]], w_recv.at[w, h, 1])

    first_stage(0, w1_own, w1_all)
    for c in late_weights:
        c.wait()
    first_stage(1, w2_own, w2_all)
    to_twins(lambda k: b_own, b_all.at[:, two(my_chip), :], b_send, b_recv)
    send_x(0, 0)
    for c in mine + x_mine + smalls:
        c.wait()
    second_stage(0, w1_all)
    for t in range(1, len(x_parts[0])):
        send_x(0, t)
    second_stage(1, w2_all)
    for t in range(len(x_parts[1])):
        send_x(1, t)

    even = lax.rem(lax.broadcasted_iota(jnp.int32, (rows, hid), 0), 2) == 0
    keep = (lax.rem(lax.broadcasted_iota(jnp.int32, (rows, 2 * hid), 0), 2) == 0) == (
        lax.broadcasted_iota(jnp.int32, (rows, 2 * hid), 1) < hid
    )

    def expand(w_all, q):
        wq = w_all[q].astype(F32)
        first = jnp.where(even, wq, pltpu.roll(wq, 1, 0))
        second = jnp.where(even, pltpu.roll(wq, rows - 1, 0), wq)
        return [jnp.where(keep, jnp.concatenate([d, d], axis=1), 0.0) for d in (first, second)]

    landed(0)
    q = 0
    while q < pairs:
        group = [q] if q + 1 == pairs else [q, q + 1]
        block = jnp.concatenate([d for g in group for d in expand(w1_all, g)], axis=0)
        w1_t[:, pl.ds(2 * rows * q, block.shape[0])] = jnp.transpose(block).astype(BF16)
        q += len(group)

    def half_sum(p):
        at = 0
        for t, per in enumerate(x_parts[p]):
            settle(x_tally.at[:, pl.ds(0, per)], x_recv.at[p, t])
            wide_x = x_img[p, pl.ds(at, per)].reshape(per * rows, chans).astype(F32)
            u = layer_norm(wide_x, g1[...], o1[...]).astype(BF16)
            last = t == len(x_parts[p]) - 1
            blocks = PAIR if last else 1
            height = PAIR * hid // blocks
            for i in range(blocks):
                span = pl.ds(height * i, height)
                before = h_mine[p, span, :] if t else widen(jnp.concatenate([b1_col[...]] * (height // hid), axis=0), wide)
                h_mine[p, span, :] = before + jnp.dot(w1_t[span, pl.ds(at * rows, per * rows)], u, preferred_element_type=F32)
                for s in range(SWAPS // blocks * i, SWAPS // blocks * (i + 1)) if last else ():
                    swap = pl.ds(piece * s, piece)
                    remote(h_mine.at[p, swap, :], h_other.at[p, swap, :], h_send.at[p, s], h_recv.at[p, s], other)
            at += per

    def activate(p):
        halves = []
        for i in range(SWAPS):
            span = pl.ds(piece * i, piece)
            settle(h_other.at[p, span, :], h_recv.at[p, i])
            halves.append(gelu(h_mine[p, span, :] + h_other[p, span, :]).astype(BF16))
        return jnp.concatenate(halves, axis=0)

    def prepare(slot, p, g, at, per):
        m = per * rows
        span = pl.ds(at * rows, m)
        tok = jnp.dot(w2_big[span, :], g, preferred_element_type=F32) + widen(b2_col[span, :], wide)
        x_mid = (x_img[p, pl.ds(at, per)].reshape(m, chans).astype(F32) + tok).astype(BF16)
        mid_part[slot, pl.ds(0, m), :] = x_mid
        v_part[slot, pl.ds(0, m), :] = layer_norm(x_mid.astype(F32), g2[...], o2[...]).astype(BF16)

    def expand_channels(slot, per):
        m = pl.ds(0, per * rows)
        v = v_part[slot, m, :]
        for f in range(ff // ff_tile):
            cols_f = pl.ds(f * ff_tile, ff_tile)
            pre = jnp.dot(v, wc1[:, cols_f], preferred_element_type=F32) + bc1[:, cols_f]
            act[m, cols_f] = gelu(pre).astype(BF16)

    def contract_channels(slot, p, at, per):
        m = pl.ds(0, per * rows)
        ch_out = jnp.dot(act[m, :], wc2[...], preferred_element_type=F32) + bc2[...]
        z_img[p, pl.ds(at, per)] = (mid_part[slot, m, :].astype(F32) + ch_out).astype(BF16).reshape(per, rows, chans)

    def own_block(i, p, at, per):
        part = pl.ds(at, per)
        away = pltpu.make_async_copy(z_img.at[p, part, two(my_chip), :], spare.at[p, part], own_sem.at[0, i])
        back = pltpu.make_async_copy(spare.at[p, part], out_ref.at[part, image_rows(my_chip, p), :], own_sem.at[1, i])
        return away, back

    settle(b_tally, b_recv)
    is_mine = lax.broadcasted_iota(jnp.int32, (rows, LANES), 0) // 2 == my_chip
    for i in range(2):
        b_all[i] = jnp.where(is_mine, jnp.broadcast_to(b_own[i, pl.ds(0, 1), :], (rows, LANES)), b_all[i])
    per_chip = hid // n_chips
    picked = b_all[0, pl.ds(0, n_chips, stride=2), :]
    spread = jnp.broadcast_to(picked.reshape(n_chips, 1, LANES), (n_chips, per_chip, LANES))
    place = lax.broadcasted_iota(jnp.int32, spread.shape, 1) - (per_chip // CORES) * my_core
    diag = place == lax.broadcasted_iota(jnp.int32, spread.shape, 2)
    col1 = jnp.broadcast_to(jnp.sum(jnp.where(diag, spread, 0.0), axis=2, keepdims=True), spread.shape)
    b1_col[...] = col1.reshape(hid, LANES)
    tail = b_all[1]
    for s in range(patches):
        b2_col[pl.ds(rows * s, rows), :] = jnp.broadcast_to(tail[:, s : s + 1], (rows, LANES))

    half_sum(0)
    landed(1)
    for q in range(pairs):
        w2_big[pl.ds(2 * rows * q, 2 * rows), :] = jnp.concatenate(expand(w2_all, q), axis=0).astype(BF16)
    for c in chan_loads:
        c.wait()

    steps = [(p, sum(parts[:t]), per) for p, parts in enumerate(z_parts) for t, per in enumerate(parts)]
    g = activate(0)
    prepare(0, 0, g, *steps[0][1:])
    own = []
    for i, (p, at, per) in enumerate(steps):
        slot = i % 2
        part = pl.ds(at, per)
        expand_channels(slot, per)
        following = steps[i + 1] if i + 1 < len(steps) else None
        if following and i:
            if following[0] != p:
                g = activate(following[0])
            prepare(1 - slot, following[0], g, *following[1:])
        contract_channels(slot, p, at, per)
        if own:
            own[-1][0].wait()
            own[-1][1].start()
        own.append(own_block(i, p, at, per))
        own[-1][0].start()
        to_twins(lambda k: z_img.at[p, part, two(k), :], out_ref.at[part, image_rows(my_chip, p), :], z_send.at[p], z_recv.at[p])
        if i == 0:
            prepare(1 - slot, p, g, *following[1:])
        if i == b_after:
            half_sum(1)

    own[-1][0].wait()
    own[-1][1].start()
    for _, back in own:
        back.wait()
    for p in range(PAIR):
        settle(x_tally, z_recv.at[p])
    for p in range(PAIR):
        settle(x_tally, z_send.at[p])
        settle(x_tally, x_send.at[p])
        settle(w_tally, w_send.at[p])
        for i in range(SWAPS):
            settle(h_mine.at[p, pl.ds(piece * i, piece), :], h_send.at[p, i])
    settle(b_tally, b_send)


def solution(mesh, x_split=((4, 3, 2), (1,)), z_split=((2, 1), (4, 3, 2)), b_after=0, ff_tile=512):
    row_spec = P("dp", AXIS, None)
    n = mesh.shape[AXIS]

    def local_layer(x_blk, w1_rows, b1_part, w2_cols, b2_part, w_ch1, b_ch1, w_ch2, b_ch2, ln1_gain, ln1_bias, ln2_gain, ln2_bias):
        x_t = jnp.transpose(x_blk, (1, 0, 2))
        w2_rows = jnp.transpose(w2_cols)
        patches, images, chans = x_t.shape
        n_chips = n // CORES
        rows = 2 * n_chips
        hid = w1_rows.shape[1]
        ff = w_ch1.shape[1]
        x_parts, z_parts = ([[patches * w // sum(ws) for w in ws] for ws in split] for split in (x_split, z_split))
        m = max(max(parts) for parts in z_parts) * rows
        hbm = pl.BlockSpec(memory_space=pltpu.HBM)
        sem = pltpu.SemaphoreType.DMA
        smalls = [v[None, :] for v in (b1_part, b2_part, b_ch1, b_ch2, ln1_gain, ln1_bias, ln2_gain, ln2_bias)]
        b1, b2, bc1, bc2, g1, o1, g2, o2 = smalls
        z_t, _ = pl.pallas_call(
            functools.partial(mixer_kernel, n, x_parts, z_parts, b_after, ff_tile),
            name="mixer",
            out_shape=(pltpu.VMEM(x_t.shape, BF16), pltpu.HBM((PAIR, patches, 2, chans), BF16)),
            in_specs=[hbm] * 13,
            out_specs=(pl.BlockSpec(memory_space=pltpu.VMEM), hbm),
            scratch_shapes=[
                pltpu.VMEM(x_t.shape, BF16),
                pltpu.VMEM((PAIR, patches, rows, chans), BF16),
                pltpu.VMEM((PAIR, patches, rows, chans), BF16),
                pltpu.VMEM((patches // 2, 2, hid), BF16),
                pltpu.VMEM((patches // 2, 2, hid), BF16),
                pltpu.VMEM((patches // 2, rows, hid), BF16),
                pltpu.VMEM((patches // 2, rows, hid), BF16),
                pltpu.VMEM((PAIR * hid, patches * rows), BF16),
                pltpu.VMEM((patches * rows, PAIR * hid), BF16),
                pltpu.VMEM((2, 2, LANES), F32),
                pltpu.VMEM((2, rows, LANES), F32),
                pltpu.VMEM((hid, LANES), F32),
                pltpu.VMEM((patches * rows, LANES), F32),
                pltpu.VMEM((PAIR, PAIR * hid, chans), F32),
                pltpu.VMEM((PAIR, PAIR * hid, chans), F32),
                pltpu.VMEM((2, m, chans), BF16),
                pltpu.VMEM((2, m, chans), BF16),
                pltpu.VMEM((m, ff), BF16),
                pltpu.VMEM(w_ch1.shape, BF16),
                pltpu.VMEM(w_ch2.shape, BF16),
                *[pltpu.VMEM(v.shape, F32) for v in smalls],
                pltpu.VMEM((n_chips - 1, patches, 2, chans), BF16),
                pltpu.VMEM((n_chips - 1, patches // 2, 2, hid), BF16),
                pltpu.VMEM((n_chips - 1, 2, 2, LANES), F32),
                sem((2, patches // 2)),
                sem((2, patches // 2)),
                sem((5,)),
                sem((8,)),
                sem((2, sum(len(parts) for parts in z_parts))),
                sem((2,)), sem((2, 2, 2)),
                sem, sem,
                sem((PAIR,)), sem((PAIR, max(len(parts) for parts in x_parts))),
                sem((PAIR, SWAPS)), sem((PAIR, SWAPS)),
                sem((PAIR,)), sem((PAIR,)),
            ],
            compiler_params=pltpu.CompilerParams(
                collective_id=0, has_side_effects=True, vmem_limit_bytes=VMEM_LIMIT - 2 * math.prod(x_t.shape)
            ),
        )(x_t, w1_rows, w2_rows, b1, b2, w_ch1, bc1, w_ch2, bc2, g1, o1, g2, o2)
        return jnp.transpose(z_t, (1, 0, 2))

    in_specs = (row_spec, P(AXIS, None), P(AXIS), P(None, AXIS), P(AXIS), P(None, None), P(None), P(None, None), P(None), P(None), P(None), P(None), P(None))
    return jax.shard_map(local_layer, mesh=mesh, in_specs=in_specs, out_specs=row_spec, check_vma=False)
```

```python
import functools
import math

import jax
import jax.numpy as jnp
from jax import lax
from jax.experimental import pallas as pl
from jax.experimental.pallas import tpu as pltpu
from jax.sharding import PartitionSpec as P

LN_EPS = 1e-6
AXIS = "sp"
LANES = 128
CORES = 2
PAIR = 2
SWAPS = 4
VMEM_LIMIT = 67043328
BF16 = jnp.bfloat16
F32 = jnp.float32


def layer_norm(values, ln_gain, ln_bias):
    mean_val = jnp.mean(values, axis=-1, keepdims=True)
    centred = values - mean_val
    var_val = jnp.mean(centred * centred, axis=-1, keepdims=True)
    return centred * lax.rsqrt(var_val + LN_EPS) * ln_gain + ln_bias


def gelu(a):
    scale = math.sqrt(2.0 / math.pi)
    half = 0.5 * a
    return half + half * jnp.tanh(a * (scale + (scale * 0.044715) * (a * a)))


def widen(column, copies):
    return jnp.concatenate([column] * copies, axis=1)


def send_order(side):
    hops = lambda d: min(d, side - d)
    flows = []
    for dx, dy in sorted(
        ((dx, dy) for dx in range(side) for dy in range(side) if dx or dy),
        key=lambda o: (hops(o[0]) + hops(o[1]), max(hops(o[0]), hops(o[1])), o),
    ):
        for flow in ((dx, dy), ((side - dx) % side, (side - dy) % side)):
            if flow not in flows:
                flows.append(flow)
    return flows[::-1]


def mixer_kernel(
    n, x_parts, z_parts, b_after, ff_tile,
    x_hbm, w1_hbm, w2_hbm, b1_hbm, b2_hbm, wc1_hbm, bc1_hbm, wc2_hbm, bc2_hbm, g1_hbm, o1_hbm, g2_hbm, o2_hbm,
    out_ref, spare,
    x_own, x_img, z_img, w1_own, w2_own, w1_all, w2_all, w1_t, w2_big, b_own, b_all, b1_col, b2_col, h_mine, h_other, v_part, mid_part, act, wc1, wc2,
    b1_v, b2_v, bc1, bc2, g1, o1, g2, o2, x_tally, w_tally, b_tally,
    local_sem, mine_sem, chan_sem, small_sem, own_sem,
    w_send, w_recv, b_send, b_recv, x_send, x_recv, h_send, h_recv, z_send, z_recv,
):
    me = lax.axis_index(AXIS)
    side = math.isqrt(n // CORES)
    my_core = lax.rem(me, CORES)
    my_chip = me // CORES
    my_x = lax.rem(my_chip, side)
    my_y = my_chip // side
    cols = [lax.rem(my_x + d, side) for d in range(side)]
    lines = [lax.rem(my_y + d, side) * side for d in range(side)]
    chips = [lines[dy] + cols[dx] for dx, dy in send_order(side)]
    row_chips = [lines[0] + cols[dx] for dx, dy in send_order(side) if dy == 0]
    col_chips = [lines[dy] + cols[0] for dx, dy in send_order(side) if dx == 0]
    other = me + 1 - 2 * my_core
    n_chips = n // CORES
    _, patches, rows, chans = x_img.shape
    pairs = patches // 2
    hid = w1_hbm.shape[1]
    wide = chans // LANES
    ff = wc1.shape[1]
    piece = PAIR * hid // SWAPS

    def two(j):
        return pl.ds(pl.multiple_of(2 * j, 2), 2)

    def image_rows(chip, p):
        return pl.ds(pl.multiple_of(2 * CORES * chip + 2 * p, 2), 2)

    def settle(counted, sem):
        pltpu.make_async_copy(counted, counted, sem).wait()

    def remote(src, dst, ss, rs, j):
        pltpu.make_async_remote_copy(src_ref=src, dst_ref=dst, send_sem=ss, recv_sem=rs, device_id={AXIS: j}).start()

    def to_twins(src, dst, ss, rs, targets=chips):
        for k in targets:
            remote(src(k), dst, ss, rs, CORES * k + my_core)

    b_all[...] = jnp.zeros_like(b_all)

    barrier = pltpu.get_barrier_semaphore()
    for j in [CORES * k + my_core for k in chips] + [other]:
        pl.semaphore_signal(barrier, inc=1, device_id={AXIS: j})

    weights, mine = [], []
    for i, (w_hbm, w_own, w_all) in enumerate(((w1_hbm, w1_own, w1_all), (w2_hbm, w2_own, w2_all))):
        for q in range(pairs):
            src = w_hbm.at[pl.ds(2 * q, 2), :]
            weights.append(pltpu.make_async_copy(src, w_own.at[q], local_sem.at[i, q]))
            mine.append(pltpu.make_async_copy(src, w_all.at[q, two(my_chip), :], mine_sem.at[i, q]))
    x_load = pltpu.make_async_copy(x_hbm, x_own, chan_sem.at[2])
    biases = [pltpu.make_async_copy(b1_hbm, b1_v, small_sem.at[0]), pltpu.make_async_copy(b2_hbm, b2_v, small_sem.at[1])]
    x_mine = [pltpu.make_async_copy(x_hbm.at[:, image_rows(my_chip, p), :], x_img.at[p, :, two(my_chip), :], chan_sem.at[3 + p]) for p in range(PAIR)]
    smalls = [
        pltpu.make_async_copy(src, dst, small_sem.at[2 + i])
        for i, (src, dst) in enumerate(((g1_hbm, g1), (o1_hbm, o1), (g2_hbm, g2), (o2_hbm, o2), (bc1_hbm, bc1), (bc2_hbm, bc2)))
    ]
    chan_loads = [pltpu.make_async_copy(wc1_hbm, wc1, chan_sem.at[0]), pltpu.make_async_copy(wc2_hbm, wc2, chan_sem.at[1])]
    for c in weights + biases + [x_load] + mine + x_mine + smalls + chan_loads:
        c.start()
    b_own[...] = jnp.zeros_like(b_own)
    for c in biases:
        c.wait()
    for i, b_v in enumerate((b1_v, b2_v)):
        b_own[i, :, pl.ds(0, b_v.shape[1])] = jnp.broadcast_to(b_v[...], (2, b_v.shape[1]))
    for c in weights + [x_load]:
        c.wait()
    pl.semaphore_wait(barrier, n_chips)

    def send_x(p, t):
        part = pl.ds(sum(x_parts[p][:t]), x_parts[p][t])
        to_twins(lambda k: x_own.at[part, image_rows(k, p), :], x_img.at[p, part, two(my_chip), :], x_send.at[p], x_recv.at[p, t])

    to_twins(lambda k: w1_own, w1_all.at[:, two(my_chip), :], w_send.at[0], w_recv.at[0, 0], row_chips)
    to_twins(lambda k: w2_own, w2_all.at[:, two(my_chip), :], w_send.at[1], w_recv.at[1, 0], col_chips)
    to_twins(lambda k: b_own, b_all.at[:, two(my_chip), :], b_send, b_recv)
    send_x(0, 0)
    for c in mine + x_mine + smalls:
        c.wait()
    near = w_tally.at[pl.ds(0, side - 1)]
    far = w_tally.at[pl.ds(0, side * (side - 1))]
    line = w1_all.at[:, pl.ds(pl.multiple_of(2 * side * my_y, 2 * side), 2 * side), :]
    settle(near, w_recv.at[0, 0])
    to_twins(lambda k: line, line, w_send.at[0], w_recv.at[0, 1], col_chips)
    for t in range(1, len(x_parts[0])):
        send_x(0, t)
    settle(near, w_recv.at[1, 0])
    for c in [my_chip] + col_chips:
        block = w2_all.at[:, two(c), :]
        to_twins(lambda k: block, block, w_send.at[1], w_recv.at[1, 1], row_chips)
    for t in range(len(x_parts[1])):
        send_x(1, t)

    even = lax.rem(lax.broadcasted_iota(jnp.int32, (rows, hid), 0), 2) == 0
    keep = (lax.rem(lax.broadcasted_iota(jnp.int32, (rows, 2 * hid), 0), 2) == 0) == (
        lax.broadcasted_iota(jnp.int32, (rows, 2 * hid), 1) < hid
    )

    def expand(w_all, q):
        wq = w_all[q].astype(F32)
        first = jnp.where(even, wq, pltpu.roll(wq, 1, 0))
        second = jnp.where(even, pltpu.roll(wq, rows - 1, 0), wq)
        return [jnp.where(keep, jnp.concatenate([d, d], axis=1), 0.0) for d in (first, second)]

    settle(far, w_recv.at[0, 1])
    q = 0
    while q < pairs:
        group = [q] if q + 1 == pairs else [q, q + 1]
        block = jnp.concatenate([d for g in group for d in expand(w1_all, g)], axis=0)
        w1_t[:, pl.ds(2 * rows * q, block.shape[0])] = jnp.transpose(block).astype(BF16)
        q += len(group)

    def half_sum(p):
        at = 0
        for t, per in enumerate(x_parts[p]):
            settle(x_tally.at[:, pl.ds(0, per)], x_recv.at[p, t])
            wide_x = x_img[p, pl.ds(at, per)].reshape(per * rows, chans).astype(F32)
            u = layer_norm(wide_x, g1[...], o1[...]).astype(BF16)
            last = t == len(x_parts[p]) - 1
            blocks = PAIR if last else 1
            height = PAIR * hid // blocks
            for i in range(blocks):
                span = pl.ds(height * i, height)
                before = h_mine[p, span, :] if t else widen(jnp.concatenate([b1_col[...]] * (height // hid), axis=0), wide)
                h_mine[p, span, :] = before + jnp.dot(w1_t[span, pl.ds(at * rows, per * rows)], u, preferred_element_type=F32)
                for s in range(SWAPS // blocks * i, SWAPS // blocks * (i + 1)) if last else ():
                    swap = pl.ds(piece * s, piece)
                    remote(h_mine.at[p, swap, :], h_other.at[p, swap, :], h_send.at[p, s], h_recv.at[p, s], other)
            at += per

    def activate(p):
        halves = []
        for i in range(SWAPS):
            span = pl.ds(piece * i, piece)
            settle(h_other.at[p, span, :], h_recv.at[p, i])
            halves.append(gelu(h_mine[p, span, :] + h_other[p, span, :]).astype(BF16))
        return jnp.concatenate(halves, axis=0)

    def prepare(slot, p, g, at, per):
        m = per * rows
        span = pl.ds(at * rows, m)
        tok = jnp.dot(w2_big[span, :], g, preferred_element_type=F32) + widen(b2_col[span, :], wide)
        x_mid = (x_img[p, pl.ds(at, per)].reshape(m, chans).astype(F32) + tok).astype(BF16)
        mid_part[slot, pl.ds(0, m), :] = x_mid
        v_part[slot, pl.ds(0, m), :] = layer_norm(x_mid.astype(F32), g2[...], o2[...]).astype(BF16)

    def expand_channels(slot, per):
        m = pl.ds(0, per * rows)
        v = v_part[slot, m, :]
        for f in range(ff // ff_tile):
            cols_f = pl.ds(f * ff_tile, ff_tile)
            pre = jnp.dot(v, wc1[:, cols_f], preferred_element_type=F32) + bc1[:, cols_f]
            act[m, cols_f] = gelu(pre).astype(BF16)

    def contract_channels(slot, p, at, per):
        m = pl.ds(0, per * rows)
        ch_out = jnp.dot(act[m, :], wc2[...], preferred_element_type=F32) + bc2[...]
        z_img[p, pl.ds(at, per)] = (mid_part[slot, m, :].astype(F32) + ch_out).astype(BF16).reshape(per, rows, chans)

    def own_block(i, p, at, per):
        part = pl.ds(at, per)
        away = pltpu.make_async_copy(z_img.at[p, part, two(my_chip), :], spare.at[p, part], own_sem.at[0, i])
        back = pltpu.make_async_copy(spare.at[p, part], out_ref.at[part, image_rows(my_chip, p), :], own_sem.at[1, i])
        return away, back

    settle(b_tally, b_recv)
    is_mine = lax.broadcasted_iota(jnp.int32, (rows, LANES), 0) // 2 == my_chip
    for i in range(2):
        b_all[i] = jnp.where(is_mine, jnp.broadcast_to(b_own[i, pl.ds(0, 1), :], (rows, LANES)), b_all[i])
    per_chip = hid // n_chips
    picked = b_all[0, pl.ds(0, n_chips, stride=2), :]
    spread = jnp.broadcast_to(picked.reshape(n_chips, 1, LANES), (n_chips, per_chip, LANES))
    place = lax.broadcasted_iota(jnp.int32, spread.shape, 1) - (per_chip // CORES) * my_core
    diag = place == lax.broadcasted_iota(jnp.int32, spread.shape, 2)
    col1 = jnp.broadcast_to(jnp.sum(jnp.where(diag, spread, 0.0), axis=2, keepdims=True), spread.shape)
    b1_col[...] = col1.reshape(hid, LANES)
    tail = b_all[1]
    for s in range(patches):
        b2_col[pl.ds(rows * s, rows), :] = jnp.broadcast_to(tail[:, s : s + 1], (rows, LANES))

    half_sum(0)
    settle(far, w_recv.at[1, 1])
    for q in range(pairs):
        w2_big[pl.ds(2 * rows * q, 2 * rows), :] = jnp.concatenate(expand(w2_all, q), axis=0).astype(BF16)
    for c in chan_loads:
        c.wait()

    steps = [(p, sum(parts[:t]), per) for p, parts in enumerate(z_parts) for t, per in enumerate(parts)]
    g = activate(0)
    prepare(0, 0, g, *steps[0][1:])
    own = []
    for i, (p, at, per) in enumerate(steps):
        slot = i % 2
        part = pl.ds(at, per)
        expand_channels(slot, per)
        following = steps[i + 1] if i + 1 < len(steps) else None
        if following and i:
            if following[0] != p:
                g = activate(following[0])
            prepare(1 - slot, following[0], g, *following[1:])
        contract_channels(slot, p, at, per)
        if own:
            own[-1][0].wait()
            own[-1][1].start()
        own.append(own_block(i, p, at, per))
        own[-1][0].start()
        to_twins(lambda k: z_img.at[p, part, two(k), :], out_ref.at[part, image_rows(my_chip, p), :], z_send.at[p], z_recv.at[p])
        if i == 0:
            prepare(1 - slot, p, g, *following[1:])
        if i == b_after:
            half_sum(1)

    own[-1][0].wait()
    own[-1][1].start()
    for _, back in own:
        back.wait()
    for p in range(PAIR):
        settle(x_tally, z_recv.at[p])
    for p in range(PAIR):
        settle(x_tally, z_send.at[p])
        settle(x_tally, x_send.at[p])
        settle(w_tally, w_send.at[p])
        for i in range(SWAPS):
            settle(h_mine.at[p, pl.ds(piece * i, piece), :], h_send.at[p, i])
    settle(b_tally, b_send)


def solution(mesh, x_split=((4, 3, 2), (1,)), z_split=((2, 1), (4, 3, 2)), b_after=0, ff_tile=512):
    row_spec = P("dp", AXIS, None)
    n = mesh.shape[AXIS]

    def local_layer(x_blk, w1_rows, b1_part, w2_cols, b2_part, w_ch1, b_ch1, w_ch2, b_ch2, ln1_gain, ln1_bias, ln2_gain, ln2_bias):
        x_t = jnp.transpose(x_blk, (1, 0, 2))
        w2_rows = jnp.transpose(w2_cols)
        patches, images, chans = x_t.shape
        n_chips = n // CORES
        rows = 2 * n_chips
        hid = w1_rows.shape[1]
        ff = w_ch1.shape[1]
        x_parts, z_parts = ([[patches * w // sum(ws) for w in ws] for ws in split] for split in (x_split, z_split))
        m = max(max(parts) for parts in z_parts) * rows
        hbm = pl.BlockSpec(memory_space=pltpu.HBM)
        sem = pltpu.SemaphoreType.DMA
        smalls = [v[None, :] for v in (b1_part, b2_part, b_ch1, b_ch2, ln1_gain, ln1_bias, ln2_gain, ln2_bias)]
        b1, b2, bc1, bc2, g1, o1, g2, o2 = smalls
        z_t, _ = pl.pallas_call(
            functools.partial(mixer_kernel, n, x_parts, z_parts, b_after, ff_tile),
            name="mixer",
            out_shape=(pltpu.VMEM(x_t.shape, BF16), pltpu.HBM((PAIR, patches, 2, chans), BF16)),
            in_specs=[hbm] * 13,
            out_specs=(pl.BlockSpec(memory_space=pltpu.VMEM), hbm),
            scratch_shapes=[
                pltpu.VMEM(x_t.shape, BF16),
                pltpu.VMEM((PAIR, patches, rows, chans), BF16),
                pltpu.VMEM((PAIR, patches, rows, chans), BF16),
                pltpu.VMEM((patches // 2, 2, hid), BF16),
                pltpu.VMEM((patches // 2, 2, hid), BF16),
                pltpu.VMEM((patches // 2, rows, hid), BF16),
                pltpu.VMEM((patches // 2, rows, hid), BF16),
                pltpu.VMEM((PAIR * hid, patches * rows), BF16),
                pltpu.VMEM((patches * rows, PAIR * hid), BF16),
                pltpu.VMEM((2, 2, LANES), F32),
                pltpu.VMEM((2, rows, LANES), F32),
                pltpu.VMEM((hid, LANES), F32),
                pltpu.VMEM((patches * rows, LANES), F32),
                pltpu.VMEM((PAIR, PAIR * hid, chans), F32),
                pltpu.VMEM((PAIR, PAIR * hid, chans), F32),
                pltpu.VMEM((2, m, chans), BF16),
                pltpu.VMEM((2, m, chans), BF16),
                pltpu.VMEM((m, ff), BF16),
                pltpu.VMEM(w_ch1.shape, BF16),
                pltpu.VMEM(w_ch2.shape, BF16),
                *[pltpu.VMEM(v.shape, F32) for v in smalls],
                pltpu.VMEM((n_chips - 1, patches, 2, chans), BF16),
                pltpu.VMEM((n_chips - 1, patches // 2, 2, hid), BF16),
                pltpu.VMEM((n_chips - 1, 2, 2, LANES), F32),
                sem((2, patches // 2)),
                sem((2, patches // 2)),
                sem((5,)),
                sem((8,)),
                sem((2, sum(len(parts) for parts in z_parts))),
                sem((2,)), sem((2, 2)),
                sem, sem,
                sem((PAIR,)), sem((PAIR, max(len(parts) for parts in x_parts))),
                sem((PAIR, SWAPS)), sem((PAIR, SWAPS)),
                sem((PAIR,)), sem((PAIR,)),
            ],
            compiler_params=pltpu.CompilerParams(
                collective_id=0, has_side_effects=True, vmem_limit_bytes=VMEM_LIMIT - 2 * math.prod(x_t.shape)
            ),
        )(x_t, w1_rows, w2_rows, b1, b2, w_ch1, bc1, w_ch2, bc2, g1, o1, g2, o2)
        return jnp.transpose(z_t, (1, 0, 2))

    in_specs = (row_spec, P(AXIS, None), P(AXIS), P(None, AXIS), P(AXIS), P(None, None), P(None), P(None, None), P(None), P(None), P(None), P(None), P(None))
    return jax.shard_map(local_layer, mesh=mesh, in_specs=in_specs, out_specs=row_spec, check_vma=False)
```

```python
import functools
import math

import jax
import jax.numpy as jnp
from jax import lax
from jax.experimental import pallas as pl
from jax.experimental.pallas import tpu as pltpu
from jax.sharding import PartitionSpec as P

LN_EPS = 1e-6
AXIS = "sp"
LANES = 128
CORES = 2
PAIR = 2
SWAPS = 4
VMEM_LIMIT = 67043328
BF16 = jnp.bfloat16
F32 = jnp.float32


def layer_norm(values, ln_gain, ln_bias):
    mean_val = jnp.mean(values, axis=-1, keepdims=True)
    centred = values - mean_val
    var_val = jnp.mean(centred * centred, axis=-1, keepdims=True)
    return centred * lax.rsqrt(var_val + LN_EPS) * ln_gain + ln_bias


def gelu(a):
    scale = math.sqrt(2.0 / math.pi)
    half = 0.5 * a
    return half + half * jnp.tanh(a * (scale + (scale * 0.044715) * (a * a)))


def widen(column, copies):
    return jnp.concatenate([column] * copies, axis=1)


def send_order(side):
    hops = lambda d: min(d, side - d)
    flows = []
    for dx, dy in sorted(
        ((dx, dy) for dx in range(side) for dy in range(side) if dx or dy),
        key=lambda o: (hops(o[0]) + hops(o[1]), max(hops(o[0]), hops(o[1])), o),
    ):
        for flow in ((dx, dy), ((side - dx) % side, (side - dy) % side)):
            if flow not in flows:
                flows.append(flow)
    return flows[::-1]


def mixer_kernel(
    n, x_parts, z_parts, b_after, ff_tile,
    x_hbm, w1_hbm, w2_hbm, b1_hbm, b2_hbm, wc1_hbm, bc1_hbm, wc2_hbm, bc2_hbm, g1_hbm, o1_hbm, g2_hbm, o2_hbm,
    out_ref, spare,
    x_own, x_img, z_img, w1_own, w2_own, w1_all, w2_all, w1_t, w2_big, b_own, b_all, b1_col, b2_col, h_mine, h_other, v_part, mid_part, act, wc1, wc2,
    b1_v, b2_v, bc1, bc2, g1, o1, g2, o2, x_tally, w_tally, b_tally,
    local_sem, mine_sem, chan_sem, small_sem, own_sem,
    w_send, w_recv, b_send, b_recv, x_send, x_recv, h_send, h_recv, z_send, z_recv,
):
    me = lax.axis_index(AXIS)
    side = math.isqrt(n // CORES)
    my_core = lax.rem(me, CORES)
    my_chip = me // CORES
    my_x = lax.rem(my_chip, side)
    my_y = my_chip // side
    cols = [lax.rem(my_x + d, side) for d in range(side)]
    lines = [lax.rem(my_y + d, side) * side for d in range(side)]
    chips = [lines[dy] + cols[dx] for dx, dy in send_order(side)]
    row_chips = [lines[0] + cols[dx] for dx, dy in send_order(side) if dy == 0]
    col_chips = [lines[dy] + cols[0] for dx, dy in send_order(side) if dx == 0]
    other = me + 1 - 2 * my_core
    n_chips = n // CORES
    _, patches, rows, chans = x_img.shape
    pairs = patches // 2
    hid = w1_hbm.shape[1]
    wide = chans // LANES
    ff = wc1.shape[1]
    piece = PAIR * hid // SWAPS

    def two(j):
        return pl.ds(pl.multiple_of(2 * j, 2), 2)

    def image_rows(chip, p):
        return pl.ds(pl.multiple_of(2 * CORES * chip + 2 * p, 2), 2)

    def settle(counted, sem):
        pltpu.make_async_copy(counted, counted, sem).wait()

    def remote(src, dst, ss, rs, j):
        pltpu.make_async_remote_copy(src_ref=src, dst_ref=dst, send_sem=ss, recv_sem=rs, device_id={AXIS: j}).start()

    def to_twins(src, dst, ss, rs, targets=chips):
        for k in targets:
            remote(src(k), dst, ss, rs, CORES * k + my_core)

    b_all[...] = jnp.zeros_like(b_all)

    barrier = pltpu.get_barrier_semaphore()
    for j in [CORES * k + my_core for k in chips] + [other]:
        pl.semaphore_signal(barrier, inc=1, device_id={AXIS: j})

    weights, mine = [], []
    for i, (w_hbm, w_own, w_all) in enumerate(((w1_hbm, w1_own, w1_all), (w2_hbm, w2_own, w2_all))):
        for q in range(pairs):
            src = w_hbm.at[pl.ds(2 * q, 2), :]
            weights.append(pltpu.make_async_copy(src, w_own.at[q], local_sem.at[i, q]))
            mine.append(pltpu.make_async_copy(src, w_all.at[q, two(my_chip), :], mine_sem.at[i, q]))
    x_load = pltpu.make_async_copy(x_hbm, x_own, chan_sem.at[2])
    biases = [pltpu.make_async_copy(b1_hbm, b1_v, small_sem.at[0]), pltpu.make_async_copy(b2_hbm, b2_v, small_sem.at[1])]
    x_mine = [pltpu.make_async_copy(x_hbm.at[:, image_rows(my_chip, p), :], x_img.at[p, :, two(my_chip), :], chan_sem.at[3 + p]) for p in range(PAIR)]
    smalls = [
        pltpu.make_async_copy(src, dst, small_sem.at[2 + i])
        for i, (src, dst) in enumerate(((g1_hbm, g1), (o1_hbm, o1), (g2_hbm, g2), (o2_hbm, o2), (bc1_hbm, bc1), (bc2_hbm, bc2)))
    ]
    chan_loads = [pltpu.make_async_copy(wc1_hbm, wc1, chan_sem.at[0]), pltpu.make_async_copy(wc2_hbm, wc2, chan_sem.at[1])]
    for c in weights + biases + [x_load] + mine + x_mine + smalls + chan_loads:
        c.start()
    b_own[...] = jnp.zeros_like(b_own)
    for c in biases:
        c.wait()
    for i, b_v in enumerate((b1_v, b2_v)):
        b_own[i, :, pl.ds(0, b_v.shape[1])] = jnp.broadcast_to(b_v[...], (2, b_v.shape[1]))
    for c in weights + [x_load]:
        c.wait()
    pl.semaphore_wait(barrier, n_chips)

    def send_x(p, t):
        part = pl.ds(sum(x_parts[p][:t]), x_parts[p][t])
        to_twins(lambda k: x_own.at[part, image_rows(k, p), :], x_img.at[p, part, two(my_chip), :], x_send.at[p], x_recv.at[p, t])

    to_twins(lambda k: w1_own, w1_all.at[:, two(my_chip), :], w_send.at[0], w_recv.at[0, 0], row_chips)
    to_twins(lambda k: w2_own, w2_all.at[:, two(my_chip), :], w_send.at[1], w_recv.at[1, 0], col_chips)
    to_twins(lambda k: b_own, b_all.at[:, two(my_chip), :], b_send, b_recv)
    send_x(0, 0)
    for c in mine + x_mine + smalls:
        c.wait()
    near = w_tally.at[pl.ds(0, side - 1)]
    far = w_tally.at[pl.ds(0, side * (side - 1))]
    line = w1_all.at[:, pl.ds(pl.multiple_of(2 * side * my_y, 2 * side), 2 * side), :]
    settle(near, w_recv.at[0, 0])
    to_twins(lambda k: line, line, w_send.at[0], w_recv.at[0, 1], col_chips)
    for t in range(1, len(x_parts[0])):
        send_x(0, t)
    settle(near, w_recv.at[1, 0])
    for c in [my_chip] + col_chips:
        block = w2_all.at[:, two(c), :]
        to_twins(lambda k: block, block, w_send.at[1], w_recv.at[1, 1], row_chips)
    for t in range(len(x_parts[1])):
        send_x(1, t)

    even = lax.rem(lax.broadcasted_iota(jnp.int32, (rows, hid), 0), 2) == 0
    keep = (lax.rem(lax.broadcasted_iota(jnp.int32, (rows, 2 * hid), 0), 2) == 0) == (
        lax.broadcasted_iota(jnp.int32, (rows, 2 * hid), 1) < hid
    )

    def expand(w_all, q):
        wq = w_all[q].astype(F32)
        first = jnp.where(even, wq, pltpu.roll(wq, 1, 0))
        second = jnp.where(even, pltpu.roll(wq, rows - 1, 0), wq)
        return [jnp.where(keep, jnp.concatenate([d, d], axis=1), 0.0) for d in (first, second)]

    settle(far, w_recv.at[0, 1])
    q = 0
    while q < pairs:
        group = [q] if q + 1 == pairs else [q, q + 1]
        block = jnp.concatenate([d for g in group for d in expand(w1_all, g)], axis=0)
        w1_t[:, pl.ds(2 * rows * q, block.shape[0])] = jnp.transpose(block).astype(BF16)
        q += len(group)

    def half_sum(p):
        at = 0
        for t, per in enumerate(x_parts[p]):
            settle(x_tally.at[:, pl.ds(0, per)], x_recv.at[p, t])
            wide_x = x_img[p, pl.ds(at, per)].reshape(per * rows, chans).astype(F32)
            u = layer_norm(wide_x, g1[...], o1[...]).astype(BF16)
            last = t == len(x_parts[p]) - 1
            blocks = PAIR if last else 1
            height = PAIR * hid // blocks
            for i in range(blocks):
                span = pl.ds(height * i, height)
                before = h_mine[p, span, :] if t else widen(jnp.concatenate([b1_col[...]] * (height // hid), axis=0), wide)
                h_mine[p, span, :] = before + jnp.dot(w1_t[span, pl.ds(at * rows, per * rows)], u, preferred_element_type=F32)
                for s in range(SWAPS // blocks * i, SWAPS // blocks * (i + 1)) if last else ():
                    swap = pl.ds(piece * s, piece)
                    remote(h_mine.at[p, swap, :], h_other.at[p, swap, :], h_send.at[p, s], h_recv.at[p, s], other)
            at += per

    def activate(p):
        halves = []
        for i in range(SWAPS):
            span = pl.ds(piece * i, piece)
            settle(h_other.at[p, span, :], h_recv.at[p, i])
            halves.append(gelu(h_mine[p, span, :] + h_other[p, span, :]).astype(BF16))
        return jnp.concatenate(halves, axis=0)

    def prepare(slot, p, g, at, per):
        m = per * rows
        span = pl.ds(at * rows, m)
        tok = jnp.dot(w2_big[span, :], g, preferred_element_type=F32) + widen(b2_col[span, :], wide)
        x_mid = (x_img[p, pl.ds(at, per)].reshape(m, chans).astype(F32) + tok).astype(BF16)
        mid_part[slot, pl.ds(0, m), :] = x_mid
        v_part[slot, pl.ds(0, m), :] = layer_norm(x_mid.astype(F32), g2[...], o2[...]).astype(BF16)

    def expand_channels(slot, per):
        m = pl.ds(0, per * rows)
        v = v_part[slot, m, :]
        for f in range(ff // ff_tile):
            cols_f = pl.ds(f * ff_tile, ff_tile)
            pre = jnp.dot(v, wc1[:, cols_f], preferred_element_type=F32) + bc1[:, cols_f]
            act[m, cols_f] = gelu(pre).astype(BF16)

    def contract_channels(slot, p, at, per):
        m = pl.ds(0, per * rows)
        ch_out = jnp.dot(act[m, :], wc2[...], preferred_element_type=F32) + bc2[...]
        z_img[p, pl.ds(at, per)] = (mid_part[slot, m, :].astype(F32) + ch_out).astype(BF16).reshape(per, rows, chans)

    def own_block(i, p, at, per):
        part = pl.ds(at, per)
        away = pltpu.make_async_copy(z_img.at[p, part, two(my_chip), :], spare.at[p, part], own_sem.at[0, i])
        back = pltpu.make_async_copy(spare.at[p, part], out_ref.at[part, image_rows(my_chip, p), :], own_sem.at[1, i])
        return away, back

    settle(b_tally, b_recv)
    is_mine = lax.broadcasted_iota(jnp.int32, (rows, LANES), 0) // 2 == my_chip
    for i in range(2):
        b_all[i] = jnp.where(is_mine, jnp.broadcast_to(b_own[i, pl.ds(0, 1), :], (rows, LANES)), b_all[i])
    per_chip = hid // n_chips
    picked = b_all[0, pl.ds(0, n_chips, stride=2), :]
    spread = jnp.broadcast_to(picked.reshape(n_chips, 1, LANES), (n_chips, per_chip, LANES))
    place = lax.broadcasted_iota(jnp.int32, spread.shape, 1) - (per_chip // CORES) * my_core
    diag = place == lax.broadcasted_iota(jnp.int32, spread.shape, 2)
    col1 = jnp.broadcast_to(jnp.sum(jnp.where(diag, spread, 0.0), axis=2, keepdims=True), spread.shape)
    b1_col[...] = col1.reshape(hid, LANES)
    tail = b_all[1]
    for s in range(patches):
        b2_col[pl.ds(rows * s, rows), :] = jnp.broadcast_to(tail[:, s : s + 1], (rows, LANES))

    half_sum(0)
    settle(far, w_recv.at[1, 1])
    for q in range(pairs):
        w2_big[pl.ds(2 * rows * q, 2 * rows), :] = jnp.concatenate(expand(w2_all, q), axis=0).astype(BF16)
    for c in chan_loads:
        c.wait()

    steps = [(p, sum(parts[:t]), per) for p, parts in enumerate(z_parts) for t, per in enumerate(parts)]
    g = activate(0)
    prepare(0, 0, g, *steps[0][1:])
    own = []
    for i, (p, at, per) in enumerate(steps):
        slot = i % 2
        part = pl.ds(at, per)
        expand_channels(slot, per)
        following = steps[i + 1] if i + 1 < len(steps) else None
        if following and i:
            if following[0] != p:
                g = activate(following[0])
            prepare(1 - slot, following[0], g, *following[1:])
        contract_channels(slot, p, at, per)
        if own:
            own[-1][0].wait()
            own[-1][1].start()
        own.append(own_block(i, p, at, per))
        own[-1][0].start()
        to_twins(lambda k: z_img.at[p, part, two(k), :], out_ref.at[part, image_rows(my_chip, p), :], z_send.at[p], z_recv.at[p])
        if i == 0:
            prepare(1 - slot, p, g, *following[1:])
        if i == b_after:
            half_sum(1)

    own[-1][0].wait()
    own[-1][1].start()
    for _, back in own:
        back.wait()
    for p in range(PAIR):
        settle(x_tally, z_recv.at[p])
    for p in range(PAIR):
        settle(x_tally, z_send.at[p])
        settle(x_tally, x_send.at[p])
        settle(w_tally, w_send.at[p])
        for i in range(SWAPS):
            settle(h_mine.at[p, pl.ds(piece * i, piece), :], h_send.at[p, i])
    settle(b_tally, b_send)


def solution(mesh, x_split=((4, 3, 2), (1,)), z_split=((2, 1), (1, 1, 1)), b_after=0, ff_tile=512):
    row_spec = P("dp", AXIS, None)
    n = mesh.shape[AXIS]

    def local_layer(x_blk, w1_rows, b1_part, w2_cols, b2_part, w_ch1, b_ch1, w_ch2, b_ch2, ln1_gain, ln1_bias, ln2_gain, ln2_bias):
        x_t = jnp.transpose(x_blk, (1, 0, 2))
        w2_rows = jnp.transpose(w2_cols)
        patches, images, chans = x_t.shape
        n_chips = n // CORES
        rows = 2 * n_chips
        hid = w1_rows.shape[1]
        ff = w_ch1.shape[1]
        x_parts, z_parts = ([[patches * w // sum(ws) for w in ws] for ws in split] for split in (x_split, z_split))
        m = max(max(parts) for parts in z_parts) * rows
        hbm = pl.BlockSpec(memory_space=pltpu.HBM)
        sem = pltpu.SemaphoreType.DMA
        smalls = [v[None, :] for v in (b1_part, b2_part, b_ch1, b_ch2, ln1_gain, ln1_bias, ln2_gain, ln2_bias)]
        b1, b2, bc1, bc2, g1, o1, g2, o2 = smalls
        z_t, _ = pl.pallas_call(
            functools.partial(mixer_kernel, n, x_parts, z_parts, b_after, ff_tile),
            name="mixer",
            out_shape=(pltpu.VMEM(x_t.shape, BF16), pltpu.HBM((PAIR, patches, 2, chans), BF16)),
            in_specs=[hbm] * 13,
            out_specs=(pl.BlockSpec(memory_space=pltpu.VMEM), hbm),
            scratch_shapes=[
                pltpu.VMEM(x_t.shape, BF16),
                pltpu.VMEM((PAIR, patches, rows, chans), BF16),
                pltpu.VMEM((PAIR, patches, rows, chans), BF16),
                pltpu.VMEM((patches // 2, 2, hid), BF16),
                pltpu.VMEM((patches // 2, 2, hid), BF16),
                pltpu.VMEM((patches // 2, rows, hid), BF16),
                pltpu.VMEM((patches // 2, rows, hid), BF16),
                pltpu.VMEM((PAIR * hid, patches * rows), BF16),
                pltpu.VMEM((patches * rows, PAIR * hid), BF16),
                pltpu.VMEM((2, 2, LANES), F32),
                pltpu.VMEM((2, rows, LANES), F32),
                pltpu.VMEM((hid, LANES), F32),
                pltpu.VMEM((patches * rows, LANES), F32),
                pltpu.VMEM((PAIR, PAIR * hid, chans), F32),
                pltpu.VMEM((PAIR, PAIR * hid, chans), F32),
                pltpu.VMEM((2, m, chans), BF16),
                pltpu.VMEM((2, m, chans), BF16),
                pltpu.VMEM((m, ff), BF16),
                pltpu.VMEM(w_ch1.shape, BF16),
                pltpu.VMEM(w_ch2.shape, BF16),
                *[pltpu.VMEM(v.shape, F32) for v in smalls],
                pltpu.VMEM((n_chips - 1, patches, 2, chans), BF16),
                pltpu.VMEM((n_chips - 1, patches // 2, 2, hid), BF16),
                pltpu.VMEM((n_chips - 1, 2, 2, LANES), F32),
                sem((2, patches // 2)),
                sem((2, patches // 2)),
                sem((5,)),
                sem((8,)),
                sem((2, sum(len(parts) for parts in z_parts))),
                sem((2,)), sem((2, 2)),
                sem, sem,
                sem((PAIR,)), sem((PAIR, max(len(parts) for parts in x_parts))),
                sem((PAIR, SWAPS)), sem((PAIR, SWAPS)),
                sem((PAIR,)), sem((PAIR,)),
            ],
            compiler_params=pltpu.CompilerParams(
                collective_id=0, has_side_effects=True, vmem_limit_bytes=VMEM_LIMIT - 2 * math.prod(x_t.shape)
            ),
        )(x_t, w1_rows, w2_rows, b1, b2, w_ch1, bc1, w_ch2, bc2, g1, o1, g2, o2)
        return jnp.transpose(z_t, (1, 0, 2))

    in_specs = (row_spec, P(AXIS, None), P(AXIS), P(None, AXIS), P(AXIS), P(None, None), P(None), P(None, None), P(None), P(None), P(None), P(None), P(None))
    return jax.shard_map(local_layer, mesh=mesh, in_specs=in_specs, out_specs=row_spec, check_vma=False)
```

```python
import functools
import math

import jax
import jax.numpy as jnp
from jax import lax
from jax.experimental import pallas as pl
from jax.experimental.pallas import tpu as pltpu
from jax.sharding import PartitionSpec as P

LN_EPS = 1e-6
AXIS = "sp"
LANES = 128
CORES = 2
PAIR = 2
SWAPS = 4
VMEM_LIMIT = 67043328
BF16 = jnp.bfloat16
F32 = jnp.float32


def layer_norm(values, ln_gain, ln_bias):
    mean_val = jnp.mean(values, axis=-1, keepdims=True)
    centred = values - mean_val
    var_val = jnp.mean(centred * centred, axis=-1, keepdims=True)
    return centred * lax.rsqrt(var_val + LN_EPS) * ln_gain + ln_bias


def gelu(a):
    scale = math.sqrt(2.0 / math.pi)
    half = 0.5 * a
    return half + half * jnp.tanh(a * (scale + (scale * 0.044715) * (a * a)))


def widen(column, copies):
    return jnp.concatenate([column] * copies, axis=1)


def send_order(side):
    hops = lambda d: min(d, side - d)
    flows = []
    for dx, dy in sorted(
        ((dx, dy) for dx in range(side) for dy in range(side) if dx or dy),
        key=lambda o: (hops(o[0]) + hops(o[1]), max(hops(o[0]), hops(o[1])), o),
    ):
        for flow in ((dx, dy), ((side - dx) % side, (side - dy) % side)):
            if flow not in flows:
                flows.append(flow)
    return flows[::-1]


def mixer_kernel(
    n, x_parts, z_parts, b_after, ff_tile,
    x_hbm, w1_hbm, w2_hbm, b1_hbm, b2_hbm, wc1_hbm, bc1_hbm, wc2_hbm, bc2_hbm, g1_hbm, o1_hbm, g2_hbm, o2_hbm,
    out_ref, spare,
    x_own, x_img, z_img, w1_own, w2_own, w1_all, w2_all, w1_t, w2_big, b_own, b_all, b1_col, b2_col, h_mine, h_other, v_part, mid_part, act, wc1, wc2,
    b1_v, b2_v, bc1, bc2, g1, o1, g2, o2, x_tally, w_tally, b_tally,
    local_sem, mine_sem, chan_sem, small_sem, own_sem,
    w_send, w_recv, b_send, b_recv, x_send, x_recv, h_send, h_recv, z_send, z_recv,
):
    me = lax.axis_index(AXIS)
    side = math.isqrt(n // CORES)
    my_core = lax.rem(me, CORES)
    my_chip = me // CORES
    my_x = lax.rem(my_chip, side)
    my_y = my_chip // side
    cols = [lax.rem(my_x + d, side) for d in range(side)]
    lines = [lax.rem(my_y + d, side) * side for d in range(side)]
    chips = [lines[dy] + cols[dx] for dx, dy in send_order(side)]
    row_chips = [lines[0] + cols[dx] for dx, dy in send_order(side) if dy == 0]
    col_chips = [lines[dy] + cols[0] for dx, dy in send_order(side) if dx == 0]
    other = me + 1 - 2 * my_core
    n_chips = n // CORES
    _, patches, rows, chans = x_img.shape
    pairs = patches // 2
    hid = w1_hbm.shape[1]
    wide = chans // LANES
    ff = wc1.shape[1]
    piece = PAIR * hid // SWAPS

    def two(j):
        return pl.ds(pl.multiple_of(2 * j, 2), 2)

    def image_rows(chip, p):
        return pl.ds(pl.multiple_of(2 * CORES * chip + 2 * p, 2), 2)

    def settle(counted, sem):
        pltpu.make_async_copy(counted, counted, sem).wait()

    def remote(src, dst, ss, rs, j):
        pltpu.make_async_remote_copy(src_ref=src, dst_ref=dst, send_sem=ss, recv_sem=rs, device_id={AXIS: j}).start()

    def to_twins(src, dst, ss, rs, targets=chips):
        for k in targets:
            remote(src(k), dst, ss, rs, CORES * k + my_core)

    b_all[...] = jnp.zeros_like(b_all)

    barrier = pltpu.get_barrier_semaphore()
    for j in [CORES * k + my_core for k in chips] + [other]:
        pl.semaphore_signal(barrier, inc=1, device_id={AXIS: j})

    weights, mine = [], []
    for i, (w_hbm, w_own, w_all) in enumerate(((w1_hbm, w1_own, w1_all), (w2_hbm, w2_own, w2_all))):
        for q in range(pairs):
            src = w_hbm.at[pl.ds(2 * q, 2), :]
            weights.append(pltpu.make_async_copy(src, w_own.at[q], local_sem.at[i, q]))
            mine.append(pltpu.make_async_copy(src, w_all.at[q, two(my_chip), :], mine_sem.at[i, q]))
    x_load = pltpu.make_async_copy(x_hbm, x_own, chan_sem.at[2])
    biases = [pltpu.make_async_copy(b1_hbm, b1_v, small_sem.at[0]), pltpu.make_async_copy(b2_hbm, b2_v, small_sem.at[1])]
    x_mine = [pltpu.make_async_copy(x_hbm.at[:, image_rows(my_chip, p), :], x_img.at[p, :, two(my_chip), :], chan_sem.at[3 + p]) for p in range(PAIR)]
    smalls = [
        pltpu.make_async_copy(src, dst, small_sem.at[2 + i])
        for i, (src, dst) in enumerate(((g1_hbm, g1), (o1_hbm, o1), (g2_hbm, g2), (o2_hbm, o2), (bc1_hbm, bc1), (bc2_hbm, bc2)))
    ]
    chan_loads = [pltpu.make_async_copy(wc1_hbm, wc1, chan_sem.at[0]), pltpu.make_async_copy(wc2_hbm, wc2, chan_sem.at[1])]
    for c in weights + biases + [x_load] + mine + x_mine + smalls + chan_loads:
        c.start()
    b_own[...] = jnp.zeros_like(b_own)
    for c in biases:
        c.wait()
    for i, b_v in enumerate((b1_v, b2_v)):
        b_own[i, :, pl.ds(0, b_v.shape[1])] = jnp.broadcast_to(b_v[...], (2, b_v.shape[1]))
    for c in weights + [x_load]:
        c.wait()
    pl.semaphore_wait(barrier, n_chips)

    def send_x(p, t):
        part = pl.ds(sum(x_parts[p][:t]), x_parts[p][t])
        to_twins(lambda k: x_own.at[part, image_rows(k, p), :], x_img.at[p, part, two(my_chip), :], x_send.at[p], x_recv.at[p, t])

    to_twins(lambda k: w1_own, w1_all.at[:, two(my_chip), :], w_send.at[0], w_recv.at[0, 0], row_chips)
    to_twins(lambda k: w2_own, w2_all.at[:, two(my_chip), :], w_send.at[1], w_recv.at[1, 0], col_chips)
    to_twins(lambda k: b_own, b_all.at[:, two(my_chip), :], b_send, b_recv)
    send_x(0, 0)
    for c in mine + x_mine + smalls:
        c.wait()
    near = w_tally.at[pl.ds(0, side - 1)]
    far = w_tally.at[pl.ds(0, side * (side - 1))]
    line = w1_all.at[:, pl.ds(pl.multiple_of(2 * side * my_y, 2 * side), 2 * side), :]
    settle(near, w_recv.at[0, 0])
    to_twins(lambda k: line, line, w_send.at[0], w_recv.at[0, 1], col_chips)
    for t in range(1, len(x_parts[0])):
        send_x(0, t)
    settle(near, w_recv.at[1, 0])
    for c in [my_chip] + col_chips:
        block = w2_all.at[:, two(c), :]
        to_twins(lambda k: block, block, w_send.at[1], w_recv.at[1, 1], row_chips)
    for t in range(len(x_parts[1])):
        send_x(1, t)

    even = lax.rem(lax.broadcasted_iota(jnp.int32, (rows, hid), 0), 2) == 0
    keep = (lax.rem(lax.broadcasted_iota(jnp.int32, (rows, 2 * hid), 0), 2) == 0) == (
        lax.broadcasted_iota(jnp.int32, (rows, 2 * hid), 1) < hid
    )

    def expand(w_all, q):
        wq = w_all[q].astype(F32)
        first = jnp.where(even, wq, pltpu.roll(wq, 1, 0))
        second = jnp.where(even, pltpu.roll(wq, rows - 1, 0), wq)
        return [jnp.where(keep, jnp.concatenate([d, d], axis=1), 0.0) for d in (first, second)]

    settle(far, w_recv.at[0, 1])
    q = 0
    while q < pairs:
        group = [q] if q + 1 == pairs else [q, q + 1]
        block = jnp.concatenate([d for g in group for d in expand(w1_all, g)], axis=0)
        w1_t[:, pl.ds(2 * rows * q, block.shape[0])] = jnp.transpose(block).astype(BF16)
        q += len(group)

    def half_sum(p):
        at = 0
        for t, per in enumerate(x_parts[p]):
            settle(x_tally.at[:, pl.ds(0, per)], x_recv.at[p, t])
            wide_x = x_img[p, pl.ds(at, per)].reshape(per * rows, chans).astype(F32)
            u = layer_norm(wide_x, g1[...], o1[...]).astype(BF16)
            last = t == len(x_parts[p]) - 1
            blocks = PAIR if last else 1
            height = PAIR * hid // blocks
            for i in range(blocks):
                span = pl.ds(height * i, height)
                before = h_mine[p, span, :] if t else widen(jnp.concatenate([b1_col[...]] * (height // hid), axis=0), wide)
                h_mine[p, span, :] = before + jnp.dot(w1_t[span, pl.ds(at * rows, per * rows)], u, preferred_element_type=F32)
                for s in range(SWAPS // blocks * i, SWAPS // blocks * (i + 1)) if last else ():
                    swap = pl.ds(piece * s, piece)
                    remote(h_mine.at[p, swap, :], h_other.at[p, swap, :], h_send.at[p, s], h_recv.at[p, s], other)
            at += per

    def activate(p):
        halves = []
        for i in range(SWAPS):
            span = pl.ds(piece * i, piece)
            settle(h_other.at[p, span, :], h_recv.at[p, i])
            halves.append(gelu(h_mine[p, span, :] + h_other[p, span, :]).astype(BF16))
        return jnp.concatenate(halves, axis=0)

    def prepare(slot, p, g, at, per):
        m = per * rows
        span = pl.ds(at * rows, m)
        tok = jnp.dot(w2_big[span, :], g, preferred_element_type=F32) + widen(b2_col[span, :], wide)
        x_mid = (x_img[p, pl.ds(at, per)].reshape(m, chans).astype(F32) + tok).astype(BF16)
        mid_part[slot, pl.ds(0, m), :] = x_mid
        v_part[slot, pl.ds(0, m), :] = layer_norm(x_mid.astype(F32), g2[...], o2[...]).astype(BF16)

    def expand_channels(slot, per):
        m = pl.ds(0, per * rows)
        v = v_part[slot, m, :]
        for f in range(ff // ff_tile):
            cols_f = pl.ds(f * ff_tile, ff_tile)
            pre = jnp.dot(v, wc1[:, cols_f], preferred_element_type=F32) + bc1[:, cols_f]
            act[m, cols_f] = gelu(pre).astype(BF16)

    def contract_channels(slot, p, at, per):
        m = pl.ds(0, per * rows)
        ch_out = jnp.dot(act[m, :], wc2[...], preferred_element_type=F32) + bc2[...]
        z_img[p, pl.ds(at, per)] = (mid_part[slot, m, :].astype(F32) + ch_out).astype(BF16).reshape(per, rows, chans)

    def own_block(i, p, at, per):
        part = pl.ds(at, per)
        away = pltpu.make_async_copy(z_img.at[p, part, two(my_chip), :], spare.at[p, part], own_sem.at[0, i])
        back = pltpu.make_async_copy(spare.at[p, part], out_ref.at[part, image_rows(my_chip, p), :], own_sem.at[1, i])
        return away, back

    settle(b_tally, b_recv)
    is_mine = lax.broadcasted_iota(jnp.int32, (rows, LANES), 0) // 2 == my_chip
    for i in range(2):
        b_all[i] = jnp.where(is_mine, jnp.broadcast_to(b_own[i, pl.ds(0, 1), :], (rows, LANES)), b_all[i])
    per_chip = hid // n_chips
    picked = b_all[0, pl.ds(0, n_chips, stride=2), :]
    spread = jnp.broadcast_to(picked.reshape(n_chips, 1, LANES), (n_chips, per_chip, LANES))
    place = lax.broadcasted_iota(jnp.int32, spread.shape, 1) - (per_chip // CORES) * my_core
    diag = place == lax.broadcasted_iota(jnp.int32, spread.shape, 2)
    col1 = jnp.broadcast_to(jnp.sum(jnp.where(diag, spread, 0.0), axis=2, keepdims=True), spread.shape)
    b1_col[...] = col1.reshape(hid, LANES)
    tail = b_all[1]
    for s in range(patches):
        b2_col[pl.ds(rows * s, rows), :] = jnp.broadcast_to(tail[:, s : s + 1], (rows, LANES))

    half_sum(0)
    settle(far, w_recv.at[1, 1])
    for q in range(pairs):
        w2_big[pl.ds(2 * rows * q, 2 * rows), :] = jnp.concatenate(expand(w2_all, q), axis=0).astype(BF16)
    for c in chan_loads:
        c.wait()

    steps = [(p, sum(parts[:t]), per) for p, parts in enumerate(z_parts) for t, per in enumerate(parts)]
    g = activate(0)
    prepare(0, 0, g, *steps[0][1:])
    own = []
    for i, (p, at, per) in enumerate(steps):
        slot = i % 2
        part = pl.ds(at, per)
        expand_channels(slot, per)
        following = steps[i + 1] if i + 1 < len(steps) else None
        if following and i:
            if following[0] != p:
                g = activate(following[0])
            prepare(1 - slot, following[0], g, *following[1:])
        contract_channels(slot, p, at, per)
        if own:
            own[-1][0].wait()
            own[-1][1].start()
        own.append(own_block(i, p, at, per))
        own[-1][0].start()
        to_twins(lambda k: z_img.at[p, part, two(k), :], out_ref.at[part, image_rows(my_chip, p), :], z_send.at[p], z_recv.at[p])
        if i == 0:
            prepare(1 - slot, p, g, *following[1:])
        if i == b_after:
            half_sum(1)

    own[-1][0].wait()
    own[-1][1].start()
    for _, back in own:
        back.wait()
    for p in range(PAIR):
        settle(x_tally, z_recv.at[p])
    for p in range(PAIR):
        settle(x_tally, z_send.at[p])
        settle(x_tally, x_send.at[p])
        settle(w_tally, w_send.at[p])
        for i in range(SWAPS):
            settle(h_mine.at[p, pl.ds(piece * i, piece), :], h_send.at[p, i])
    settle(b_tally, b_send)


def solution(mesh, x_split=((4, 3, 2), (1,)), z_split=((2, 1), (3, 2, 1)), b_after=0, ff_tile=512):
    row_spec = P("dp", AXIS, None)
    n = mesh.shape[AXIS]

    def local_layer(x_blk, w1_rows, b1_part, w2_cols, b2_part, w_ch1, b_ch1, w_ch2, b_ch2, ln1_gain, ln1_bias, ln2_gain, ln2_bias):
        x_t = jnp.transpose(x_blk, (1, 0, 2))
        w2_rows = jnp.transpose(w2_cols)
        patches, images, chans = x_t.shape
        n_chips = n // CORES
        rows = 2 * n_chips
        hid = w1_rows.shape[1]
        ff = w_ch1.shape[1]
        x_parts, z_parts = ([[patches * w // sum(ws) for w in ws] for ws in split] for split in (x_split, z_split))
        m = max(max(parts) for parts in z_parts) * rows
        hbm = pl.BlockSpec(memory_space=pltpu.HBM)
        sem = pltpu.SemaphoreType.DMA
        smalls = [v[None, :] for v in (b1_part, b2_part, b_ch1, b_ch2, ln1_gain, ln1_bias, ln2_gain, ln2_bias)]
        b1, b2, bc1, bc2, g1, o1, g2, o2 = smalls
        z_t, _ = pl.pallas_call(
            functools.partial(mixer_kernel, n, x_parts, z_parts, b_after, ff_tile),
            name="mixer",
            out_shape=(pltpu.VMEM(x_t.shape, BF16), pltpu.HBM((PAIR, patches, 2, chans), BF16)),
            in_specs=[hbm] * 13,
            out_specs=(pl.BlockSpec(memory_space=pltpu.VMEM), hbm),
            scratch_shapes=[
                pltpu.VMEM(x_t.shape, BF16),
                pltpu.VMEM((PAIR, patches, rows, chans), BF16),
                pltpu.VMEM((PAIR, patches, rows, chans), BF16),
                pltpu.VMEM((patches // 2, 2, hid), BF16),
                pltpu.VMEM((patches // 2, 2, hid), BF16),
                pltpu.VMEM((patches // 2, rows, hid), BF16),
                pltpu.VMEM((patches // 2, rows, hid), BF16),
                pltpu.VMEM((PAIR * hid, patches * rows), BF16),
                pltpu.VMEM((patches * rows, PAIR * hid), BF16),
                pltpu.VMEM((2, 2, LANES), F32),
                pltpu.VMEM((2, rows, LANES), F32),
                pltpu.VMEM((hid, LANES), F32),
                pltpu.VMEM((patches * rows, LANES), F32),
                pltpu.VMEM((PAIR, PAIR * hid, chans), F32),
                pltpu.VMEM((PAIR, PAIR * hid, chans), F32),
                pltpu.VMEM((2, m, chans), BF16),
                pltpu.VMEM((2, m, chans), BF16),
                pltpu.VMEM((m, ff), BF16),
                pltpu.VMEM(w_ch1.shape, BF16),
                pltpu.VMEM(w_ch2.shape, BF16),
                *[pltpu.VMEM(v.shape, F32) for v in smalls],
                pltpu.VMEM((n_chips - 1, patches, 2, chans), BF16),
                pltpu.VMEM((n_chips - 1, patches // 2, 2, hid), BF16),
                pltpu.VMEM((n_chips - 1, 2, 2, LANES), F32),
                sem((2, patches // 2)),
                sem((2, patches // 2)),
                sem((5,)),
                sem((8,)),
                sem((2, sum(len(parts) for parts in z_parts))),
                sem((2,)), sem((2, 2)),
                sem, sem,
                sem((PAIR,)), sem((PAIR, max(len(parts) for parts in x_parts))),
                sem((PAIR, SWAPS)), sem((PAIR, SWAPS)),
                sem((PAIR,)), sem((PAIR,)),
            ],
            compiler_params=pltpu.CompilerParams(
                collective_id=0, has_side_effects=True, vmem_limit_bytes=VMEM_LIMIT - 2 * math.prod(x_t.shape)
            ),
        )(x_t, w1_rows, w2_rows, b1, b2, w_ch1, bc1, w_ch2, bc2, g1, o1, g2, o2)
        return jnp.transpose(z_t, (1, 0, 2))

    in_specs = (row_spec, P(AXIS, None), P(AXIS), P(None, AXIS), P(AXIS), P(None, None), P(None), P(None, None), P(None), P(None), P(None), P(None), P(None))
    return jax.shard_map(local_layer, mesh=mesh, in_specs=in_specs, out_specs=row_spec, check_vma=False)
```

```python
import functools
import math

import jax
import jax.numpy as jnp
from jax import lax
from jax.experimental import pallas as pl
from jax.experimental.pallas import tpu as pltpu
from jax.sharding import PartitionSpec as P

LN_EPS = 1e-6
AXIS = "sp"
LANES = 128
CORES = 2
PAIR = 2
SWAPS = 4
VMEM_LIMIT = 67043328
BF16 = jnp.bfloat16
F32 = jnp.float32


def layer_norm(values, ln_gain, ln_bias):
    mean_val = jnp.mean(values, axis=-1, keepdims=True)
    centred = values - mean_val
    var_val = jnp.mean(centred * centred, axis=-1, keepdims=True)
    return centred * lax.rsqrt(var_val + LN_EPS) * ln_gain + ln_bias


def gelu(a):
    scale = math.sqrt(2.0 / math.pi)
    half = 0.5 * a
    return half + half * jnp.tanh(a * (scale + (scale * 0.044715) * (a * a)))


def widen(column, copies):
    return jnp.concatenate([column] * copies, axis=1)


def send_order(side):
    hops = lambda d: min(d, side - d)
    flows = []
    for dx, dy in sorted(
        ((dx, dy) for dx in range(side) for dy in range(side) if dx or dy),
        key=lambda o: (hops(o[0]) + hops(o[1]), max(hops(o[0]), hops(o[1])), o),
    ):
        for flow in ((dx, dy), ((side - dx) % side, (side - dy) % side)):
            if flow not in flows:
                flows.append(flow)
    return flows[::-1]


def mixer_kernel(
    n, x_parts, z_parts, b_after, ff_tile,
    x_hbm, w1_hbm, w2_hbm, b1_hbm, b2_hbm, wc1_hbm, bc1_hbm, wc2_hbm, bc2_hbm, g1_hbm, o1_hbm, g2_hbm, o2_hbm,
    out_ref, spare,
    x_own, x_img, z_img, w1_own, w2_own, w1_all, w2_all, w1_t, w2_big, b_own, b_all, b1_col, b2_col, h_mine, h_other, v_part, mid_part, act, wc1, wc2,
    b1_v, b2_v, bc1, bc2, g1, o1, g2, o2, x_tally, w_tally, b_tally,
    local_sem, mine_sem, chan_sem, small_sem, own_sem,
    w_send, w_recv, b_send, b_recv, x_send, x_recv, h_send, h_recv, z_send, z_recv,
):
    me = lax.axis_index(AXIS)
    side = math.isqrt(n // CORES)
    my_core = lax.rem(me, CORES)
    my_chip = me // CORES
    my_x = lax.rem(my_chip, side)
    my_y = my_chip // side
    cols = [lax.rem(my_x + d, side) for d in range(side)]
    lines = [lax.rem(my_y + d, side) * side for d in range(side)]
    chips = [lines[dy] + cols[dx] for dx, dy in send_order(side)]
    row_chips = [lines[0] + cols[dx] for dx, dy in send_order(side) if dy == 0]
    col_chips = [lines[dy] + cols[0] for dx, dy in send_order(side) if dx == 0]
    other = me + 1 - 2 * my_core
    n_chips = n // CORES
    _, patches, rows, chans = x_img.shape
    pairs = patches // 2
    hid = w1_hbm.shape[1]
    wide = chans // LANES
    ff = wc1.shape[1]
    piece = PAIR * hid // SWAPS

    def two(j):
        return pl.ds(pl.multiple_of(2 * j, 2), 2)

    def image_rows(chip, p):
        return pl.ds(pl.multiple_of(2 * CORES * chip + 2 * p, 2), 2)

    def settle(counted, sem):
        pltpu.make_async_copy(counted, counted, sem).wait()

    def remote(src, dst, ss, rs, j):
        pltpu.make_async_remote_copy(src_ref=src, dst_ref=dst, send_sem=ss, recv_sem=rs, device_id={AXIS: j}).start()

    def to_twins(src, dst, ss, rs, targets=chips):
        for k in targets:
            remote(src(k), dst, ss, rs, CORES * k + my_core)

    b_all[...] = jnp.zeros_like(b_all)

    barrier = pltpu.get_barrier_semaphore()
    for j in [CORES * k + my_core for k in chips] + [other]:
        pl.semaphore_signal(barrier, inc=1, device_id={AXIS: j})

    weights, mine = [], []
    for i, (w_hbm, w_own, w_all) in enumerate(((w1_hbm, w1_own, w1_all), (w2_hbm, w2_own, w2_all))):
        for q in range(pairs):
            src = w_hbm.at[pl.ds(2 * q, 2), :]
            weights.append(pltpu.make_async_copy(src, w_own.at[q], local_sem.at[i, q]))
            mine.append(pltpu.make_async_copy(src, w_all.at[q, two(my_chip), :], mine_sem.at[i, q]))
    x_load = pltpu.make_async_copy(x_hbm, x_own, chan_sem.at[2])
    biases = [pltpu.make_async_copy(b1_hbm, b1_v, small_sem.at[0]), pltpu.make_async_copy(b2_hbm, b2_v, small_sem.at[1])]
    x_mine = [pltpu.make_async_copy(x_hbm.at[:, image_rows(my_chip, p), :], x_img.at[p, :, two(my_chip), :], chan_sem.at[3 + p]) for p in range(PAIR)]
    smalls = [
        pltpu.make_async_copy(src, dst, small_sem.at[2 + i])
        for i, (src, dst) in enumerate(((g1_hbm, g1), (o1_hbm, o1), (g2_hbm, g2), (o2_hbm, o2), (bc1_hbm, bc1), (bc2_hbm, bc2)))
    ]
    chan_loads = [pltpu.make_async_copy(wc1_hbm, wc1, chan_sem.at[0]), pltpu.make_async_copy(wc2_hbm, wc2, chan_sem.at[1])]
    for c in weights + biases + [x_load] + mine + x_mine + smalls + chan_loads:
        c.start()
    b_own[...] = jnp.zeros_like(b_own)
    for c in biases:
        c.wait()
    for i, b_v in enumerate((b1_v, b2_v)):
        b_own[i, :, pl.ds(0, b_v.shape[1])] = jnp.broadcast_to(b_v[...], (2, b_v.shape[1]))
    for c in weights + [x_load]:
        c.wait()
    pl.semaphore_wait(barrier, n_chips)

    def send_x(p, t):
        part = pl.ds(sum(x_parts[p][:t]), x_parts[p][t])
        to_twins(lambda k: x_own.at[part, image_rows(k, p), :], x_img.at[p, part, two(my_chip), :], x_send.at[p], x_recv.at[p, t])

    to_twins(lambda k: w1_own, w1_all.at[:, two(my_chip), :], w_send.at[0], w_recv.at[0, 0], row_chips)
    to_twins(lambda k: w2_own, w2_all.at[:, two(my_chip), :], w_send.at[1], w_recv.at[1, 0], col_chips)
    to_twins(lambda k: b_own, b_all.at[:, two(my_chip), :], b_send, b_recv)
    send_x(0, 0)
    for c in mine + x_mine + smalls:
        c.wait()
    near = w_tally.at[pl.ds(0, side - 1)]
    far = w_tally.at[pl.ds(0, side * (side - 1))]
    line = w1_all.at[:, pl.ds(pl.multiple_of(2 * side * my_y, 2 * side), 2 * side), :]
    settle(near, w_recv.at[0, 0])
    to_twins(lambda k: line, line, w_send.at[0], w_recv.at[0, 1], col_chips)
    for t in range(1, len(x_parts[0])):
        send_x(0, t)
    settle(near, w_recv.at[1, 0])
    for c in [my_chip] + col_chips:
        block = w2_all.at[:, two(c), :]
        to_twins(lambda k: block, block, w_send.at[1], w_recv.at[1, 1], row_chips)
    for t in range(len(x_parts[1])):
        send_x(1, t)

    even = lax.rem(lax.broadcasted_iota(jnp.int32, (rows, hid), 0), 2) == 0
    keep = (lax.rem(lax.broadcasted_iota(jnp.int32, (rows, 2 * hid), 0), 2) == 0) == (
        lax.broadcasted_iota(jnp.int32, (rows, 2 * hid), 1) < hid
    )

    def expand(w_all, q):
        wq = w_all[q].astype(F32)
        first = jnp.where(even, wq, pltpu.roll(wq, 1, 0))
        second = jnp.where(even, pltpu.roll(wq, rows - 1, 0), wq)
        return [jnp.where(keep, jnp.concatenate([d, d], axis=1), 0.0) for d in (first, second)]

    settle(far, w_recv.at[0, 1])
    q = 0
    while q < pairs:
        group = [q] if q + 1 == pairs else [q, q + 1]
        block = jnp.concatenate([d for g in group for d in expand(w1_all, g)], axis=0)
        w1_t[:, pl.ds(2 * rows * q, block.shape[0])] = jnp.transpose(block).astype(BF16)
        q += len(group)

    def half_sum(p):
        at = 0
        for t, per in enumerate(x_parts[p]):
            settle(x_tally.at[:, pl.ds(0, per)], x_recv.at[p, t])
            wide_x = x_img[p, pl.ds(at, per)].reshape(per * rows, chans).astype(F32)
            u = layer_norm(wide_x, g1[...], o1[...]).astype(BF16)
            last = t == len(x_parts[p]) - 1
            blocks = PAIR if last else 1
            height = PAIR * hid // blocks
            for i in range(blocks):
                span = pl.ds(height * i, height)
                before = h_mine[p, span, :] if t else widen(jnp.concatenate([b1_col[...]] * (height // hid), axis=0), wide)
                h_mine[p, span, :] = before + jnp.dot(w1_t[span, pl.ds(at * rows, per * rows)], u, preferred_element_type=F32)
                for s in range(SWAPS // blocks * i, SWAPS // blocks * (i + 1)) if last else ():
                    swap = pl.ds(piece * s, piece)
                    remote(h_mine.at[p, swap, :], h_other.at[p, swap, :], h_send.at[p, s], h_recv.at[p, s], other)
            at += per

    def activate(p):
        halves = []
        for i in range(SWAPS):
            span = pl.ds(piece * i, piece)
            settle(h_other.at[p, span, :], h_recv.at[p, i])
            halves.append(gelu(h_mine[p, span, :] + h_other[p, span, :]).astype(BF16))
        return jnp.concatenate(halves, axis=0)

    def prepare(slot, p, g, at, per):
        m = per * rows
        span = pl.ds(at * rows, m)
        tok = jnp.dot(w2_big[span, :], g, preferred_element_type=F32) + widen(b2_col[span, :], wide)
        x_mid = (x_img[p, pl.ds(at, per)].reshape(m, chans).astype(F32) + tok).astype(BF16)
        mid_part[slot, pl.ds(0, m), :] = x_mid
        v_part[slot, pl.ds(0, m), :] = layer_norm(x_mid.astype(F32), g2[...], o2[...]).astype(BF16)

    def expand_channels(slot, per):
        m = pl.ds(0, per * rows)
        v = v_part[slot, m, :]
        for f in range(ff // ff_tile):
            cols_f = pl.ds(f * ff_tile, ff_tile)
            pre = jnp.dot(v, wc1[:, cols_f], preferred_element_type=F32) + bc1[:, cols_f]
            act[m, cols_f] = gelu(pre).astype(BF16)

    def contract_channels(slot, p, at, per):
        m = pl.ds(0, per * rows)
        ch_out = jnp.dot(act[m, :], wc2[...], preferred_element_type=F32) + bc2[...]
        z_img[p, pl.ds(at, per)] = (mid_part[slot, m, :].astype(F32) + ch_out).astype(BF16).reshape(per, rows, chans)

    def own_block(i, p, at, per):
        part = pl.ds(at, per)
        away = pltpu.make_async_copy(z_img.at[p, part, two(my_chip), :], spare.at[p, part], own_sem.at[0, i])
        back = pltpu.make_async_copy(spare.at[p, part], out_ref.at[part, image_rows(my_chip, p), :], own_sem.at[1, i])
        return away, back

    settle(b_tally, b_recv)
    is_mine = lax.broadcasted_iota(jnp.int32, (rows, LANES), 0) // 2 == my_chip
    for i in range(2):
        b_all[i] = jnp.where(is_mine, jnp.broadcast_to(b_own[i, pl.ds(0, 1), :], (rows, LANES)), b_all[i])
    per_chip = hid // n_chips
    picked = b_all[0, pl.ds(0, n_chips, stride=2), :]
    spread = jnp.broadcast_to(picked.reshape(n_chips, 1, LANES), (n_chips, per_chip, LANES))
    place = lax.broadcasted_iota(jnp.int32, spread.shape, 1) - (per_chip // CORES) * my_core
    diag = place == lax.broadcasted_iota(jnp.int32, spread.shape, 2)
    col1 = jnp.broadcast_to(jnp.sum(jnp.where(diag, spread, 0.0), axis=2, keepdims=True), spread.shape)
    b1_col[...] = col1.reshape(hid, LANES)
    tail = b_all[1]
    for s in range(patches):
        b2_col[pl.ds(rows * s, rows), :] = jnp.broadcast_to(tail[:, s : s + 1], (rows, LANES))

    half_sum(0)
    settle(far, w_recv.at[1, 1])
    for q in range(pairs):
        w2_big[pl.ds(2 * rows * q, 2 * rows), :] = jnp.concatenate(expand(w2_all, q), axis=0).astype(BF16)
    for c in chan_loads:
        c.wait()

    steps = [(p, sum(parts[:t]), per) for p, parts in enumerate(z_parts) for t, per in enumerate(parts)]
    g = activate(0)
    prepare(0, 0, g, *steps[0][1:])
    own = []
    for i, (p, at, per) in enumerate(steps):
        slot = i % 2
        part = pl.ds(at, per)
        expand_channels(slot, per)
        following = steps[i + 1] if i + 1 < len(steps) else None
        if following and i and following[0] == p:
            prepare(1 - slot, p, g, *following[1:])
        contract_channels(slot, p, at, per)
        if own:
            own[-1][0].wait()
            own[-1][1].start()
        own.append(own_block(i, p, at, per))
        own[-1][0].start()
        to_twins(lambda k: z_img.at[p, part, two(k), :], out_ref.at[part, image_rows(my_chip, p), :], z_send.at[p], z_recv.at[p])
        if i == 0:
            prepare(1 - slot, p, g, *following[1:])
        elif following and following[0] != p:
            g = activate(following[0])
            prepare(1 - slot, following[0], g, *following[1:])
        if i == b_after:
            half_sum(1)

    own[-1][0].wait()
    own[-1][1].start()
    for _, back in own:
        back.wait()
    for p in range(PAIR):
        settle(x_tally, z_recv.at[p])
    for p in range(PAIR):
        settle(x_tally, z_send.at[p])
        settle(x_tally, x_send.at[p])
        settle(w_tally, w_send.at[p])
        for i in range(SWAPS):
            settle(h_mine.at[p, pl.ds(piece * i, piece), :], h_send.at[p, i])
    settle(b_tally, b_send)


def solution(mesh, x_split=((4, 3, 2), (1,)), z_split=((2, 1), (4, 3, 2)), b_after=0, ff_tile=512):
    row_spec = P("dp", AXIS, None)
    n = mesh.shape[AXIS]

    def local_layer(x_blk, w1_rows, b1_part, w2_cols, b2_part, w_ch1, b_ch1, w_ch2, b_ch2, ln1_gain, ln1_bias, ln2_gain, ln2_bias):
        x_t = jnp.transpose(x_blk, (1, 0, 2))
        w2_rows = jnp.transpose(w2_cols)
        patches, images, chans = x_t.shape
        n_chips = n // CORES
        rows = 2 * n_chips
        hid = w1_rows.shape[1]
        ff = w_ch1.shape[1]
        x_parts, z_parts = ([[patches * w // sum(ws) for w in ws] for ws in split] for split in (x_split, z_split))
        m = max(max(parts) for parts in z_parts) * rows
        hbm = pl.BlockSpec(memory_space=pltpu.HBM)
        sem = pltpu.SemaphoreType.DMA
        smalls = [v[None, :] for v in (b1_part, b2_part, b_ch1, b_ch2, ln1_gain, ln1_bias, ln2_gain, ln2_bias)]
        b1, b2, bc1, bc2, g1, o1, g2, o2 = smalls
        z_t, _ = pl.pallas_call(
            functools.partial(mixer_kernel, n, x_parts, z_parts, b_after, ff_tile),
            name="mixer",
            out_shape=(pltpu.VMEM(x_t.shape, BF16), pltpu.HBM((PAIR, patches, 2, chans), BF16)),
            in_specs=[hbm] * 13,
            out_specs=(pl.BlockSpec(memory_space=pltpu.VMEM), hbm),
            scratch_shapes=[
                pltpu.VMEM(x_t.shape, BF16),
                pltpu.VMEM((PAIR, patches, rows, chans), BF16),
                pltpu.VMEM((PAIR, patches, rows, chans), BF16),
                pltpu.VMEM((patches // 2, 2, hid), BF16),
                pltpu.VMEM((patches // 2, 2, hid), BF16),
                pltpu.VMEM((patches // 2, rows, hid), BF16),
                pltpu.VMEM((patches // 2, rows, hid), BF16),
                pltpu.VMEM((PAIR * hid, patches * rows), BF16),
                pltpu.VMEM((patches * rows, PAIR * hid), BF16),
                pltpu.VMEM((2, 2, LANES), F32),
                pltpu.VMEM((2, rows, LANES), F32),
                pltpu.VMEM((hid, LANES), F32),
                pltpu.VMEM((patches * rows, LANES), F32),
                pltpu.VMEM((PAIR, PAIR * hid, chans), F32),
                pltpu.VMEM((PAIR, PAIR * hid, chans), F32),
                pltpu.VMEM((2, m, chans), BF16),
                pltpu.VMEM((2, m, chans), BF16),
                pltpu.VMEM((m, ff), BF16),
                pltpu.VMEM(w_ch1.shape, BF16),
                pltpu.VMEM(w_ch2.shape, BF16),
                *[pltpu.VMEM(v.shape, F32) for v in smalls],
                pltpu.VMEM((n_chips - 1, patches, 2, chans), BF16),
                pltpu.VMEM((n_chips - 1, patches // 2, 2, hid), BF16),
                pltpu.VMEM((n_chips - 1, 2, 2, LANES), F32),
                sem((2, patches // 2)),
                sem((2, patches // 2)),
                sem((5,)),
                sem((8,)),
                sem((2, sum(len(parts) for parts in z_parts))),
                sem((2,)), sem((2, 2)),
                sem, sem,
                sem((PAIR,)), sem((PAIR, max(len(parts) for parts in x_parts))),
                sem((PAIR, SWAPS)), sem((PAIR, SWAPS)),
                sem((PAIR,)), sem((PAIR,)),
            ],
            compiler_params=pltpu.CompilerParams(
                collective_id=0, has_side_effects=True, vmem_limit_bytes=VMEM_LIMIT - 2 * math.prod(x_t.shape)
            ),
        )(x_t, w1_rows, w2_rows, b1, b2, w_ch1, bc1, w_ch2, bc2, g1, o1, g2, o2)
        return jnp.transpose(z_t, (1, 0, 2))

    in_specs = (row_spec, P(AXIS, None), P(AXIS), P(None, AXIS), P(AXIS), P(None, None), P(None), P(None, None), P(None), P(None), P(None), P(None), P(None))
    return jax.shard_map(local_layer, mesh=mesh, in_specs=in_specs, out_specs=row_spec, check_vma=False)
```
